32 devices in a mesh: dp: 1 (over z), tp: 4 (over y), sp: 8 (over x, core).
Axes of the slice: x: 4, y: 4, z: 1, core: 2. Of those that a mesh axis runs over, the one named last changes fastest.
The devices are a block of a 4x4x8 slice.
Arguments:
- hidden: bfloat16 [256, 6144], P('dp')
- lengths: int32 [256], P('dp')
- k_cache: bfloat16 [256, 256, 8, 128], P('dp', 'sp', 'tp')
- v_cache: bfloat16 [256, 256, 8, 128], P('dp', 'sp', 'tp')
- norm_gain: bfloat16 [6144], replicated
- w_query: bfloat16 [6144, 6144], P(None, 'tp')
- w_key: bfloat16 [6144, 1024], P(None, 'tp')
- w_value: bfloat16 [6144, 1024], P(None, 'tp')
- w_out: bfloat16 [6144, 6144], P('tp')
Outputs:
- output 1: bfloat16 [256, 6144], P('dp')
- output 2: bfloat16 [256, 256, 8, 128], P('dp', 'sp', 'tp')
- output 3: bfloat16 [256, 256, 8, 128], P('dp', 'sp', 'tp')
All inputs are finite; a program needn't handle non-finite values.
Results may differ from the reference program's by a relative error of at most 0.00455691.
Values sent between devices are 32-bit elements.
A program may use at most 768 MiB of HBM per device.

```python
import jax
import jax.numpy as jnp
from jax import lax

D_MODEL = 6144
HEADS = 48
KV_HEADS = 8
HEAD_DIM = 128
BATCH = 256
SEQ_LEN = 256

GROUP_SIZE = HEADS // KV_HEADS
SCALE = HEAD_DIM ** -0.5
EPS = 1e-6
NEG_BIG = -1e30


def setup_inputs(seed: int = 0, part: int = 0) -> dict:
    part_keys = jax.random.split(jax.random.fold_in(jax.random.key(seed), part), 4)
    shared_keys = jax.random.split(jax.random.key(seed + 1), 5)
    cache_shape = (BATCH, SEQ_LEN, KV_HEADS, HEAD_DIM)
    hidden = jax.random.normal(part_keys[0], (BATCH, D_MODEL), jnp.float32)
    lengths = jax.random.randint(part_keys[1], (BATCH,), 0, SEQ_LEN, jnp.int32)
    lengths = lengths.at[0].set(SEQ_LEN - 1)
    k_cache = jax.random.normal(part_keys[2], cache_shape, jnp.float32)
    steps = jax.random.normal(part_keys[3], cache_shape, jnp.float32)
    v_cache = jnp.cumsum(steps, axis=1) * (2.0 / SEQ_LEN) ** 0.5 + steps
    norm_gain = 1.0 + 0.5 * jax.random.normal(shared_keys[0], (D_MODEL,), jnp.float32)
    w_query = jax.random.normal(shared_keys[1], (D_MODEL, HEADS * HEAD_DIM), jnp.float32) * D_MODEL ** -0.5
    w_key = jax.random.normal(shared_keys[2], (D_MODEL, KV_HEADS * HEAD_DIM), jnp.float32) * D_MODEL ** -0.5
    w_value = jax.random.normal(shared_keys[3], (D_MODEL, KV_HEADS * HEAD_DIM), jnp.float32) * D_MODEL ** -0.5
    w_out = jax.random.normal(shared_keys[4], (HEADS * HEAD_DIM, D_MODEL), jnp.float32) * (HEADS * HEAD_DIM) ** -0.5
    return {
        'hidden': hidden.astype(jnp.bfloat16),
        'lengths': lengths,
        'k_cache': k_cache.astype(jnp.bfloat16),
        'v_cache': v_cache.astype(jnp.bfloat16),
        'norm_gain': norm_gain.astype(jnp.bfloat16),
        'w_query': w_query.astype(jnp.bfloat16),
        'w_key': w_key.astype(jnp.bfloat16),
        'w_value': w_value.astype(jnp.bfloat16),
        'w_out': w_out.astype(jnp.bfloat16),
    }


def reference(hidden, lengths, k_cache, v_cache, norm_gain, w_query, w_key, w_value, w_out):
    hid_f32 = hidden.astype(jnp.float32)
    inv_rms = lax.rsqrt(jnp.mean(hid_f32 * hid_f32, axis=-1, keepdims=True) + EPS)
    normed = (hid_f32 * inv_rms * norm_gain.astype(jnp.float32)).astype(jnp.bfloat16)
    query = jnp.dot(normed, w_query, preferred_element_type=jnp.float32).astype(jnp.bfloat16)
    new_key = jnp.dot(normed, w_key, preferred_element_type=jnp.float32).astype(jnp.bfloat16)
    new_value = jnp.dot(normed, w_value, preferred_element_type=jnp.float32).astype(jnp.bfloat16)
    positions = jnp.arange(SEQ_LEN)
    at_slot = (positions[None, :] == lengths[:, None])[:, :, None, None]
    k_new = jnp.where(at_slot, new_key.reshape(BATCH, 1, KV_HEADS, HEAD_DIM), k_cache)
    v_new = jnp.where(at_slot, new_value.reshape(BATCH, 1, KV_HEADS, HEAD_DIM), v_cache)
    query_groups = query.reshape(BATCH, KV_HEADS, GROUP_SIZE, HEAD_DIM)

    def one_sequence(item):
        q_seq, k_seq, v_seq, length = item
        scores = jnp.einsum('kgd,tkd->kgt', q_seq.astype(jnp.float32), k_seq.astype(jnp.float32)) * SCALE
        valid = positions <= length
        scores = jnp.where(valid, scores, NEG_BIG)
        peak = jnp.max(scores, axis=-1, keepdims=True)
        exp_vals = jnp.where(valid, jnp.exp(scores - peak), 0.0)
        denom_sum = jnp.sum(exp_vals, axis=-1, keepdims=True)
        weighted = jnp.einsum('kgt,tkd->kgd', exp_vals.astype(jnp.bfloat16).astype(jnp.float32), v_seq.astype(jnp.float32))
        return (weighted / denom_sum).astype(jnp.bfloat16)

    attn_out = lax.map(one_sequence, (query_groups, k_new, v_new, lengths))
    proj_sum = jnp.dot(attn_out.reshape(BATCH, HEADS * HEAD_DIM), w_out, preferred_element_type=jnp.float32)
    hidden_out = (hid_f32 + proj_sum).astype(jnp.bfloat16)
    return (hidden_out, k_new, v_new)
```

```python
import functools
import math

import jax
import jax.numpy as jnp
from jax import lax
from jax.experimental import pallas as pl
from jax.experimental.pallas import tpu as pltpu
from jax.sharding import PartitionSpec as P

EPS = 1e-6
NEG_BIG = -1e30
MESH = pl.DeviceIdType.MESH
F32 = jnp.float32
BF16 = jnp.bfloat16
MIB = 1 << 20


def attention_kernel(dims, len_ref, hid_hbm, gain_ref, wq_hbm, wk_hbm, wv_hbm, kc_hbm, vc_hbm,
                     acc_ref, kout_hbm, vout_hbm,
                     hbuf, nbuf, wbuf, kbuf, vbuf, qs, ks, vs,
                     sem_h, sem_w, sem_k, sem_v, sem_ko, sem_vo):
    batch, d_model, heads, kv, group, head_dim, seq_block, sp = dims
    n_wq = wq_hbm.shape[1] // 256
    n_w = n_wq + 2
    base = lax.axis_index('sp') * seq_block
    chunk = batch // sp
    rows_h = batch // 4

    hid_copies = [pltpu.make_async_copy(hid_hbm.at[pl.ds(i * rows_h, rows_h)], hbuf.at[pl.ds(i * rows_h, rows_h)], sem_h.at[i])
                  for i in range(4)]
    w_copies = [pltpu.make_async_copy(wq_hbm.at[:, pl.ds(j * 256, 256)], wbuf.at[j], sem_w.at[j]) for j in range(n_wq)]
    w_copies.append(pltpu.make_async_copy(wk_hbm, wbuf.at[n_wq], sem_w.at[n_wq]))
    w_copies.append(pltpu.make_async_copy(wv_hbm, wbuf.at[n_wq + 1], sem_w.at[n_wq + 1]))
    crow = chunk * seq_block

    def cache_copy(c, src, buf, sem):
        return pltpu.make_async_copy(src.at[pl.ds(c * crow, crow)], buf.at[pl.ds(c * crow, crow)], sem.at[c])

    def cache_back(c, buf, dst, sem):
        return pltpu.make_async_copy(buf.at[pl.ds(c * crow, crow)], dst.at[pl.ds(c * crow, crow)], sem.at[c])

    for cp in hid_copies:
        cp.start()
    for cp in w_copies:
        cp.start()
    for c in range(sp):
        cache_copy(c, kc_hbm, kbuf, sem_k).start()
        cache_copy(c, vc_hbm, vbuf, sem_v).start()

    step = 16
    wide = 1024
    for i in range(4):
        hid_copies[i].wait()

        def norm_rows(r, carry, i=i):
            row = pl.multiple_of(i * rows_h + r * step, step)
            total = jnp.zeros((step, 1), F32)
            for w in range(d_model // wide):
                x = hbuf[pl.ds(row, step), w * wide:(w + 1) * wide].astype(F32)
                total = total + jnp.sum(x * x, axis=1, keepdims=True)
            inv = lax.rsqrt(total / d_model + EPS)
            for w in range(d_model // wide):
                x = hbuf[pl.ds(row, step), w * wide:(w + 1) * wide].astype(F32)
                g = gain_ref[:, w * wide:(w + 1) * wide].astype(F32)
                nbuf[pl.ds(row, step), w * wide:(w + 1) * wide] = (x * inv * g).astype(BF16)
            return carry

        lax.fori_loop(0, rows_h // step, norm_rows, 0)

    def project_q(j, carry):
        pltpu.make_async_copy(wk_hbm, wbuf.at[j], sem_w.at[j]).wait()
        res = jnp.dot(nbuf[...], wbuf[j], preferred_element_type=F32)
        for i in range(2):
            qs[pl.ds(2 * j + i, batch, stride=heads), :] = res[:, i * head_dim:(i + 1) * head_dim]
        return carry

    lax.fori_loop(0, n_wq, project_q, 0)
    for n, dst in ((n_wq, ks), (n_wq + 1, vs)):
        w_copies[n].wait()
        res = jnp.dot(nbuf[...], wbuf[n], preferred_element_type=F32)
        for i in range(kv):
            dst[pl.ds(i, batch, stride=kv), :] = res[:, i * head_dim:(i + 1) * head_dim]

    gs = 4
    qrows = gs * heads
    krows = gs * seq_block * kv
    row_id = lax.broadcasted_iota(jnp.int32, (qrows, krows), 0)
    col_id = lax.broadcasted_iota(jnp.int32, (qrows, krows), 1)
    same = ((row_id // heads == col_id // (seq_block * kv))
            & ((row_id % heads) // group == col_id % kv))
    col_row = lax.broadcasted_iota(jnp.int32, (1, krows), 1)
    col_seq = col_row // (seq_block * kv)
    col_pos = (col_row % (seq_block * kv)) // kv
    half_rows = chunk * heads // 2
    diag = (lax.broadcasted_iota(jnp.int32, (half_rows, 128), 0) % 128
            == lax.broadcasted_iota(jnp.int32, (half_rows, 128), 1))
    fold = (head_dim ** -0.5) * math.log2(math.e)
    spare = batch * seq_block

    def pack_column(col):
        spread = jnp.where(diag, jnp.broadcast_to(col, (half_rows, 128)), 0.0)
        out = []
        for r in range(0, half_rows, 128):
            out.append(jnp.sum(spread[r:min(r + 128, half_rows)], axis=0, keepdims=True))
        return jnp.concatenate(out, axis=0)

    def attend(c, carry):
        cache_copy(c, kc_hbm, kbuf, sem_k).wait()
        cache_copy(c, vc_hbm, vbuf, sem_v).wait()
        b_first = c * chunk
        for g in range(chunk // gs):
            b0 = b_first + g * gs
            kn = ks[pl.ds(pl.multiple_of(b0 * kv, 8), gs * kv), :].astype(BF16)
            vn = vs[pl.ds(pl.multiple_of(b0 * kv, 8), gs * kv), :].astype(BF16)
            for i in range(gs):
                p = len_ref[b0 + i] - base
                inside = (p >= 0) & (p < seq_block)
                at = jnp.where(inside, (b0 + i) * seq_block + p, spare)
                kbuf[at] = kn[i * kv:(i + 1) * kv]
                vbuf[at] = vn[i * kv:(i + 1) * kv]
        cache_back(c, kbuf, kout_hbm, sem_ko).start()
        cache_back(c, vbuf, vout_hbm, sem_vo).start()
        ms, ls = [], []
        for g in range(chunk // gs):
            b0 = b_first + g * gs
            q = qs[pl.ds(pl.multiple_of(b0 * heads, 8), qrows), :].astype(BF16)
            k = kbuf.at[pl.ds(b0 * seq_block, gs * seq_block)].reshape(krows, head_dim)[...]
            v = vbuf.at[pl.ds(b0 * seq_block, gs * seq_block)].reshape(krows, head_dim)[...]
            s = lax.dot_general(q, k, (((1,), (1,)), ((), ())), preferred_element_type=F32)
            last = jnp.full((1, krows), len_ref[b0] - base, jnp.int32)
            for i in range(1, gs):
                last = jnp.where(col_seq == i, len_ref[b0 + i] - base, last)
            mask = same & (col_pos <= last)
            s = jnp.where(mask, s * fold, NEG_BIG)
            m = jnp.max(s, axis=1, keepdims=True)
            e = jnp.where(mask, jnp.exp2(s - m), 0.0)
            ls.append(jnp.sum(e, axis=1, keepdims=True))
            ms.append(m)
            o = jnp.dot(e.astype(BF16), v, preferred_element_type=F32)
            half, part = divmod(g, chunk // gs // 2)
            acc_ref[2 * c + half, part * qrows:(part + 1) * qrows, :] = o
        per = chunk // gs // 2
        for half in range(2):
            mp = pack_column(jnp.concatenate(ms[half * per:(half + 1) * per], axis=0))
            lp = pack_column(jnp.concatenate(ls[half * per:(half + 1) * per], axis=0))
            acc_ref[2 * c + half, half_rows:half_rows + 8, :] = jnp.concatenate(
                [mp, lp, jnp.zeros((4, 128), F32)], axis=0)
        return carry

    lax.fori_loop(0, sp, attend, 0)
    for c in range(sp):
        cache_back(c, kbuf, kout_hbm, sem_ko).wait()
        cache_back(c, vbuf, vout_hbm, sem_vo).wait()


def exchange_kernel(dims, acc_ref, hid_hbm, wo_hbm, out_ref,
                    pbuf, xsend, xrecv, obuf, lhs, wbuf, ysend, yrecv, hblk, gbuf,
                    sem_w, sem_hid, sem_ps, sem_pr, sem_xs, sem_xr, sem_os, sem_or, sem_ys, sem_yr,
                    sem_fs, sem_fr, sem_ss, sem_sr, sem_ds, sem_dr):
    batch, d_model, heads, kv, group, head_dim, seq_block, sp = dims
    tp_n = lax.axis_size('tp')
    nx, ny = sp // 2, tp_n
    spi = lax.axis_index('sp')
    y = lax.axis_index('tp')
    x, c = spi // 2, spi % 2
    hr = (batch // sp) * heads // 2
    rows = batch // nx
    cols = d_model // (2 * ny)
    hc = cols // 2

    def at_x(d):
        return (x + d) % nx

    def at_y(d):
        return (y + d) % ny

    def to(tp_pos, sp_pos):
        return {'tp': tp_pos, 'sp': sp_pos}

    partner = to(y, x * 2 + 1 - c)

    def x_dev(d):
        return to(y, at_x(d) * 2 + c)

    def y_dev(d):
        return to(at_y(d), spi)

    def remote(src, dst, ssem, rsem, dev):
        return pltpu.make_async_remote_copy(src_ref=src, dst_ref=dst, send_sem=ssem, recv_sem=rsem,
                                            device_id=dev, device_id_type=MESH)

    order = (2, 1, -1, 0)
    w_copies = []
    for k, d in enumerate(order):
        first = pl.multiple_of(c * (d_model // 2) + at_y(d) * cols, 128)
        w_copies.append(pltpu.make_async_copy(wo_hbm.at[:, pl.ds(first, cols)], wbuf.at[k], sem_w.at[k]))
    hid_copy = pltpu.make_async_copy(
        hid_hbm.at[pl.ds(pl.multiple_of(x * rows, rows), rows), pl.ds(pl.multiple_of(c * (d_model // 2) + y * cols, 128), cols)],
        hblk, sem_hid)

    barrier = pltpu.get_barrier_semaphore()
    peers = [partner, x_dev(1), x_dev(-1), y_dev(1), y_dev(-1)]
    for dev in peers:
        pl.semaphore_signal(barrier, inc=1, device_id=dev, device_id_type=MESH)
    for cp in w_copies:
        cp.start()
    hid_copy.start()
    pl.semaphore_wait(barrier, len(peers))

    pair = []
    for k, d in enumerate(order):
        src = acc_ref.at[pl.ds(4 * at_x(d) + 2 * (1 - c), 2)]
        pair.append(remote(src, pbuf.at[k], sem_ps.at[k], sem_pr.at[k], partner))
        pair[-1].start()

    eye = (lax.broadcasted_iota(jnp.int32, (hr, 128), 0) % 128
           == lax.broadcasted_iota(jnp.int32, (hr, 128), 1))
    n_stat = -(-hr // 128)

    def column(stat):
        parts = []
        for i in range(n_stat):
            size = min(128, hr - i * 128)
            parts.append(jnp.broadcast_to(stat[i:i + 1, :], (size, 128)))
        spread = jnp.where(eye, jnp.concatenate(parts, axis=0), 0.0)
        return jnp.sum(spread, axis=1, keepdims=True)

    def stats(ref):
        return ref[hr:hr + n_stat, :], ref[hr + n_stat:hr + 2 * n_stat, :]

    def merge(refs):
        both = [stats(r) for r in refs]
        peak = functools.reduce(jnp.maximum, [m for m, _ in both])
        scale = [jnp.exp2(m - peak) for m, _ in both]
        denom = sum(l * s for (_, l), s in zip(both, scale))
        total = sum(r[0:hr, :] * column(s) for r, s in zip(refs, scale))
        return total, peak, denom

    def merge_into(dst, refs):
        total, peak, denom = merge(refs)
        dst[0:hr, :] = total
        dst[hr:hr + 8, :] = jnp.concatenate([peak, denom, jnp.zeros((8 - 2 * n_stat, 128), F32)], axis=0)

    def mine(d, half):
        return acc_ref.at[4 * at_x(d) + 2 * c + half]

    xc = [remote(xsend.at[i], xrecv.at[i], sem_xs.at[i], sem_xr.at[i], x_dev(1 if i in (0, 2, 4) else -1))
          for i in range(6)]
    pair[0].wait_recv()
    merge_into(xsend.at[0], [mine(2, 0), pbuf.at[0, 0]])
    xc[0].start()
    merge_into(xsend.at[1], [mine(2, 1), pbuf.at[0, 1]])
    xc[1].start()
    pair[1].wait_recv()
    merge_into(xsend.at[2], [mine(1, 1), pbuf.at[1, 1]])
    xc[2].start()
    pair[2].wait_recv()
    merge_into(xsend.at[3], [mine(-1, 0), pbuf.at[2, 0]])
    xc[3].start()
    xc[0].wait_recv()
    merge_into(xsend.at[4], [mine(1, 0), pbuf.at[1, 0], xrecv.at[0]])
    xc[4].start()
    xc[1].wait_recv()
    merge_into(xsend.at[5], [mine(-1, 1), pbuf.at[2, 1], xrecv.at[1]])
    xc[5].start()
    pair[3].wait_recv()
    oc = []
    for half, (near, far) in enumerate(((3, 4), (2, 5))):
        xc[near].wait_recv()
        xc[far].wait_recv()
        total, _, denom = merge([mine(0, half), pbuf.at[3, half], xrecv.at[near], xrecv.at[far]])
        o = total / column(denom)
        obuf[c, half * hr:(half + 1) * hr, :] = o.astype(BF16).astype(F32)
        oc.append(remote(obuf.at[c, pl.ds(half * hr, hr)], obuf.at[c, pl.ds(half * hr, hr)],
                         sem_os.at[half], sem_or.at[half], partner))
        oc[-1].start()
    for cp in oc:
        cp.wait_recv()
    half_seq = rows // 2
    for core in range(2):
        for h in range(heads):
            lhs[core * half_seq:(core + 1) * half_seq, h * head_dim:(h + 1) * head_dim] = (
                obuf[core, pl.ds(h, half_seq, stride=heads), :].astype(BF16))

    yc = [remote(ysend.at[i], yrecv.at[i], sem_ys.at[i], sem_yr.at[i], y_dev(1 if i in (0, 2, 4) else -1))
          for i in range(6)]

    def product(k):
        w_copies[k].wait()
        return jnp.dot(lhs[...], wbuf[k], preferred_element_type=F32)

    far_part = product(0)
    ysend[0] = far_part[:, :hc]
    ysend[1] = far_part[:, hc:]
    yc[0].start()
    yc[1].start()
    right_part = product(1)
    ysend[2] = right_part[:, hc:]
    ysend[4] = right_part[:, :hc]
    yc[2].start()
    left_part = product(2)
    ysend[3] = left_part[:, :hc]
    ysend[5] = left_part[:, hc:]
    yc[3].start()
    yc[0].wait_recv()
    ysend[4] = ysend[4] + yrecv[0]
    yc[4].start()
    yc[1].wait_recv()
    ysend[5] = ysend[5] + yrecv[1]
    yc[5].start()
    own_part = product(3)
    hid_copy.wait()

    f = x + c * (y - x)
    s = y + c * (x - y)

    def f_dev(d):
        return to((y + c * d) % ny, ((x + (1 - c) * d) % nx) * 2 + c)

    def s_dev(d):
        return to((y + (1 - c) * d) % ny, ((x + c * d) % nx) * 2 + c)

    def slot(fd, sd, half):
        return gbuf.at[c, (f + fd) % nx, (s + sd) % ny, half]

    def d2d(fd, sd, half):
        i = ((fd % nx) * ny + (sd % ny)) * 2 + half
        return remote(slot(fd, sd, half), slot(fd, sd, half), sem_ds.at[i], sem_dr.at[i], partner)

    def f_copy(fd, half, direction):
        i = ((fd % nx) * 2 + half) * 2 + (direction > 0)
        return remote(slot(fd, 0, half), slot(fd, 0, half), sem_fs.at[i], sem_fr.at[i], f_dev(direction))

    def f_arrival(fd, half, direction):
        i = (((fd + direction) % nx) * 2 + half) * 2 + (direction > 0)
        return remote(slot(fd, 0, half), slot(fd, 0, half), sem_fs.at[i], sem_fr.at[i], f_dev(direction))

    def s_index(fd, sd, half, direction):
        return (((fd % nx) * ny + (sd % ny)) * 2 + half) * 2 + (direction > 0)

    def s_copy(fd, sd, half, direction):
        i = s_index(fd, sd, half, direction)
        return remote(slot(fd, sd, half), slot(fd, sd, half), sem_ss.at[i], sem_sr.at[i], s_dev(direction))

    started = []

    def go(copy):
        copy.start()
        started.append(copy)

    for half, (near, far) in enumerate(((3, 4), (2, 5))):
        yc[near].wait_recv()
        yc[far].wait_recv()
        mid = own_part[:, half * hc:(half + 1) * hc] + yrecv[near] + yrecv[far]
        val = hblk[:, half * hc:(half + 1) * hc].astype(F32) + mid
        gbuf[c, f, s, half] = val.astype(BF16).astype(F32)
        for direction in (1, -1):
            go(f_copy(0, half, direction))
            go(s_copy(0, 0, half, direction))
        go(d2d(0, 0, half))

    def f_wait(fd, half, direction):
        i = (((fd + direction) % nx) * 2 + half) * 2 + (direction > 0)
        remote(slot(fd, 0, half), slot(fd, 0, half), sem_fs.at[i], sem_fr.at[i], f_dev(direction)).wait_recv()

    def s_wait(fd, sd, half, direction):
        i = s_index(fd, sd + direction, half, direction)
        remote(slot(fd, sd, half), slot(fd, sd, half), sem_ss.at[i], sem_sr.at[i], s_dev(direction)).wait_recv()

    def spread(fd, half):
        for direction in (1, -1):
            go(s_copy(fd, 0, half, direction))
        go(d2d(fd, 0, half))

    def ring(fd):
        for half, sd in ((0, -1), (1, 1)):
            s_wait(fd, sd, half, -sd)
            go(s_copy(fd, sd, half, -sd))
            go(d2d(fd, sd, half))
        for half, sd in ((1, -1), (0, 1)):
            s_wait(fd, sd, half, -sd)
            go(d2d(fd, sd, half))

    def ring_end(fd):
        for half, direction in ((0, 1), (1, -1)):
            s_wait(fd, 2, half, direction)
            go(d2d(fd, 2, half))

    def place(core, fd, sd):
        fi = (f + fd) % nx
        si = (s + sd) % ny
        if core is None:
            xi, yi, ci = fi + c * (si - fi), si + c * (fi - si), c
        else:
            xi, yi, ci = si + c * (fi - si), fi + c * (si - fi), 1 - c
        first = ci * (d_model // 2) + yi * cols
        for half in range(2):
            out_ref[pl.ds(pl.multiple_of(xi * rows, rows), rows),
                    pl.ds(pl.multiple_of(first + half * hc, 128), hc)] = gbuf[ci, fi, si, half].astype(BF16)

    f_wait(-1, 0, 1)
    go(f_copy(-1, 0, 1))
    spread(-1, 0)
    f_wait(1, 1, -1)
    go(f_copy(1, 1, -1))
    spread(1, 1)
    f_wait(-1, 1, 1)
    spread(-1, 1)
    f_wait(1, 0, -1)
    spread(1, 0)
    place(None, 0, 0)
    ring(0)
    place(None, -1, 0)
    place(None, 1, 0)
    f_wait(2, 0, 1)
    spread(2, 0)
    f_wait(2, 1, -1)
    spread(2, 1)
    place(None, 0, -1)
    place(None, 0, 1)
    ring(-1)
    place(None, 2, 0)
    ring(1)
    ring_end(0)
    place(None, -1, -1)
    place(None, -1, 1)
    place(None, 1, -1)
    place(None, 1, 1)
    place(None, 0, 2)
    ring(2)
    ring_end(-1)
    place(None, 2, -1)
    place(None, 2, 1)
    place(None, -1, 2)
    ring_end(1)
    place(None, 1, 2)
    ring_end(2)
    place(None, 2, 2)

    def d2d_wait(fd, sd, half):
        i = ((fd % nx) * ny + (sd % ny)) * 2 + half
        there = gbuf.at[1 - c, (s + fd) % nx, (f + sd) % ny, half]
        remote(there, there, sem_ds.at[i], sem_dr.at[i], partner).wait_recv()

    def place_other(fd, sd):
        fi, si = (s + fd) % nx, (f + sd) % ny
        ci = 1 - c
        xi = si + c * (fi - si)
        yi = fi + c * (si - fi)
        first = ci * (d_model // 2) + yi * cols
        for half in range(2):
            out_ref[pl.ds(pl.multiple_of(xi * rows, rows), rows),
                    pl.ds(pl.multiple_of(first + half * hc, 128), hc)] = gbuf[ci, fi, si, half].astype(BF16)

    for fd, sd in ((0, 0), (-1, 0), (1, 0), (0, -1), (0, 1), (2, 0), (-1, -1), (-1, 1), (1, -1), (1, 1), (0, 2),
                   (2, -1), (2, 1), (-1, 2), (1, 2), (2, 2)):
        for half in range(2):
            d2d_wait(fd, sd, half)
        place_other(fd, sd)

    for cp in pair + xc + oc + yc + started:
        cp.wait_send()


def solution(mesh):
    cache_spec = P('dp', 'sp', 'tp', None)
    sp = mesh.shape['sp']
    tp = mesh.shape['tp']

    def local_step(hidden, lengths, k_cache, v_cache, norm_gain, w_query, w_key, w_value, w_out):
        batch, seq_block, kv, head_dim = k_cache.shape
        d_model = hidden.shape[1]
        heads = w_query.shape[1] // head_dim
        group = heads // kv
        dims = (batch, d_model, heads, kv, group, head_dim, seq_block, sp)
        hr = (batch // sp) * heads // 2
        n_w = w_query.shape[1] // 256 + 2
        flat = batch * seq_block
        anyspec = pl.BlockSpec(memory_space=pl.ANY)
        vspec = pl.BlockSpec(memory_space=pltpu.VMEM)
        dma = pltpu.SemaphoreType.DMA

        acc, k_new, v_new = pl.pallas_call(
            functools.partial(attention_kernel, dims),
            out_shape=(jax.ShapeDtypeStruct((2 * sp, hr + 8, 128), F32),
                       jax.ShapeDtypeStruct((flat, kv, head_dim), BF16),
                       jax.ShapeDtypeStruct((flat, kv, head_dim), BF16)),
            in_specs=[pl.BlockSpec(memory_space=pltpu.SMEM), anyspec, vspec] + [anyspec] * 5,
            out_specs=(vspec, anyspec, anyspec),
            scratch_shapes=[
                pltpu.VMEM((batch, d_model), BF16),
                pltpu.VMEM((batch, d_model), BF16),
                pltpu.VMEM((n_w, d_model, 256), BF16),
                pltpu.VMEM((flat + 8, kv, head_dim), BF16),
                pltpu.VMEM((flat + 8, kv, head_dim), BF16),
                pltpu.VMEM((batch * heads, head_dim), F32),
                pltpu.VMEM((batch * kv, head_dim), F32),
                pltpu.VMEM((batch * kv, head_dim), F32),
                dma((4,)), dma((n_w,)), dma((sp,)), dma((sp,)), dma((sp,)), dma((sp,)),
            ],
            compiler_params=pltpu.CompilerParams(vmem_limit_bytes=50 * MIB),
            name='local_attention',
        )(lengths, hidden, norm_gain.reshape(1, d_model), w_query, w_key, w_value,
          k_cache.reshape(flat, kv, head_dim), v_cache.reshape(flat, kv, head_dim))

        nx = sp // 2
        rows = batch // nx
        cols = d_model // (2 * tp)
        n_blocks = nx * tp
        out = pl.pallas_call(
            functools.partial(exchange_kernel, dims),
            out_shape=jax.ShapeDtypeStruct((batch, d_model), BF16),
            in_specs=[vspec, anyspec, anyspec],
            out_specs=vspec,
            scratch_shapes=[
                pltpu.VMEM((4, 2, hr + 8, 128), F32),
                pltpu.VMEM((6, hr + 8, 128), F32),
                pltpu.VMEM((6, hr + 8, 128), F32),
                pltpu.VMEM((2, 2 * hr, 128), F32),
                pltpu.VMEM((rows, heads * head_dim), BF16),
                pltpu.VMEM((4, heads * head_dim, cols), BF16),
                pltpu.VMEM((6, rows, cols // 2), F32),
                pltpu.VMEM((6, rows, cols // 2), F32),
                pltpu.VMEM((rows, cols), BF16),
                pltpu.VMEM((2, nx, tp, 2, rows, cols // 2), F32),
                dma((4,)), dma, dma((4,)), dma((4,)), dma((6,)), dma((6,)), dma((2,)), dma((2,)), dma((6,)), dma((6,)),
                dma((nx * 4,)), dma((nx * 4,)), dma((n_blocks * 4,)), dma((n_blocks * 4,)),
                dma((n_blocks * 2,)), dma((n_blocks * 2,)),
            ],
            compiler_params=pltpu.CompilerParams(collective_id=0, has_side_effects=True, vmem_limit_bytes=40 * MIB),
            name='exchange',
        )(acc, hidden, w_out)
        return out, k_new.reshape(k_cache.shape), v_new.reshape(v_cache.shape)

    return jax.shard_map(
        local_step,
        mesh=mesh,
        in_specs=(P('dp', None), P('dp'), cache_spec, cache_spec, P(None), P(None, 'tp'), P(None, 'tp'), P(None, 'tp'), P('tp', None)),
        out_specs=(P('dp', None), cache_spec, cache_spec),
        check_vma=False,
    )
```

```python
import functools
import math

import jax
import jax.numpy as jnp
from jax import lax
from jax.experimental import pallas as pl
from jax.experimental.pallas import tpu as pltpu
from jax.sharding import PartitionSpec as P

EPS = 1e-6
NEG_BIG = -1e30
FLOOR = -0.999e30
LOG2E = math.log2(math.e)
MIB = 1 << 20
VMEM_MIB = 52
F32 = jnp.float32
BF16 = jnp.bfloat16
LANES = 128
SUB = 8
BLOCK = 256
GROUP = 4
SPLITS = 2
PIECES = 16
HID = 4
FAR, RIGHT, OWN, LEFT = range(4)
SLOTS = 6
ROUTES = 4
N_INPUTS, N_OUTS, N_PROJECT = 8, 3, 12
STAT = SUB


def remote(src, dst, ssem, rsem, dev):
    return pltpu.make_async_remote_copy(src_ref=src, dst_ref=dst, send_sem=ssem, recv_sem=rsem,
                                        device_id=dev, device_id_type=pl.DeviceIdType.MESH)


def meet(peers):
    barrier = pltpu.get_barrier_semaphore()
    for dev in peers:
        pl.semaphore_signal(barrier, inc=1, device_id=dev, device_id_type=pl.DeviceIdType.MESH)
    return barrier


def iota(shape, dim):
    return lax.broadcasted_iota(jnp.int32, shape, dim)


def project(seq_block, kv, enter, len_hbm, hid_hbm, gain_hbm, wq_hbm, wk_hbm, wv_hbm, kc_hbm, vc_hbm,
            kbuf, vbuf, kvq, len_ref, hbuf, gain_raw, gain_ref, nbuf, wbuf,
            sem_l, sem_g, sem_h, sem_w, sem_k, sem_v, sem_s, sem_r):
    batch, d_model = hid_hbm.shape
    n_w = wbuf.shape[0]
    spi, y = lax.axis_index('sp'), lax.axis_index('tp')
    c = spi % 2
    partner = {'tp': y, 'sp': spi + 1 - 2 * c}
    base = spi * seq_block
    rows_h = batch // HID
    seq_rows = seq_block * kv
    per_piece = batch // PIECES
    crow = per_piece * seq_rows

    hid_copies = [pltpu.make_async_copy(hid_hbm.at[pl.ds(i * rows_h, rows_h)], hbuf.at[pl.ds(i * rows_h, rows_h)], sem_h.at[i])
                  for i in range(HID)]
    len_copy = pltpu.make_async_copy(len_hbm, len_ref, sem_l)
    gain_copy = pltpu.make_async_copy(gain_hbm, gain_raw, sem_g)

    def w_copy(j, src, first):
        return pltpu.make_async_copy(src.at[:, pl.ds(first, BLOCK)], wbuf.at[j], sem_w.at[j])

    def q_copy(j):
        return w_copy(j, wq_hbm, pl.multiple_of(c * (n_w - 1) * BLOCK + (j - 1) * BLOCK, BLOCK))

    def cache_copies(p):
        part = pl.ds(pl.multiple_of(p * crow, crow), crow)
        return [pltpu.make_async_copy(src.at[part], buf.at[part], sem.at[p])
                for src, buf, sem in ((kc_hbm, kbuf, sem_k), (vc_hbm, vbuf, sem_v))]

    def trade(j):
        slot = kvq.at[c * n_w + j]
        return remote(slot, slot, sem_s.at[j], sem_r.at[j], partner)

    def arrival(j):
        slot = kvq.at[(1 - c) * n_w + j]
        return remote(slot, slot, sem_s.at[j], sem_r.at[j], partner)

    for cp in hid_copies + [gain_copy]:
        cp.start()

    @pl.when(c == 0)
    def _():
        w_copy(0, wk_hbm, 0).start()

    @pl.when(c == 1)
    def _():
        w_copy(0, wv_hbm, 0).start()

    q_copy(1).start()
    len_copy.start()

    step = 2 * SUB
    wide = SUB * LANES

    def norm_rows(r, carry):
        row = pl.ds(pl.multiple_of(r * step, step), step)
        cuts = [slice(w, w + wide) for w in range(0, d_model, wide)]
        total = jnp.zeros((step, 1), F32)
        for cut in cuts:
            v = hbuf[row, cut].astype(F32)
            total = total + jnp.sum(v * v, axis=1, keepdims=True)
        inv = lax.rsqrt(total / d_model + EPS)
        for cut in cuts:
            nbuf[row, cut] = (hbuf[row, cut].astype(F32) * inv * gain_ref[:, cut]).astype(BF16)
        return carry

    gain_copy.wait()
    gain_ref[...] = gain_raw[...].astype(F32).reshape(gain_ref.shape)
    for i in range(HID):
        hid_copies[i].wait()
        if i % 2:
            q_copy(2 + i // 2).start()
        lax.fori_loop(i * rows_h // step, (i + 1) * rows_h // step, norm_rows, 0)
    enter()

    per_step = PIECES // n_w

    def columns(j, carry):
        w_copy(j, wk_hbm, 0).wait()
        for i in range(per_step):
            for cp in cache_copies(j * per_step + i):
                cp.start()

        @pl.when(j > 0)
        def _():
            trade(j - 1).start()

        res = jnp.dot(nbuf[...], wbuf[j], preferred_element_type=F32)
        for i in range(BLOCK // LANES):
            kvq[c * n_w + j, pl.ds(i, batch, stride=BLOCK // LANES), :] = res[:, i * LANES:(i + 1) * LANES]
        return carry

    lax.fori_loop(0, n_w, columns, 0)
    trade(n_w - 1).start()
    len_copy.wait()
    arrival(0).wait_recv()

    pair_row = iota((step, LANES), 0) % kv
    slot_pos = iota((seq_rows, LANES), 0) // kv

    def update(p, carry):
        for cp in cache_copies(p):
            cp.wait()
        for i in range(per_piece):
            b = p * per_piece + i
            here = slot_pos == len_ref[b] - base
            rows = pl.ds(pl.multiple_of(b * seq_rows, step), seq_rows)
            for core, buf in enumerate((kbuf, vbuf)):
                new = kvq[core * n_w, pl.ds(b * kv, 1), :]
                for n in range(1, kv):
                    new = jnp.where(pair_row == n, kvq[core * n_w, pl.ds(b * kv + n, 1), :], new)
                new = jnp.concatenate([new.astype(BF16)] * (seq_rows // step), axis=0)
                buf[rows, :] = jnp.where(here, new, buf[rows, :])
        return carry

    lax.fori_loop(0, PIECES, update, 0)
    for j in range(1, n_w):
        arrival(j).wait_recv()
    for j in range(n_w):
        trade(j).wait_send()


def decode_kernel(seq_block, kv, heads, *refs):
    inputs, wo_hbm, outs = refs[:N_INPUTS], refs[N_INPUTS], refs[N_INPUTS + 1:N_INPUTS + N_OUTS + 1]
    kvq, len_ref, hbuf, *rest = refs[N_INPUTS + N_OUTS + 1:]
    kbuf, vbuf, out_ref = outs

    def first(enter):
        project(seq_block, kv, enter, *inputs, kbuf, vbuf, kvq, len_ref, hbuf, *rest[:N_PROJECT])

    exchange(seq_block, kv, heads, first, kbuf, vbuf, kvq, len_ref, hbuf, wo_hbm, out_ref, *rest[N_PROJECT:])


def exchange(seq_block, kv, heads, first_part, kbuf, vbuf, kvq, len_ref, hbuf, wo_hbm, out_ref,
             acc, pbuf, xsend, xrecv, obuf, lhs, wbuf, ysend, yrecv, gbuf,
             sem_w, sem_ps, sem_pr, sem_xs, sem_xr, sem_os, sem_or, sem_ys, sem_yr,
             sem_fs, sem_fr, sem_ss, sem_sr, sem_ds, sem_dr):
    batch, d_model = out_ref.shape
    spi, y = lax.axis_index('sp'), lax.axis_index('tp')
    sp, ny = lax.axis_size('sp'), lax.axis_size('tp')
    nx = sp // 2
    x, c = spi // 2, spi % 2
    base = spi * seq_block
    seq_rows = seq_block * kv
    n_w = kvq.shape[0] // 2
    unit = batch // (sp * SPLITS * 2)
    ur = unit * heads
    rows = batch // nx
    part = rows // (2 * SPLITS)
    half_d = d_model // 2
    cols = half_d // ny
    hc = cols // 2

    def at_x(d):
        return (x + d + nx) % nx

    def at_y(d):
        return (y + d + ny) % ny

    partner = {'tp': y, 'sp': spi + 1 - 2 * c}
    x_dev = {d: {'tp': y, 'sp': at_x(d) * 2 + c} for d in (1, -1)}
    y_dev = {d: {'tp': at_y(d), 'sp': spi} for d in (1, -1)}

    barrier = meet([partner, *x_dev.values(), *y_dev.values()])
    w_copies = []
    for k in range(ROUTES):
        first = pl.multiple_of(c * half_d + at_y(2 - k) * cols, LANES)
        w_copies.append(pltpu.make_async_copy(wo_hbm.at[:, pl.ds(first, cols)], wbuf.at[k], sem_w.at[k]))
    first_part(lambda: pl.semaphore_wait(barrier, 1 + len(x_dev) + len(y_dev)))
    for cp in w_copies:
        cp.start()

    per = BLOCK // LANES
    tile = GROUP * per
    n_tiles = heads // per
    qrows = GROUP * heads
    krows = GROUP * seq_rows
    row_id, col_id = iota((qrows, krows), 0), iota((qrows, krows), 1)
    same = (row_id % tile // per == col_id // seq_rows) & (row_id // (qrows // kv) == col_id % kv)
    col_row = iota((1, krows), 1)
    col_seq = col_row // seq_rows
    col_pos = col_row % seq_rows // kv
    diag = iota((ur, LANES), 0) == iota((ur, LANES), 1)
    fold = LANES ** -0.5 * LOG2E
    halves = [(core, h) for core in range(2) for h in range(2)]
    groups = [(core, h, g) for core, h in halves for g in range(unit // GROUP)]

    def pair(k, n):
        return remote(acc.at[n, k, 1 - c], pbuf.at[n, k], sem_ps.at[n * ROUTES + k], sem_pr.at[n * ROUTES + k], partner)

    def attend(n):
        def one(k, carry):
            dest = at_x(2 - k)

            def first(core, h, g):
                return (((dest * 2 + core) * SPLITS + n) * 2 + h) * unit + g * GROUP

            scores = []
            for where in groups:
                b0 = first(*where)
                rows8 = pl.ds(pl.multiple_of(b0 * per, tile), tile)
                q = jnp.concatenate([kvq[core * n_w + j, rows8, :] for core in range(2) for j in range(1, n_w)], axis=0)
                keys = kbuf[pl.ds(pl.multiple_of(b0 * seq_rows, krows), krows), :]
                s = lax.dot_general(q.astype(BF16), keys, (((1,), (1,)), ((), ())), preferred_element_type=F32)
                last = jnp.full((1, krows), len_ref[b0] - base, jnp.int32)
                for i in range(1, GROUP):
                    last = jnp.where(col_seq == i, len_ref[b0 + i] - base, last)
                scores.append(jnp.where(same & (col_pos <= last), s * fold, NEG_BIG))
            peaks = [jnp.maximum(jnp.max(s, axis=1, keepdims=True), FLOOR) for s in scores]
            exps = [jnp.exp2(s - m) for s, m in zip(scores, peaks)]
            sums = [jnp.sum(e, axis=1, keepdims=True) for e in exps]
            for where, e in zip(groups, exps):
                core, h, g = where
                values = vbuf[pl.ds(pl.multiple_of(first(*where) * seq_rows, krows), krows), :]
                o = jnp.dot(e.astype(BF16), values, preferred_element_type=F32)
                for t in range(n_tiles):
                    at = (t * (unit // GROUP) + g) * tile
                    acc[n, k, core, h, at:at + tile, :] = o[t * tile:(t + 1) * tile]
            for core, h in halves:
                packed = []
                for stat in (peaks, sums):
                    mine = [s for where, s in zip(groups, stat) if where[:2] == (core, h)]
                    col = jnp.concatenate([s[t * tile:(t + 1) * tile] for t in range(n_tiles) for s in mine], axis=0)
                    spread = jnp.where(diag, jnp.broadcast_to(col, diag.shape), 0.0)
                    packed.append(jnp.sum(spread, axis=0, keepdims=True))
                packed.append(jnp.zeros((STAT - len(packed), LANES), F32))
                acc[n, k, core, h, ur:ur + STAT, :] = jnp.concatenate(packed, axis=0)

            pair(k, n).start()
            return carry

        lax.fori_loop(0, ROUTES, one, 0)

    def column(stat):
        return jnp.sum(jnp.where(diag, jnp.broadcast_to(stat, diag.shape), 0.0), axis=1, keepdims=True)

    def merge(refs):
        both = [(r[ur:ur + 1, :], r[ur + 1:ur + 2, :]) for r in refs]
        peak = functools.reduce(jnp.maximum, [m for m, _ in both])
        scale = [jnp.exp2(m - peak) for m, _ in both]
        denom = sum(l * s for (_, l), s in zip(both, scale))
        total = sum(r[:ur, :] * column(s) for r, s in zip(refs, scale))
        return total, peak, denom

    def merge_into(dst, refs):
        total, peak, denom = merge(refs)
        dst[:ur, :] = total
        dst[ur:ur + STAT, :] = jnp.concatenate([peak, denom, jnp.zeros((STAT - 2, LANES), F32)], axis=0)

    FAR0, FAR1, RAW_R, RAW_L, SUM_R, SUM_L = range(SLOTS)
    ends = ((RAW_L, SUM_R), (RAW_R, SUM_L))

    def ring_copies(send, recv, ssem, rsem, devs):
        return [[remote(send.at[n, i], recv.at[n, i], ssem.at[n * SLOTS + i], rsem.at[n * SLOTS + i],
                        devs[1 if i in (FAR0, RAW_R, SUM_R) else -1]) for i in range(SLOTS)] for n in range(SPLITS)]

    xc = ring_copies(xsend, xrecv, sem_xs, sem_xr, x_dev)
    yc = ring_copies(ysend, yrecv, sem_ys, sem_yr, y_dev)
    oc = [remote(obuf.at[n, c], obuf.at[n, c], sem_os.at[n], sem_or.at[n], partner) for n in range(SPLITS)]

    def both(n, k, h):
        return [acc.at[n, k, c, h], pbuf.at[n, k, h]]

    def x_start(n):
        for k, todo in ((FAR, ((FAR0, 0), (FAR1, 1))), (RIGHT, ((RAW_R, 1),)), (LEFT, ((RAW_L, 0),))):
            pair(k, n).wait_recv()
            for slot, h in todo:
                merge_into(xsend.at[n, slot], both(n, k, h))
                xc[n][slot].start()

    def x_pass(n):
        for came, slot, k, h in ((FAR0, SUM_R, RIGHT, 0), (FAR1, SUM_L, LEFT, 1)):
            xc[n][came].wait_recv()
            merge_into(xsend.at[n, slot], both(n, k, h) + [xrecv.at[n, came]])
            xc[n][slot].start()

    def x_end(n):
        pair(OWN, n).wait_recv()
        for h, came in enumerate(ends):
            for slot in came:
                xc[n][slot].wait_recv()
            total, _, denom = merge(both(n, OWN, h) + [xrecv.at[n, slot] for slot in came])
            obuf[n, c, h * ur:(h + 1) * ur, :] = (total / column(denom)).astype(BF16).astype(F32)
        oc[n].start()

    def y_start(n):
        oc[n].wait_recv()
        for core, h in halves:
            at = core * part + h * unit
            for t in range(n_tiles):
                for i in range(per):
                    head = (t * per + i) * LANES
                    lhs[n, at:at + unit, head:head + LANES] = obuf[
                        n, core, pl.ds(h * ur + t * unit * per + i, unit, stride=per), :]
        for k, first, second in ((FAR, FAR0, FAR1), (RIGHT, SUM_R, RAW_R), (LEFT, RAW_L, SUM_L)):
            if n == 0:
                w_copies[k].wait()
            prod = product(n, k)
            ysend[n, first] = prod[:, :hc]
            ysend[n, second] = prod[:, hc:]
            for slot in (first, second):
                if slot not in (SUM_R, SUM_L):
                    yc[n][slot].start()

    def product(n, k):
        return jnp.dot(lhs[n].astype(BF16), wbuf[k], preferred_element_type=F32)

    def y_pass(n):
        for came, slot in ((FAR0, SUM_R), (FAR1, SUM_L)):
            yc[n][came].wait_recv()
            ysend[n, slot] = ysend[n, slot] + yrecv[n, came]
            yc[n][slot].start()

    f = x + c * (y - x)
    s = y + c * (x - y)
    sent = []

    def go(copy):
        copy.start()
        sent.append(copy)

    def f_dev(d):
        return {'tp': (y + c * d + ny) % ny, 'sp': ((x + (1 - c) * d + nx) % nx) * 2 + c}

    def s_dev(d):
        return {'tp': (y + (1 - c) * d + ny) % ny, 'sp': ((x + c * d + nx) % nx) * 2 + c}

    def block(n, fd, sd):
        return gbuf.at[n, c, (f + fd + nx) % nx, (s + sd + ny) % ny]

    def kind(d, is_half):
        return is_half * 2 + (d > 0)

    def along(ring, n, fd, sd, d, is_half=False):
        ref = block(n, fd, sd)
        if is_half:
            ref = ref.at[0 if d > 0 else 1]
        if ring == 'f':
            i = n * ROUTES + kind(d, is_half)
            return remote(ref, ref, sem_fs.at[i], sem_fr.at[i], f_dev(d))
        i = (n * nx + fd % nx) * ROUTES + kind(d, is_half)
        return remote(ref, ref, sem_ss.at[i], sem_sr.at[i], s_dev(d))

    def over(n, fd, sd):
        i = (n * nx + fd % nx) * ny + sd % ny
        ref = block(n, fd, sd)
        return remote(ref, ref, sem_ds.at[i], sem_dr.at[i], partner)

    def place(n, ci, fi, si, swap):
        xi, yi = fi + swap * (si - fi), si + swap * (fi - si)
        for h in range(2):
            at = pl.ds(pl.multiple_of(ci * half_d + yi * cols + h * hc, LANES), hc)
            for core in range(2):
                first = pl.multiple_of(xi * rows + (core * SPLITS + n) * part, part)
                out_ref[pl.ds(first, part), at] = gbuf[n, ci, fi, si, h, core * part:(core + 1) * part, :].astype(BF16)

    def place_here(n, fd, sd):
        place(n, c, (f + fd + nx) % nx, (s + sd + ny) % ny, c)

    def spread(n, fd):
        for d in (1, -1):
            go(along('s', n, fd, 0, d))
        go(over(n, fd, 0))

    def y_end(n):
        if n == 0:
            w_copies[OWN].wait()
        own = product(n, OWN)
        for h, came in enumerate(ends):
            for slot in came:
                yc[n][slot].wait_recv()
            total = own[:, h * hc:(h + 1) * hc] + yrecv[n, came[0]] + yrecv[n, came[1]]
            at = pl.ds(pl.multiple_of(c * half_d + y * cols + h * hc, LANES), hc)
            kept = jnp.concatenate([hbuf[pl.ds(pl.multiple_of(x * rows + (core * SPLITS + n) * part, part), part), at]
                                    for core in range(2)], axis=0)
            gbuf[n, c, f, s, h] = (kept.astype(F32) + total).astype(BF16).astype(F32)
        for d in (1, -1):
            go(along('f', n, 0, 0, d))
        spread(n, 0)
        place_here(n, 0, 0)

    def pass_on(ring, n, fd, sd, d):
        along(ring, n, fd, sd, d).wait_recv()
        go(along(ring, n, fd, sd, d, True))

    def f_ring(n):
        for d in (1, -1):
            pass_on('f', n, -d, 0, d)
            spread(n, -d)
        for d in (1, -1):
            place_here(n, -d, 0)

    def f_end(n):
        for d in (1, -1):
            along('f', n, 2, 0, d, True).wait_recv()
        spread(n, 2)
        place_here(n, 2, 0)

    def s_ring(n, fd):
        for d in (1, -1):
            pass_on('s', n, fd, -d, d)
            go(over(n, fd, -d))
        for d in (1, -1):
            place_here(n, fd, -d)

    def s_end(n, fd):
        for d in (1, -1):
            along('s', n, fd, 2, d, True).wait_recv()
        go(over(n, fd, 2))
        place_here(n, fd, 2)

    def take(n, fd, sd):
        i = (n * nx + fd % nx) * ny + sd % ny
        fi, si = (s + fd + nx) % nx, (f + sd + ny) % ny
        ref = gbuf.at[n, 1 - c, fi, si]
        remote(ref, ref, sem_ds.at[i], sem_dr.at[i], partner).wait_recv()
        place(n, 1 - c, fi, si, 1 - c)

    def stage(n, i):
        if i == 0:
            f_ring(n)
            s_ring(n, 0)
        elif i == 1:
            f_end(n)
            s_ring(n, -1)
            s_ring(n, 1)
            s_end(n, 0)
        elif i == 2:
            for fd in (0, -1, 1):
                take(n, fd, 0)
            s_ring(n, 2)
            s_end(n, -1)
            s_end(n, 1)
        else:
            for fd, sd in ((2, 0), (0, -1), (0, 1), (0, 2), (-1, -1), (-1, 1), (1, -1), (1, 1)):
                take(n, fd, sd)
            s_end(n, 2)

    attend(0)
    x_start(0)
    attend(1)
    x_pass(0)
    x_start(1)
    x_end(0)
    x_pass(1)
    y_start(0)
    x_end(1)
    y_pass(0)
    y_start(1)
    y_end(0)
    y_pass(1)
    y_end(1)
    for i in range(ROUTES):
        for n in range(SPLITS):
            stage(n, i)
    for n in range(SPLITS):
        for fd, sd in ((2, -1), (2, 1), (-1, 2), (1, 2), (2, 2)):
            take(n, fd, sd)
    for n in range(SPLITS):
        for k in range(ROUTES):
            pair(k, n).wait_send()
    for cp in xc + yc:
        for one in cp:
            one.wait_send()
    for cp in oc + sent:
        cp.wait_send()


def solution(mesh):
    cache_spec = P('dp', 'sp', 'tp', None)
    sp = mesh.shape['sp']
    tp = mesh.shape['tp']

    def local_step(hidden, lengths, k_cache, v_cache, norm_gain, w_query, w_key, w_value, w_out):
        batch, seq_block, kv, head_dim = k_cache.shape
        d_model = hidden.shape[1]
        width = w_query.shape[1]
        heads = width // head_dim
        n_w = width // (2 * BLOCK) + 1
        flat = batch * seq_block * kv
        hbm = pl.BlockSpec(memory_space=pltpu.HBM)
        vmem = pl.BlockSpec(memory_space=pltpu.VMEM)
        shape = jax.ShapeDtypeStruct
        buf = pltpu.VMEM

        def dma(*shapes):
            return [pltpu.SemaphoreType.DMA(s) if s else pltpu.SemaphoreType.DMA for s in shapes]

        nx = sp // 2
        rows = batch // nx
        cols = d_model // (2 * tp)
        ur = batch // (sp * SPLITS * 2) * heads
        travel = buf((SPLITS, SLOTS, ur + STAT, head_dim), F32)
        yblock = buf((SPLITS, SLOTS, rows // SPLITS, cols // 2), F32)
        n_x, n_f = SPLITS * SLOTS, SPLITS * ROUTES
        n_s = n_f * nx
        n_d = SPLITS * nx * tp
        k_new, v_new, out = pl.pallas_call(
            functools.partial(decode_kernel, seq_block, kv, heads),
            out_shape=(buf((flat, head_dim), BF16), buf((flat, head_dim), BF16), buf((batch, d_model), BF16)),
            in_specs=[hbm] * (N_INPUTS + 1),
            out_specs=(vmem, vmem, vmem),
            scratch_shapes=[
                buf((2 * n_w, batch * BLOCK // head_dim, head_dim), F32),
                pltpu.SMEM((batch,), jnp.int32),
                buf((batch, d_model), BF16),
                buf((d_model,), BF16),
                buf((1, d_model), F32),
                buf((batch, d_model), BF16),
                buf((n_w, d_model, BLOCK), BF16),
                *dma((), (), (HID,), (n_w,), (PIECES,), (PIECES,), (n_w,), (n_w,)),
                buf((SPLITS, ROUTES, 2, 2, ur + STAT, head_dim), F32),
                buf((SPLITS, ROUTES, 2, ur + STAT, head_dim), F32),
                travel, travel,
                buf((SPLITS, 2, 2 * ur, head_dim), F32),
                buf((SPLITS, rows // SPLITS, width), F32),
                buf((ROUTES, width, cols), BF16),
                yblock, yblock,
                buf((SPLITS, 2, nx, tp, 2, rows // SPLITS, cols // 2), F32),
                *dma((ROUTES,), (n_f,), (n_f,), (n_x,), (n_x,), (SPLITS,), (SPLITS,), (n_x,), (n_x,),
                     (n_f,), (n_f,), (n_s,), (n_s,), (n_d,), (n_d,)),
            ],
            compiler_params=pltpu.CompilerParams(collective_id=0, has_side_effects=True, vmem_limit_bytes=VMEM_MIB * MIB),
            name='decode_step',
        )(lengths, hidden, norm_gain, w_query, w_key, w_value,
          k_cache.reshape(flat, head_dim), v_cache.reshape(flat, head_dim), w_out)
        return out, k_new.reshape(k_cache.shape), v_new.reshape(v_cache.shape)

    return jax.shard_map(
        local_step,
        mesh=mesh,
        in_specs=(P('dp', None), P('dp'), cache_spec, cache_spec, P(None), P(None, 'tp'), P(None, 'tp'), P(None, 'tp'), P('tp', None)),
        out_specs=(P('dp', None), cache_spec, cache_spec),
        check_vma=False,
    )
```

```python
import functools
import math

import jax
import jax.numpy as jnp
from jax import lax
from jax.experimental import pallas as pl
from jax.experimental.pallas import tpu as pltpu
from jax.sharding import PartitionSpec as P

EPS = 1e-6
NEG_BIG = -1e30
FLOOR = -0.999e30
LOG2E = math.log2(math.e)
MIB = 1 << 20
VMEM_MIB = 52
F32 = jnp.float32
BF16 = jnp.bfloat16
LANES = 128
SUB = 8
BLOCK = 256
GROUP = 4
SPLITS = 2
PIECES = 16
HID = 4
FAR, RIGHT, OWN, LEFT = range(4)
AWAY = 3
ROUTES = 4
N_INPUTS, N_OUTS, N_PROJECT = 8, 3, 12
STAT = SUB


def remote(src, dst, ssem, rsem, dev):
    return pltpu.make_async_remote_copy(src_ref=src, dst_ref=dst, send_sem=ssem, recv_sem=rsem,
                                        device_id=dev, device_id_type=pl.DeviceIdType.MESH)


def meet(peers):
    barrier = pltpu.get_barrier_semaphore()
    for dev in peers:
        pl.semaphore_signal(barrier, inc=1, device_id=dev, device_id_type=pl.DeviceIdType.MESH)
    return barrier


def iota(shape, dim):
    return lax.broadcasted_iota(jnp.int32, shape, dim)


def project(seq_block, kv, enter, len_hbm, hid_hbm, gain_hbm, wq_hbm, wk_hbm, wv_hbm, kc_hbm, vc_hbm,
            kbuf, vbuf, kvq, len_ref, hbuf, gain_raw, gain_ref, nbuf, wbuf,
            sem_l, sem_g, sem_h, sem_w, sem_k, sem_v, sem_s, sem_r):
    batch, d_model = hid_hbm.shape
    n_w = wbuf.shape[0]
    spi, y = lax.axis_index('sp'), lax.axis_index('tp')
    c = spi % 2
    partner = {'tp': y, 'sp': spi + 1 - 2 * c}
    base = spi * seq_block
    rows_h = batch // HID
    seq_rows = seq_block * kv
    per_piece = batch // PIECES
    crow = per_piece * seq_rows

    hid_copies = [pltpu.make_async_copy(hid_hbm.at[pl.ds(i * rows_h, rows_h)], hbuf.at[pl.ds(i * rows_h, rows_h)], sem_h.at[i])
                  for i in range(HID)]
    len_copy = pltpu.make_async_copy(len_hbm, len_ref, sem_l)
    gain_copy = pltpu.make_async_copy(gain_hbm, gain_raw, sem_g)

    def w_copy(j, src, first):
        return pltpu.make_async_copy(src.at[:, pl.ds(first, BLOCK)], wbuf.at[j], sem_w.at[j])

    def q_copy(j):
        return w_copy(j, wq_hbm, pl.multiple_of(c * (n_w - 1) * BLOCK + (j - 1) * BLOCK, BLOCK))

    def cache_copies(p):
        part = pl.ds(pl.multiple_of(p * crow, crow), crow)
        return [pltpu.make_async_copy(src.at[part], buf.at[part], sem.at[p])
                for src, buf, sem in ((kc_hbm, kbuf, sem_k), (vc_hbm, vbuf, sem_v))]

    def trade(j):
        slot = kvq.at[c * n_w + j]
        return remote(slot, slot, sem_s.at[j], sem_r.at[j], partner)

    def arrival(j):
        slot = kvq.at[(1 - c) * n_w + j]
        return remote(slot, slot, sem_s.at[j], sem_r.at[j], partner)

    for cp in hid_copies + [gain_copy, len_copy]:
        cp.start()
    gain_copy.wait()
    gain_ref[...] = gain_raw[...].astype(F32).reshape(gain_ref.shape)
    hid_copies[0].wait()

    @pl.when(c == 0)
    def _():
        w_copy(0, wk_hbm, 0).start()

    @pl.when(c == 1)
    def _():
        w_copy(0, wv_hbm, 0).start()

    step = 2 * SUB
    wide = SUB * LANES

    def norm_rows(r, carry):
        row = pl.ds(pl.multiple_of(r * step, step), step)
        cuts = [slice(w, w + wide) for w in range(0, d_model, wide)]
        total = jnp.zeros((step, 1), F32)
        for cut in cuts:
            v = hbuf[row, cut].astype(F32)
            total = total + jnp.sum(v * v, axis=1, keepdims=True)
        inv = lax.rsqrt(total / d_model + EPS)
        for cut in cuts:
            nbuf[row, cut] = (hbuf[row, cut].astype(F32) * inv * gain_ref[:, cut]).astype(BF16)
        return carry

    for i in range(HID):
        if i:
            hid_copies[i].wait()
            q_copy(i).start()
        lax.fori_loop(i * rows_h // step, (i + 1) * rows_h // step, norm_rows, 0)
    enter()

    per_step = PIECES // n_w

    def columns(j, carry):
        w_copy(j, wk_hbm, 0).wait()
        for i in range(per_step):
            for cp in cache_copies(j * per_step + i):
                cp.start()

        @pl.when(j > 0)
        def _():
            trade(j - 1).start()

        res = jnp.dot(nbuf[...], wbuf[j], preferred_element_type=F32)
        for i in range(BLOCK // LANES):
            kvq[c * n_w + j, pl.ds(i, batch, stride=BLOCK // LANES), :] = res[:, i * LANES:(i + 1) * LANES]
        return carry

    lax.fori_loop(0, n_w, columns, 0)
    trade(n_w - 1).start()
    len_copy.wait()
    arrival(0).wait_recv()

    pair_row = iota((step, LANES), 0) % kv
    slot_pos = iota((seq_rows, LANES), 0) // kv

    def update(p, carry):
        for cp in cache_copies(p):
            cp.wait()
        for i in range(per_piece):
            b = p * per_piece + i
            here = slot_pos == len_ref[b] - base
            rows = pl.ds(pl.multiple_of(b * seq_rows, step), seq_rows)
            for core, buf in enumerate((kbuf, vbuf)):
                new = kvq[core * n_w, pl.ds(b * kv, 1), :]
                for n in range(1, kv):
                    new = jnp.where(pair_row == n, kvq[core * n_w, pl.ds(b * kv + n, 1), :], new)
                new = jnp.concatenate([new.astype(BF16)] * (seq_rows // step), axis=0)
                buf[rows, :] = jnp.where(here, new, buf[rows, :])
        return carry

    lax.fori_loop(0, PIECES, update, 0)
    for j in range(1, n_w):
        arrival(j).wait_recv()
    for j in range(n_w):
        trade(j).wait_send()


def store_kernel(*refs):
    copies = [pltpu.make_async_copy(refs[i], refs[N_OUTS + i], refs[-1].at[i]) for i in range(N_OUTS)]
    for cp in copies:
        cp.start()
    for cp in copies:
        cp.wait()


def decode_kernel(seq_block, kv, heads, *refs):
    inputs, wo_hbm, outs = refs[:N_INPUTS], refs[N_INPUTS], refs[N_INPUTS + 1:N_INPUTS + N_OUTS + 1]
    kvq, len_ref, hbuf, *rest = refs[N_INPUTS + N_OUTS + 1:]
    kbuf, vbuf, out_ref = outs

    def first(enter):
        project(seq_block, kv, enter, *inputs, kbuf, vbuf, kvq, len_ref, hbuf, *rest[:N_PROJECT])

    exchange(seq_block, kv, heads, first, kbuf, vbuf, kvq, len_ref, hbuf, wo_hbm, out_ref, *rest[N_PROJECT:])


def exchange(seq_block, kv, heads, first_part, kbuf, vbuf, kvq, len_ref, hbuf, wo_hbm, out_ref,
             acc, pbuf, xsend, xrecv, obuf, lhs, wbuf, ysend, yrecv, gbuf,
             sem_w, sem_ps, sem_pr, sem_xs, sem_xr, sem_os, sem_or, sem_ys, sem_yr,
             sem_fs, sem_fr, sem_ss, sem_sr, sem_ds, sem_dr):
    batch, d_model = out_ref.shape
    spi, y = lax.axis_index('sp'), lax.axis_index('tp')
    sp, ny = lax.axis_size('sp'), lax.axis_size('tp')
    nx = sp // 2
    x, c = spi // 2, spi % 2
    base = spi * seq_block
    seq_rows = seq_block * kv
    n_w = kvq.shape[0] // 2
    unit = batch // (sp * SPLITS * 2)
    ur = unit * heads
    rows = batch // nx
    part = rows // (2 * SPLITS)
    half_d = d_model // 2
    cols = half_d // ny
    hc = cols // 2

    def at_x(d):
        return (x + d + nx) % nx

    def at_y(d):
        return (y + d + ny) % ny

    partner = {'tp': y, 'sp': spi + 1 - 2 * c}
    x_dev = {d: {'tp': y, 'sp': at_x(d) * 2 + c} for d in (2, 1, -1)}
    y_dev = {d: {'tp': at_y(d), 'sp': spi} for d in (2, 1, -1)}

    barrier = meet([partner, *x_dev.values(), *y_dev.values()])
    w_copies = []
    for k in range(ROUTES):
        first = pl.multiple_of(c * half_d + at_y(2 - k) * cols, LANES)
        w_copies.append(pltpu.make_async_copy(wo_hbm.at[:, pl.ds(first, cols)], wbuf.at[k], sem_w.at[k]))
    first_part(lambda: pl.semaphore_wait(barrier, 1 + len(x_dev) + len(y_dev)))
    for cp in w_copies:
        cp.start()

    per = BLOCK // LANES
    tile = GROUP * per
    n_tiles = heads // per
    qrows = GROUP * heads
    krows = GROUP * seq_rows
    row_id, col_id = iota((qrows, krows), 0), iota((qrows, krows), 1)
    same = (row_id % tile // per == col_id // seq_rows) & (row_id // (qrows // kv) == col_id % kv)
    col_row = iota((1, krows), 1)
    col_seq = col_row // seq_rows
    col_pos = col_row % seq_rows // kv
    diag = iota((ur, LANES), 0) == iota((ur, LANES), 1)
    fold = LANES ** -0.5 * LOG2E
    halves = [(core, h) for core in range(2) for h in range(2)]
    groups = [(core, h, g) for core, h in halves for g in range(unit // GROUP)]

    def pair(k, n):
        return remote(acc.at[n, k, 1 - c], pbuf.at[n, k], sem_ps.at[n * ROUTES + k], sem_pr.at[n * ROUTES + k], partner)

    def attend(n):
        def one(k, carry):
            dest = at_x(2 - k)

            def first(core, h, g):
                return (((dest * 2 + core) * SPLITS + n) * 2 + h) * unit + g * GROUP

            scores = []
            for where in groups:
                b0 = first(*where)
                rows8 = pl.ds(pl.multiple_of(b0 * per, tile), tile)
                q = jnp.concatenate([kvq[core * n_w + j, rows8, :] for core in range(2) for j in range(1, n_w)], axis=0)
                keys = kbuf[pl.ds(pl.multiple_of(b0 * seq_rows, krows), krows), :]
                s = lax.dot_general(q.astype(BF16), keys, (((1,), (1,)), ((), ())), preferred_element_type=F32)
                last = jnp.full((1, krows), len_ref[b0] - base, jnp.int32)
                for i in range(1, GROUP):
                    last = jnp.where(col_seq == i, len_ref[b0 + i] - base, last)
                scores.append(jnp.where(same & (col_pos <= last), s * fold, NEG_BIG))
            peaks = [jnp.maximum(jnp.max(s, axis=1, keepdims=True), FLOOR) for s in scores]
            exps = [jnp.exp2(s - m) for s, m in zip(scores, peaks)]
            sums = [jnp.sum(e, axis=1, keepdims=True) for e in exps]
            for where, e in zip(groups, exps):
                core, h, g = where
                values = vbuf[pl.ds(pl.multiple_of(first(*where) * seq_rows, krows), krows), :]
                o = jnp.dot(e.astype(BF16), values, preferred_element_type=F32)
                for t in range(n_tiles):
                    at = (t * (unit // GROUP) + g) * tile
                    acc[n, k, core, h, at:at + tile, :] = o[t * tile:(t + 1) * tile]
            for core, h in halves:
                packed = []
                for stat in (peaks, sums):
                    mine = [s for where, s in zip(groups, stat) if where[:2] == (core, h)]
                    col = jnp.concatenate([s[t * tile:(t + 1) * tile] for t in range(n_tiles) for s in mine], axis=0)
                    spread = jnp.where(diag, jnp.broadcast_to(col, diag.shape), 0.0)
                    packed.append(jnp.sum(spread, axis=0, keepdims=True))
                packed.append(jnp.zeros((STAT - len(packed), LANES), F32))
                acc[n, k, core, h, ur:ur + STAT, :] = jnp.concatenate(packed, axis=0)

            pair(k, n).start()
            return carry

        lax.fori_loop(0, ROUTES, one, 0)

    def column(stat):
        return jnp.sum(jnp.where(diag, jnp.broadcast_to(stat, diag.shape), 0.0), axis=1, keepdims=True)

    def merge(refs):
        both = [(r[ur:ur + 1, :], r[ur + 1:ur + 2, :]) for r in refs]
        peak = functools.reduce(jnp.maximum, [m for m, _ in both])
        scale = [jnp.exp2(m - peak) for m, _ in both]
        denom = sum(l * s for (_, l), s in zip(both, scale))
        total = sum(r[:ur, :] * column(s) for r, s in zip(refs, scale))
        return total, peak, denom

    def merge_into(dst, refs):
        total, peak, denom = merge(refs)
        dst[:ur, :] = total
        dst[ur:ur + STAT, :] = jnp.concatenate([peak, denom, jnp.zeros((STAT - 2, LANES), F32)], axis=0)

    def sends(send, recv, ssem, rsem, devs):
        return [[remote(send.at[n, i], recv.at[n, i], ssem.at[n * AWAY + i], rsem.at[n * AWAY + i], devs[d])
                 for i, d in enumerate((2, 1, -1))] for n in range(SPLITS)]

    xc = sends(xsend, xrecv, sem_xs, sem_xr, x_dev)
    yc = sends(ysend, yrecv, sem_ys, sem_yr, y_dev)
    oc = [remote(obuf.at[n, c], obuf.at[n, c], sem_os.at[n], sem_or.at[n], partner) for n in range(SPLITS)]
    away = (FAR, RIGHT, LEFT)

    def both(n, k, h):
        return [acc.at[n, k, c, h], pbuf.at[n, k, h]]

    def x_start(n):
        for i, k in enumerate(away):
            pair(k, n).wait_recv()
            for h in range(2):
                merge_into(xsend.at[n, i, h], both(n, k, h))
            xc[n][i].start()

    def x_end(n):
        pair(OWN, n).wait_recv()
        for cp in xc[n]:
            cp.wait_recv()
        for h in range(2):
            total, _, denom = merge(both(n, OWN, h) + [xrecv.at[n, i, h] for i in range(AWAY)])
            obuf[n, c, h * ur:(h + 1) * ur, :] = (total / column(denom)).astype(BF16).astype(F32)
        oc[n].start()

    def product(n, k):
        if n == 0:
            w_copies[k].wait()
        return jnp.dot(lhs[n].astype(BF16), wbuf[k], preferred_element_type=F32)

    def y_start(n):
        oc[n].wait_recv()
        for core, h in halves:
            at = core * part + h * unit
            for t in range(n_tiles):
                for i in range(per):
                    head = (t * per + i) * LANES
                    lhs[n, at:at + unit, head:head + LANES] = obuf[
                        n, core, pl.ds(h * ur + t * unit * per + i, unit, stride=per), :]
        for i, k in enumerate(away):
            prod = product(n, k)
            for h in range(2):
                ysend[n, i, h] = prod[:, h * hc:(h + 1) * hc]
            yc[n][i].start()

    f = x + c * (y - x)
    s = y + c * (x - y)
    sent = []

    def go(copy):
        copy.start()
        sent.append(copy)

    def f_dev(d):
        return {'tp': (y + c * d + ny) % ny, 'sp': ((x + (1 - c) * d + nx) % nx) * 2 + c}

    def s_dev(d):
        return {'tp': (y + (1 - c) * d + ny) % ny, 'sp': ((x + c * d + nx) % nx) * 2 + c}

    def block(n, fd, sd):
        return gbuf.at[n, c, (f + fd + nx) % nx, (s + sd + ny) % ny]

    def kind(d, is_half):
        return is_half * 2 + (d > 0)

    def along(ring, n, fd, sd, d, is_half=False):
        ref = block(n, fd, sd)
        if is_half:
            ref = ref.at[0 if d > 0 else 1]
        if ring == 'f':
            i = n * ROUTES + kind(d, is_half)
            return remote(ref, ref, sem_fs.at[i], sem_fr.at[i], f_dev(d))
        i = (n * nx + fd % nx) * ROUTES + kind(d, is_half)
        return remote(ref, ref, sem_ss.at[i], sem_sr.at[i], s_dev(d))

    def over(n, fd, sd):
        i = (n * nx + fd % nx) * ny + sd % ny
        ref = block(n, fd, sd)
        return remote(ref, ref, sem_ds.at[i], sem_dr.at[i], partner)

    def place(n, ci, fi, si, swap):
        xi, yi = fi + swap * (si - fi), si + swap * (fi - si)
        for h in range(2):
            at = pl.ds(pl.multiple_of(ci * half_d + yi * cols + h * hc, LANES), hc)
            for core in range(2):
                first = pl.multiple_of(xi * rows + (core * SPLITS + n) * part, part)
                out_ref[pl.ds(first, part), at] = gbuf[n, ci, fi, si, h, core * part:(core + 1) * part, :].astype(BF16)

    def place_here(n, fd, sd):
        place(n, c, (f + fd + nx) % nx, (s + sd + ny) % ny, c)

    def spread(n, fd):
        for d in (1, -1):
            go(along('s', n, fd, 0, d))
        go(over(n, fd, 0))

    def y_end(n):
        own = product(n, OWN)
        for cp in yc[n]:
            cp.wait_recv()
        for h in range(2):
            total = sum([yrecv[n, i, h] for i in range(AWAY)], own[:, h * hc:(h + 1) * hc])
            at = pl.ds(pl.multiple_of(c * half_d + y * cols + h * hc, LANES), hc)
            kept = jnp.concatenate([hbuf[pl.ds(pl.multiple_of(x * rows + (core * SPLITS + n) * part, part), part), at]
                                    for core in range(2)], axis=0)
            gbuf[n, c, f, s, h] = (kept.astype(F32) + total).astype(BF16).astype(F32)
        for d in (1, -1):
            go(along('f', n, 0, 0, d))
        spread(n, 0)
        place_here(n, 0, 0)

    def pass_on(ring, n, fd, sd, d):
        along(ring, n, fd, sd, d).wait_recv()
        go(along(ring, n, fd, sd, d, True))

    def f_ring(n):
        for d in (1, -1):
            pass_on('f', n, -d, 0, d)
            spread(n, -d)
        for d in (1, -1):
            place_here(n, -d, 0)

    def f_end(n):
        for d in (1, -1):
            along('f', n, 2, 0, d, True).wait_recv()
        spread(n, 2)
        place_here(n, 2, 0)

    def s_ring(n, fd):
        for d in (1, -1):
            pass_on('s', n, fd, -d, d)
            go(over(n, fd, -d))
        for d in (1, -1):
            place_here(n, fd, -d)

    def s_end(n, fd):
        for d in (1, -1):
            along('s', n, fd, 2, d, True).wait_recv()
        go(over(n, fd, 2))
        place_here(n, fd, 2)

    def take(n, fd, sd):
        i = (n * nx + fd % nx) * ny + sd % ny
        fi, si = (s + fd + nx) % nx, (f + sd + ny) % ny
        ref = gbuf.at[n, 1 - c, fi, si]
        remote(ref, ref, sem_ds.at[i], sem_dr.at[i], partner).wait_recv()
        place(n, 1 - c, fi, si, 1 - c)

    def stage(n, i):
        if i == 0:
            f_ring(n)
            s_ring(n, 0)
        elif i == 1:
            f_end(n)
            s_ring(n, -1)
            s_ring(n, 1)
            s_end(n, 0)
        elif i == 2:
            for fd in (0, -1, 1):
                take(n, fd, 0)
            s_ring(n, 2)
            s_end(n, -1)
            s_end(n, 1)
        else:
            for fd, sd in ((2, 0), (0, -1), (0, 1), (0, 2), (-1, -1), (-1, 1), (1, -1), (1, 1)):
                take(n, fd, sd)
            s_end(n, 2)

    attend(0)
    x_start(0)
    attend(1)
    x_start(1)
    x_end(0)
    y_start(0)
    x_end(1)
    y_start(1)
    y_end(0)
    y_end(1)
    for i in range(ROUTES):
        for n in range(SPLITS):
            stage(n, i)
    for n in range(SPLITS):
        for fd, sd in ((2, -1), (2, 1), (-1, 2), (1, 2), (2, 2)):
            take(n, fd, sd)
    for n in range(SPLITS):
        for k in range(ROUTES):
            pair(k, n).wait_send()
    for cp in xc + yc:
        for one in cp:
            one.wait_send()
    for cp in oc + sent:
        cp.wait_send()


def solution(mesh):
    cache_spec = P('dp', 'sp', 'tp', None)
    sp = mesh.shape['sp']
    tp = mesh.shape['tp']

    def local_step(hidden, lengths, k_cache, v_cache, norm_gain, w_query, w_key, w_value, w_out):
        batch, seq_block, kv, head_dim = k_cache.shape
        d_model = hidden.shape[1]
        width = w_query.shape[1]
        heads = width // head_dim
        n_w = width // (2 * BLOCK) + 1
        flat = batch * seq_block * kv
        hbm = pl.BlockSpec(memory_space=pltpu.HBM)
        vmem = pl.BlockSpec(memory_space=pltpu.VMEM)
        shape = jax.ShapeDtypeStruct
        buf = pltpu.VMEM

        def dma(*shapes):
            return [pltpu.SemaphoreType.DMA(s) if s else pltpu.SemaphoreType.DMA for s in shapes]

        nx = sp // 2
        rows = batch // nx
        cols = d_model // (2 * tp)
        ur = batch // (sp * SPLITS * 2) * heads
        travel = buf((SPLITS, AWAY, 2, ur + STAT, head_dim), F32)
        yblock = buf((SPLITS, AWAY, 2, rows // SPLITS, cols // 2), F32)
        n_x, n_f = SPLITS * AWAY, SPLITS * ROUTES
        n_s = n_f * nx
        n_d = SPLITS * nx * tp
        k_new, v_new, out = pl.pallas_call(
            functools.partial(decode_kernel, seq_block, kv, heads),
            out_shape=(buf((flat, head_dim), BF16), buf((flat, head_dim), BF16), buf((batch, d_model), BF16)),
            in_specs=[hbm] * (N_INPUTS + 1),
            out_specs=(vmem, vmem, vmem),
            scratch_shapes=[
                buf((2 * n_w, batch * BLOCK // head_dim, head_dim), F32),
                pltpu.SMEM((batch,), jnp.int32),
                buf((batch, d_model), BF16),
                buf((d_model,), BF16),
                buf((1, d_model), F32),
                buf((batch, d_model), BF16),
                buf((n_w, d_model, BLOCK), BF16),
                *dma((), (), (HID,), (n_w,), (PIECES,), (PIECES,), (n_w,), (n_w,)),
                buf((SPLITS, ROUTES, 2, 2, ur + STAT, head_dim), F32),
                buf((SPLITS, ROUTES, 2, ur + STAT, head_dim), F32),
                travel, travel,
                buf((SPLITS, 2, 2 * ur, head_dim), F32),
                buf((SPLITS, rows // SPLITS, width), F32),
                buf((ROUTES, width, cols), BF16),
                yblock, yblock,
                buf((SPLITS, 2, nx, tp, 2, rows // SPLITS, cols // 2), F32),
                *dma((ROUTES,), (n_f,), (n_f,), (n_x,), (n_x,), (SPLITS,), (SPLITS,), (n_x,), (n_x,),
                     (n_f,), (n_f,), (n_s,), (n_s,), (n_d,), (n_d,)),
            ],
            compiler_params=pltpu.CompilerParams(collective_id=0, has_side_effects=True, vmem_limit_bytes=VMEM_MIB * MIB),
            name='decode_step',
        )(lengths, hidden, norm_gain, w_query, w_key, w_value,
          k_cache.reshape(flat, head_dim), v_cache.reshape(flat, head_dim), w_out)
        results = (k_new, v_new, out)
        k_new, v_new, out = pl.pallas_call(
            store_kernel,
            out_shape=tuple(shape(r.shape, r.dtype) for r in results),
            in_specs=[vmem] * N_OUTS,
            out_specs=(hbm,) * N_OUTS,
            scratch_shapes=dma((N_OUTS,)),
            compiler_params=pltpu.CompilerParams(vmem_limit_bytes=MIB),
            name='store',
        )(*results)
        return out, k_new.reshape(k_cache.shape), v_new.reshape(v_cache.shape)

    return jax.shard_map(
        local_step,
        mesh=mesh,
        in_specs=(P('dp', None), P('dp'), cache_spec, cache_spec, P(None), P(None, 'tp'), P(None, 'tp'), P(None, 'tp'), P('tp', None)),
        out_specs=(P('dp', None), cache_spec, cache_spec),
        check_vma=False,
    )
```

```python
import functools
import math

import jax
import jax.numpy as jnp
from jax import lax
from jax.experimental import pallas as pl
from jax.experimental.pallas import tpu as pltpu
from jax.sharding import PartitionSpec as P

EPS = 1e-6
NEG_BIG = -1e30
FLOOR = -0.999e30
LOG2E = math.log2(math.e)
MIB = 1 << 20
VMEM_MIB = 52
F32 = jnp.float32
BF16 = jnp.bfloat16
LANES = 128
SUB = 8
BLOCK = 256
GROUP = 4
SPLITS = 2
PIECES = 16
HID = 4
FAR, RIGHT, LEFT, OWN = range(4)
HOPS = (2, 1, -1, 0)
LAG = 3
AWAY = 3
ROUTES = 4
N_INPUTS, N_OUTS, N_PROJECT = 8, 3, 12
STAT = SUB


def remote(src, dst, ssem, rsem, dev):
    return pltpu.make_async_remote_copy(src_ref=src, dst_ref=dst, send_sem=ssem, recv_sem=rsem,
                                        device_id=dev, device_id_type=pl.DeviceIdType.MESH)


def meet(peers):
    barrier = pltpu.get_barrier_semaphore()
    for dev in peers:
        pl.semaphore_signal(barrier, inc=1, device_id=dev, device_id_type=pl.DeviceIdType.MESH)
    return barrier


def iota(shape, dim):
    return lax.broadcasted_iota(jnp.int32, shape, dim)


def project(seq_block, kv, enter, len_hbm, hid_hbm, gain_hbm, wq_hbm, wk_hbm, wv_hbm, kc_hbm, vc_hbm,
            kbuf, vbuf, kvq, len_ref, hbuf, gain_raw, gain_ref, nbuf, wbuf,
            sem_l, sem_g, sem_h, sem_w, sem_k, sem_v, sem_s, sem_r):
    batch, d_model = hid_hbm.shape
    n_w = wbuf.shape[0]
    spi, y = lax.axis_index('sp'), lax.axis_index('tp')
    c = spi % 2
    partner = {'tp': y, 'sp': spi + 1 - 2 * c}
    base = spi * seq_block
    rows_h = batch // HID
    seq_rows = seq_block * kv
    per_piece = batch // PIECES
    crow = per_piece * seq_rows

    hid_copies = [pltpu.make_async_copy(hid_hbm.at[pl.ds(i * rows_h, rows_h)], hbuf.at[pl.ds(i * rows_h, rows_h)], sem_h.at[i])
                  for i in range(HID)]
    len_copy = pltpu.make_async_copy(len_hbm, len_ref, sem_l)
    gain_copy = pltpu.make_async_copy(gain_hbm, gain_raw, sem_g)

    def w_copy(j, src, first):
        return pltpu.make_async_copy(src.at[:, pl.ds(first, BLOCK)], wbuf.at[j], sem_w.at[j])

    def q_copy(j):
        return w_copy(j, wq_hbm, pl.multiple_of(c * (n_w - 1) * BLOCK + (j - 1) * BLOCK, BLOCK))

    def cache_copies(p):
        part = pl.ds(pl.multiple_of(p * crow, crow), crow)
        return [pltpu.make_async_copy(src.at[part], buf.at[part], sem.at[p])
                for src, buf, sem in ((kc_hbm, kbuf, sem_k), (vc_hbm, vbuf, sem_v))]

    def trade(j):
        slot = kvq.at[c * n_w + j]
        return remote(slot, slot, sem_s.at[j], sem_r.at[j], partner)

    def arrival(j):
        slot = kvq.at[(1 - c) * n_w + j]
        return remote(slot, slot, sem_s.at[j], sem_r.at[j], partner)

    for cp in hid_copies + [gain_copy, len_copy]:
        cp.start()
    gain_copy.wait()
    gain_ref[...] = gain_raw[...].astype(F32).reshape(gain_ref.shape)
    hid_copies[0].wait()

    q_copy(1).start()

    def kv_start():
        @pl.when(c == 0)
        def _():
            w_copy(0, wk_hbm, 0).start()

        @pl.when(c == 1)
        def _():
            w_copy(0, wv_hbm, 0).start()

    step = 2 * SUB
    wide = SUB * LANES

    def norm_rows(r, carry):
        row = pl.ds(pl.multiple_of(r * step, step), step)
        cuts = [slice(w, w + wide) for w in range(0, d_model, wide)]
        total = jnp.zeros((step, 1), F32)
        for cut in cuts:
            v = hbuf[row, cut].astype(F32)
            total = total + jnp.sum(v * v, axis=1, keepdims=True)
        inv = lax.rsqrt(total / d_model + EPS)
        for cut in cuts:
            nbuf[row, cut] = (hbuf[row, cut].astype(F32) * inv * gain_ref[:, cut]).astype(BF16)
        return carry

    for i in range(HID):
        if i:
            hid_copies[i].wait()
            if i + 1 < n_w:
                q_copy(i + 1).start()
            else:
                kv_start()
        lax.fori_loop(i * rows_h // step, (i + 1) * rows_h // step, norm_rows, 0)
    enter()

    per_step = PIECES // n_w

    def columns(it, carry):
        j = (it + 1) % n_w
        w_copy(j, wk_hbm, 0).wait()
        for i in range(per_step):
            for cp in cache_copies(it * per_step + i):
                cp.start()

        @pl.when(it > 0)
        def _():
            trade(it).start()

        res = jnp.dot(nbuf[...], wbuf[j], preferred_element_type=F32)
        for i in range(BLOCK // LANES):
            kvq[c * n_w + j, pl.ds(i, batch, stride=BLOCK // LANES), :] = res[:, i * LANES:(i + 1) * LANES]
        return carry

    lax.fori_loop(0, n_w, columns, 0)
    trade(0).start()
    len_copy.wait()
    for p in range(PIECES):
        for cp in cache_copies(p):
            cp.wait()
    for j in range(1, n_w):
        arrival(j).wait_recv()

    pair_row = iota((step, LANES), 0) % kv
    slot_pos = iota((seq_rows, LANES), 0) // kv

    def update(p, carry):
        for i in range(per_piece):
            b = p * per_piece + i
            here = slot_pos == len_ref[b] - base
            rows = pl.ds(pl.multiple_of(b * seq_rows, step), seq_rows)
            for core, buf in enumerate((kbuf, vbuf)):
                new = kvq[core * n_w, pl.ds(b * kv, 1), :]
                for n in range(1, kv):
                    new = jnp.where(pair_row == n, kvq[core * n_w, pl.ds(b * kv + n, 1), :], new)
                new = jnp.concatenate([new.astype(BF16)] * (seq_rows // step), axis=0)
                buf[rows, :] = jnp.where(here, new, buf[rows, :])
        return carry

    def new_tokens():
        lax.fori_loop(0, PIECES, update, 0)
        for j in range(n_w):
            trade(j).wait_send()

    return arrival(0).wait_recv, new_tokens


def store_kernel(*refs):
    copies = [pltpu.make_async_copy(refs[i], refs[N_OUTS + i], refs[-1].at[i]) for i in range(N_OUTS)]
    for cp in copies:
        cp.start()
    for cp in copies:
        cp.wait()


def decode_kernel(seq_block, kv, heads, *refs):
    inputs, wo_hbm, outs = refs[:N_INPUTS], refs[N_INPUTS], refs[N_INPUTS + 1:N_INPUTS + N_OUTS + 1]
    kvq, len_ref, hbuf, *rest = refs[N_INPUTS + N_OUTS + 1:]
    kbuf, vbuf, out_ref = outs

    def first(enter):
        return project(seq_block, kv, enter, *inputs, kbuf, vbuf, kvq, len_ref, hbuf, *rest[:N_PROJECT])

    exchange(seq_block, kv, heads, first, kbuf, vbuf, kvq, len_ref, hbuf, wo_hbm, out_ref, *rest[N_PROJECT:])


def exchange(seq_block, kv, heads, first_part, kbuf, vbuf, kvq, len_ref, hbuf, wo_hbm, out_ref,
             score_a, score_b, newest, acc, pbuf, xsend, xrecv, obuf, lhs, wbuf, ysend, yrecv, gbuf,
             sem_w, sem_ps, sem_pr, sem_xs, sem_xr, sem_os, sem_or, sem_ys, sem_yr,
             sem_fs, sem_fr, sem_ss, sem_sr, sem_ds, sem_dr):
    batch, d_model = out_ref.shape
    spi, y = lax.axis_index('sp'), lax.axis_index('tp')
    sp, ny = lax.axis_size('sp'), lax.axis_size('tp')
    nx = sp // 2
    x, c = spi // 2, spi % 2
    base = spi * seq_block
    seq_rows = seq_block * kv
    n_w = kvq.shape[0] // 2
    unit = batch // (sp * SPLITS * 2)
    ur = unit * heads
    rows = batch // nx
    part = rows // (2 * SPLITS)
    half_d = d_model // 2
    cols = half_d // ny
    hc = cols // 2

    def at_x(d):
        return (x + d + nx) % nx

    def at_y(d):
        return (y + d + ny) % ny

    partner = {'tp': y, 'sp': spi + 1 - 2 * c}
    x_dev = {d: {'tp': y, 'sp': at_x(d) * 2 + c} for d in (2, 1, -1)}
    y_dev = {d: {'tp': at_y(d), 'sp': spi} for d in (2, 1, -1)}

    barrier = meet([partner, *x_dev.values(), *y_dev.values()])
    w_copies = []
    for k in range(ROUTES):
        col = pl.multiple_of(c * half_d + at_y(HOPS[k]) * cols, LANES)
        w_copies.append(pltpu.make_async_copy(wo_hbm.at[:, pl.ds(col, cols)], wbuf.at[k], sem_w.at[k]))
    new_arrived, new_tokens = first_part(lambda: pl.semaphore_wait(barrier, 1 + len(x_dev) + len(y_dev)))
    for cp in w_copies:
        cp.start()

    per = BLOCK // LANES
    tile = GROUP * per
    n_tiles = heads // per
    qrows = GROUP * heads
    krows = GROUP * seq_rows
    row_id, col_id = iota((qrows, krows), 0), iota((qrows, krows), 1)
    same = (row_id % tile // per == col_id // seq_rows) & (row_id // (qrows // kv) == col_id % kv)
    col_row = iota((1, krows), 1)
    col_seq = col_row // seq_rows
    col_pos = col_row % seq_rows // kv
    diag = iota((ur, LANES), 0) == iota((ur, LANES), 1)
    fold = LANES ** -0.5 * LOG2E
    halves = [(core, h) for core in range(2) for h in range(2)]
    groups = [(core, h, g) for core, h in halves for g in range(unit // GROUP)]

    def pair(k, n):
        return remote(acc.at[n, k, 1 - c], pbuf.at[n, k], sem_ps.at[n * ROUTES + k], sem_pr.at[n * ROUTES + k], partner)

    def first(n, k, core, h, g):
        dest = at_x(HOPS[k])
        return (((dest * 2 + core) * SPLITS + n) * 2 + h) * unit + g * GROUP

    def score(n, k, sbuf):
        for at, where in enumerate(groups):
            b0 = first(n, k, *where)
            rows8 = pl.ds(pl.multiple_of(b0 * per, tile), tile)
            q = jnp.concatenate([kvq[core * n_w + j, rows8, :] for core in range(2) for j in range(1, n_w)], axis=0)
            keys = kbuf[pl.ds(pl.multiple_of(b0 * seq_rows, krows), krows), :]
            s = lax.dot_general(q.astype(BF16), keys, (((1,), (1,)), ((), ())), preferred_element_type=F32)
            last = jnp.full((1, krows), len_ref[b0] - base, jnp.int32)
            for i in range(1, GROUP):
                last = jnp.where(col_seq == i, len_ref[b0 + i] - base, last)
            sbuf[at] = jnp.where(same & (col_pos < last), s * fold, NEG_BIG)

    def finish(n, k, sbuf):
        stats = []
        for at, where in enumerate(groups):
            core, h, g = where
            s = sbuf[at]
            m = jnp.maximum(jnp.max(s, axis=1, keepdims=True), FLOOR)
            e = jnp.exp2(s - m)
            stats.append((m, jnp.sum(e, axis=1, keepdims=True)))
            values = vbuf[pl.ds(pl.multiple_of(first(n, k, *where) * seq_rows, krows), krows), :]
            o = jnp.dot(e.astype(BF16), values, preferred_element_type=F32)
            for t in range(n_tiles):
                row = (t * (unit // GROUP) + g) * tile
                acc[n, k, core, h, row:row + tile, :] = o[t * tile:(t + 1) * tile]
        for core, h in halves:
            mine = [stat for where, stat in zip(groups, stats) if where[:2] == (core, h)]
            packed = []
            for which in range(2):
                col = jnp.concatenate([stat[which][t * tile:(t + 1) * tile] for t in range(n_tiles) for stat in mine], axis=0)
                packed.append(jnp.sum(jnp.where(diag, jnp.broadcast_to(col, diag.shape), 0.0), axis=0, keepdims=True))
            packed.append(jnp.zeros((STAT - len(packed), LANES), F32))
            acc[n, k, core, h, ur:ur + STAT, :] = jnp.concatenate(packed, axis=0)
        pair(k, n).start()

    def column(stat):
        return jnp.sum(jnp.where(diag, jnp.broadcast_to(stat, diag.shape), 0.0), axis=1, keepdims=True)

    def merge(refs):
        both = [(r[ur:ur + 1, :], r[ur + 1:ur + 2, :]) for r in refs]
        peak = functools.reduce(jnp.maximum, [m for m, _ in both])
        scale = [jnp.exp2(m - peak) for m, _ in both]
        denom = sum(l * s for (_, l), s in zip(both, scale))
        total = sum(r[:ur, :] * column(s) for r, s in zip(refs, scale))
        return total, peak, denom

    def merge_into(dst, refs):
        total, peak, denom = merge(refs)
        dst[:ur, :] = total
        dst[ur:ur + STAT, :] = jnp.concatenate([peak, denom, jnp.zeros((STAT - 2, LANES), F32)], axis=0)

    def sends(send, recv, ssem, rsem, devs):
        return [[remote(send.at[n, i], recv.at[n, i], ssem.at[n * AWAY + i], rsem.at[n * AWAY + i], devs[d])
                 for i, d in enumerate(HOPS[:AWAY])] for n in range(SPLITS)]

    xc = sends(xsend, xrecv, sem_xs, sem_xr, x_dev)
    yc = sends(ysend, yrecv, sem_ys, sem_yr, y_dev)
    oc = [remote(obuf.at[n, c], obuf.at[n, c], sem_os.at[n], sem_or.at[n], partner) for n in range(SPLITS)]

    def both(n, k, h):
        return [acc.at[n, k, c, h], pbuf.at[n, k, h]]

    def x_start(n, k):
        if k == OWN:
            return
        pair(k, n).wait_recv()
        for h in range(2):
            merge_into(xsend.at[n, k, h], both(n, k, h))
        xc[n][k].start()

    def fresh(n):
        two = unit * kv
        parity = iota((two, LANES), 0) % kv
        for h in range(2):
            rows16 = pl.ds(pl.multiple_of((((x * 2 + c) * SPLITS + n) * 2 + h) * two, two), two)
            score_col = []
            for core in range(kv):
                k, v = [jnp.where(parity == core, r, pltpu.roll(r, 1 if core == 0 else two - 1, 0))
                        for r in (kvq[i * n_w, rows16, :].astype(BF16).astype(F32) for i in range(2))]
                for j in range(1, n_w):
                    q = kvq[core * n_w + j, rows16, :].astype(BF16).astype(F32)
                    score_col.append(jnp.sum(q * k, axis=1, keepdims=True) * fold)
                    at = (core * (n_w - 1) + j - 1) * two
                    newest[n, h, at:at + two, :] = v
            col = jnp.broadcast_to(jnp.concatenate(score_col, axis=0), diag.shape)
            peak = jnp.sum(jnp.where(diag, col, 0.0), axis=0, keepdims=True)
            newest[n, h, ur:ur + STAT, :] = jnp.where(iota((STAT, LANES), 0) == 0, jnp.broadcast_to(peak, (STAT, LANES)), 1.0)

    def x_end(n):
        pair(OWN, n).wait_recv()
        for cp in xc[n]:
            cp.wait_recv()
        for h in range(2):
            total, _, denom = merge(both(n, OWN, h) + [newest.at[n, h]] + [xrecv.at[n, i, h] for i in range(AWAY)])
            obuf[n, c, h * ur:(h + 1) * ur, :] = (total / column(denom)).astype(BF16).astype(F32)
        oc[n].start()

    def product(n, k):
        if n == 0:
            w_copies[k].wait()
        return jnp.dot(lhs[n].astype(BF16), wbuf[k], preferred_element_type=F32)

    def y_start(n):
        oc[n].wait_recv()
        for core, h in halves:
            at = core * part + h * unit
            for t in range(n_tiles):
                for i in range(per):
                    head = (t * per + i) * LANES
                    lhs[n, at:at + unit, head:head + LANES] = obuf[
                        n, core, pl.ds(h * ur + t * unit * per + i, unit, stride=per), :]
        for i in range(AWAY):
            prod = product(n, i)
            for h in range(2):
                ysend[n, i, h] = prod[:, h * hc:(h + 1) * hc]
            yc[n][i].start()

    f = x + c * (y - x)
    s = y + c * (x - y)
    sent = []

    def go(copy):
        copy.start()
        sent.append(copy)

    def f_dev(d):
        return {'tp': (y + c * d + ny) % ny, 'sp': ((x + (1 - c) * d + nx) % nx) * 2 + c}

    def s_dev(d):
        return {'tp': (y + (1 - c) * d + ny) % ny, 'sp': ((x + c * d + nx) % nx) * 2 + c}

    def block(n, fd, sd):
        return gbuf.at[n, c, (f + fd + nx) % nx, (s + sd + ny) % ny]

    def kind(d, is_half):
        return is_half * 2 + (d > 0)

    def along(ring, n, fd, sd, d, is_half=False):
        ref = block(n, fd, sd)
        if is_half:
            ref = ref.at[0 if d > 0 else 1]
        if ring == 'f':
            i = n * ROUTES + kind(d, is_half)
            return remote(ref, ref, sem_fs.at[i], sem_fr.at[i], f_dev(d))
        i = (n * nx + fd % nx) * ROUTES + kind(d, is_half)
        return remote(ref, ref, sem_ss.at[i], sem_sr.at[i], s_dev(d))

    def over(n, fd, sd):
        i = (n * nx + fd % nx) * ny + sd % ny
        ref = block(n, fd, sd)
        return remote(ref, ref, sem_ds.at[i], sem_dr.at[i], partner)

    def place(n, ci, fi, si, swap):
        xi, yi = fi + swap * (si - fi), si + swap * (fi - si)
        for h in range(2):
            at = pl.ds(pl.multiple_of(ci * half_d + yi * cols + h * hc, LANES), hc)
            for core in range(2):
                first = pl.multiple_of(xi * rows + (core * SPLITS + n) * part, part)
                out_ref[pl.ds(first, part), at] = gbuf[n, ci, fi, si, h, core * part:(core + 1) * part, :].astype(BF16)

    def place_here(n, fd, sd):
        place(n, c, (f + fd + nx) % nx, (s + sd + ny) % ny, c)

    def spread(n, fd):
        for d in (1, -1):
            go(along('s', n, fd, 0, d))
        go(over(n, fd, 0))

    def y_end(n):
        own = product(n, OWN)
        for cp in yc[n]:
            cp.wait_recv()
        for h in range(2):
            total = sum([yrecv[n, i, h] for i in range(AWAY)], own[:, h * hc:(h + 1) * hc])
            at = pl.ds(pl.multiple_of(c * half_d + y * cols + h * hc, LANES), hc)
            kept = jnp.concatenate([hbuf[pl.ds(pl.multiple_of(x * rows + (core * SPLITS + n) * part, part), part), at]
                                    for core in range(2)], axis=0)
            gbuf[n, c, f, s, h] = (kept.astype(F32) + total).astype(BF16).astype(F32)
        for d in (1, -1):
            go(along('f', n, 0, 0, d))
        spread(n, 0)
        place_here(n, 0, 0)

    def pass_on(ring, n, fd, sd, d):
        along(ring, n, fd, sd, d).wait_recv()
        go(along(ring, n, fd, sd, d, True))

    def f_ring(n):
        for d in (1, -1):
            pass_on('f', n, -d, 0, d)
            spread(n, -d)
        for d in (1, -1):
            place_here(n, -d, 0)

    def f_end(n):
        for d in (1, -1):
            along('f', n, 2, 0, d, True).wait_recv()
        spread(n, 2)
        place_here(n, 2, 0)

    def s_ring(n, fd):
        for d in (1, -1):
            pass_on('s', n, fd, -d, d)
            go(over(n, fd, -d))
        for d in (1, -1):
            place_here(n, fd, -d)

    def s_end(n, fd):
        for d in (1, -1):
            along('s', n, fd, 2, d, True).wait_recv()
        go(over(n, fd, 2))
        place_here(n, fd, 2)

    def take(n, fd, sd):
        i = (n * nx + fd % nx) * ny + sd % ny
        fi, si = (s + fd + nx) % nx, (f + sd + ny) % ny
        ref = gbuf.at[n, 1 - c, fi, si]
        remote(ref, ref, sem_ds.at[i], sem_dr.at[i], partner).wait_recv()
        place(n, 1 - c, fi, si, 1 - c)

    def stage(n, i):
        if i == 0:
            f_ring(n)
            s_ring(n, 0)
        elif i == 1:
            f_end(n)
            s_ring(n, -1)
            s_ring(n, 1)
            s_end(n, 0)
        elif i == 2:
            for fd in (0, -1, 1):
                take(n, fd, 0)
            s_ring(n, 2)
            s_end(n, -1)
            s_end(n, 1)
        else:
            for fd, sd in ((2, 0), (0, -1), (0, 1), (0, 2), (-1, -1), (-1, 1), (1, -1), (1, 1)):
                take(n, fd, sd)
            s_end(n, 2)

    scores = (score_a, score_b)
    steps = [(n, k) for n in range(SPLITS) for k in range(ROUTES)]
    score(*steps[0], scores[0])
    for i, step in enumerate(steps):
        if i + 1 < len(steps):
            score(*steps[i + 1], scores[(i + 1) % 2])
        finish(*step, scores[i % 2])
        if i >= LAG:
            x_start(*steps[i - LAG])
    for step in steps[-LAG:]:
        x_start(*step)
    new_arrived()
    for n in range(SPLITS):
        fresh(n)
    new_tokens()
    x_end(0)
    y_start(0)
    x_end(1)
    y_start(1)
    y_end(0)
    y_end(1)
    for i in range(ROUTES):
        for n in range(SPLITS):
            stage(n, i)
    for n in range(SPLITS):
        for fd, sd in ((2, -1), (2, 1), (-1, 2), (1, 2), (2, 2)):
            take(n, fd, sd)
    for n in range(SPLITS):
        for k in range(ROUTES):
            pair(k, n).wait_send()
    for cp in xc + yc:
        for one in cp:
            one.wait_send()
    for cp in oc + sent:
        cp.wait_send()


def solution(mesh):
    cache_spec = P('dp', 'sp', 'tp', None)
    sp = mesh.shape['sp']
    tp = mesh.shape['tp']

    def local_step(hidden, lengths, k_cache, v_cache, norm_gain, w_query, w_key, w_value, w_out):
        batch, seq_block, kv, head_dim = k_cache.shape
        d_model = hidden.shape[1]
        width = w_query.shape[1]
        heads = width // head_dim
        n_w = width // (2 * BLOCK) + 1
        flat = batch * seq_block * kv
        hbm = pl.BlockSpec(memory_space=pltpu.HBM)
        vmem = pl.BlockSpec(memory_space=pltpu.VMEM)
        shape = jax.ShapeDtypeStruct
        buf = pltpu.VMEM

        def dma(*shapes):
            return [pltpu.SemaphoreType.DMA(s) if s else pltpu.SemaphoreType.DMA for s in shapes]

        nx = sp // 2
        rows = batch // nx
        cols = d_model // (2 * tp)
        ur = batch // (sp * SPLITS * 2) * heads
        scored = buf((batch // (ROUTES * SPLITS * GROUP), GROUP * heads, GROUP * seq_block * kv), F32)
        travel = buf((SPLITS, AWAY, 2, ur + STAT, head_dim), F32)
        yblock = buf((SPLITS, AWAY, 2, rows // SPLITS, cols // 2), F32)
        n_x, n_f = SPLITS * AWAY, SPLITS * ROUTES
        n_s = n_f * nx
        n_d = SPLITS * nx * tp
        k_new, v_new, out = pl.pallas_call(
            functools.partial(decode_kernel, seq_block, kv, heads),
            out_shape=(buf((flat, head_dim), BF16), buf((flat, head_dim), BF16), buf((batch, d_model), BF16)),
            in_specs=[hbm] * (N_INPUTS + 1),
            out_specs=(vmem, vmem, vmem),
            scratch_shapes=[
                buf((2 * n_w, batch * BLOCK // head_dim, head_dim), F32),
                pltpu.SMEM((batch,), jnp.int32),
                buf((batch, d_model), BF16),
                buf((d_model,), BF16),
                buf((1, d_model), F32),
                buf((batch, d_model), BF16),
                buf((n_w, d_model, BLOCK), BF16),
                *dma((), (), (HID,), (n_w,), (PIECES,), (PIECES,), (n_w,), (n_w,)),
                scored, scored,
                buf((SPLITS, 2, ur + STAT, head_dim), F32),
                buf((SPLITS, ROUTES, 2, 2, ur + STAT, head_dim), F32),
                buf((SPLITS, ROUTES, 2, ur + STAT, head_dim), F32),
                travel, travel,
                buf((SPLITS, 2, 2 * ur, head_dim), F32),
                buf((SPLITS, rows // SPLITS, width), F32),
                buf((ROUTES, width, cols), BF16),
                yblock, yblock,
                buf((SPLITS, 2, nx, tp, 2, rows // SPLITS, cols // 2), F32),
                *dma((ROUTES,), (n_f,), (n_f,), (n_x,), (n_x,), (SPLITS,), (SPLITS,), (n_x,), (n_x,),
                     (n_f,), (n_f,), (n_s,), (n_s,), (n_d,), (n_d,)),
            ],
            compiler_params=pltpu.CompilerParams(collective_id=0, has_side_effects=True, vmem_limit_bytes=VMEM_MIB * MIB),
            name='decode_step',
        )(lengths, hidden, norm_gain, w_query, w_key, w_value,
          k_cache.reshape(flat, head_dim), v_cache.reshape(flat, head_dim), w_out)
        results = (k_new, v_new, out)
        k_new, v_new, out = pl.pallas_call(
            store_kernel,
            out_shape=tuple(shape(r.shape, r.dtype) for r in results),
            in_specs=[vmem] * N_OUTS,
            out_specs=(hbm,) * N_OUTS,
            scratch_shapes=dma((N_OUTS,)),
            compiler_params=pltpu.CompilerParams(vmem_limit_bytes=MIB),
            name='store',
        )(*results)
        return out, k_new.reshape(k_cache.shape), v_new.reshape(v_cache.shape)

    return jax.shard_map(
        local_step,
        mesh=mesh,
        in_specs=(P('dp', None), P('dp'), cache_spec, cache_spec, P(None), P(None, 'tp'), P(None, 'tp'), P(None, 'tp'), P('tp', None)),
        out_specs=(P('dp', None), cache_spec, cache_spec),
        check_vma=False,
    )
```

```python
import functools
import math

import jax
import jax.numpy as jnp
from jax import lax
from jax.experimental import pallas as pl
from jax.experimental.pallas import tpu as pltpu
from jax.sharding import PartitionSpec as P

EPS = 1e-6
NEG_BIG = -1e30
FLOOR = -0.999e30
LOG2E = math.log2(math.e)
MIB = 1 << 20
VMEM_MIB = 52
F32 = jnp.float32
BF16 = jnp.bfloat16
LANES = 128
SUB = 8
BLOCK = 256
GROUP = 4
SPLITS = 2
PIECES = 16
HID = 4
FAR, RIGHT, LEFT, OWN = range(4)
HOPS = (2, 1, -1, 0)
LAG = 3
AWAY = 3
ROUTES = 4
N_INPUTS, N_OUTS, N_PROJECT = 8, 3, 12
STAT = SUB


def remote(src, dst, ssem, rsem, dev):
    return pltpu.make_async_remote_copy(src_ref=src, dst_ref=dst, send_sem=ssem, recv_sem=rsem,
                                        device_id=dev, device_id_type=pl.DeviceIdType.MESH)


def meet(peers):
    barrier = pltpu.get_barrier_semaphore()
    for dev in peers:
        pl.semaphore_signal(barrier, inc=1, device_id=dev, device_id_type=pl.DeviceIdType.MESH)
    return barrier


def iota(shape, dim):
    return lax.broadcasted_iota(jnp.int32, shape, dim)


def project(seq_block, kv, enter, len_hbm, hid_hbm, gain_hbm, wq_hbm, wk_hbm, wv_hbm, kc_hbm, vc_hbm,
            kbuf, vbuf, kvq, len_ref, hbuf, gain_raw, gain_ref, nbuf, wbuf,
            sem_l, sem_g, sem_h, sem_w, sem_k, sem_v, sem_s, sem_r):
    batch, d_model = hid_hbm.shape
    n_w = wbuf.shape[0]
    spi, y = lax.axis_index('sp'), lax.axis_index('tp')
    c = spi % 2
    partner = {'tp': y, 'sp': spi + 1 - 2 * c}
    base = spi * seq_block
    rows_h = batch // HID
    seq_rows = seq_block * kv
    per_piece = batch // PIECES
    crow = per_piece * seq_rows

    hid_copies = [pltpu.make_async_copy(hid_hbm.at[pl.ds(i * rows_h, rows_h)], hbuf.at[pl.ds(i * rows_h, rows_h)], sem_h.at[i])
                  for i in range(HID)]
    len_copy = pltpu.make_async_copy(len_hbm, len_ref, sem_l)
    gain_copy = pltpu.make_async_copy(gain_hbm, gain_raw, sem_g)

    def w_copy(j, src, first):
        return pltpu.make_async_copy(src.at[:, pl.ds(first, BLOCK)], wbuf.at[j], sem_w.at[j])

    def q_copy(j):
        return w_copy(j, wq_hbm, pl.multiple_of(c * (n_w - 1) * BLOCK + (j - 1) * BLOCK, BLOCK))

    def cache_copies(p):
        part = pl.ds(pl.multiple_of(p * crow, crow), crow)
        return [pltpu.make_async_copy(src.at[part], buf.at[part], sem)
                for src, buf, sem in ((kc_hbm, kbuf, sem_k), (vc_hbm, vbuf, sem_v))]

    def trade(j):
        slot = kvq.at[c * n_w + j]
        return remote(slot, slot, sem_s, sem_r.at[j], partner)

    def arrival(j):
        slot = kvq.at[(1 - c) * n_w + j]
        return remote(slot, slot, sem_s, sem_r.at[j], partner)

    for cp in hid_copies + [gain_copy, len_copy]:
        cp.start()
    gain_copy.wait()
    gain_ref[...] = gain_raw[...].astype(F32).reshape(gain_ref.shape)
    hid_copies[0].wait()

    q_copy(1).start()

    def kv_start():
        @pl.when(c == 0)
        def _():
            w_copy(0, wk_hbm, 0).start()

        @pl.when(c == 1)
        def _():
            w_copy(0, wv_hbm, 0).start()

    step = 2 * SUB
    wide = SUB * LANES

    def norm_rows(r, carry):
        row = pl.ds(pl.multiple_of(r * step, step), step)
        cuts = [slice(w, w + wide) for w in range(0, d_model, wide)]
        total = jnp.zeros((step, 1), F32)
        for cut in cuts:
            v = hbuf[row, cut].astype(F32)
            total = total + jnp.sum(v * v, axis=1, keepdims=True)
        inv = lax.rsqrt(total / d_model + EPS)
        for cut in cuts:
            nbuf[row, cut] = (hbuf[row, cut].astype(F32) * inv * gain_ref[:, cut]).astype(BF16)
        return carry

    for i in range(HID):
        if i:
            hid_copies[i].wait()
            if i + 1 < n_w:
                q_copy(i + 1).start()
            else:
                kv_start()
        lax.fori_loop(i * rows_h // step, (i + 1) * rows_h // step, norm_rows, 0, unroll=True)
    enter()

    per_step = PIECES // n_w

    def columns(it, carry):
        j = (it + 1) % n_w
        w_copy(j, wk_hbm, 0).wait()
        for i in range(per_step):
            for cp in cache_copies(it * per_step + i):
                cp.start()

        @pl.when(it > 0)
        def _():
            trade(it).start()

        res = jnp.dot(nbuf[...], wbuf[j], preferred_element_type=F32)
        for i in range(BLOCK // LANES):
            kvq[c * n_w + j, pl.ds(i, batch, stride=BLOCK // LANES), :] = res[:, i * LANES:(i + 1) * LANES]
        return carry

    lax.fori_loop(0, n_w, columns, 0)
    trade(0).start()
    len_copy.wait()
    for src, buf, sem in ((kc_hbm, kbuf, sem_k), (vc_hbm, vbuf, sem_v)):
        pltpu.make_async_copy(src, buf, sem).wait()
    for j in range(1, n_w):
        arrival(j).wait_recv()

    pair_row = iota((step, LANES), 0) % kv
    slot_pos = iota((seq_rows, LANES), 0) // kv

    def update(p, carry):
        for i in range(per_piece):
            b = p * per_piece + i
            here = slot_pos == len_ref[b] - base
            rows = pl.ds(pl.multiple_of(b * seq_rows, step), seq_rows)
            for core, buf in enumerate((kbuf, vbuf)):
                new = kvq[core * n_w, pl.ds(b * kv, 1), :]
                for n in range(1, kv):
                    new = jnp.where(pair_row == n, kvq[core * n_w, pl.ds(b * kv + n, 1), :], new)
                new = jnp.concatenate([new.astype(BF16)] * (seq_rows // step), axis=0)
                buf[rows, :] = jnp.where(here, new, buf[rows, :])
        return carry

    def new_tokens():
        lax.fori_loop(0, PIECES, update, 0)
        sent = kvq.at[pl.ds(c * n_w, n_w)]
        remote(sent, sent, sem_s, sem_r.at[0], partner).wait_send()

    return arrival(0).wait_recv, new_tokens


def store_kernel(*refs):
    copies = [pltpu.make_async_copy(refs[i], refs[N_OUTS + i], refs[-1].at[i]) for i in range(N_OUTS)]
    for cp in copies:
        cp.start()
    for cp in copies:
        cp.wait()


def decode_kernel(seq_block, kv, heads, *refs):
    inputs, wo_hbm, outs = refs[:N_INPUTS], refs[N_INPUTS], refs[N_INPUTS + 1:N_INPUTS + N_OUTS + 1]
    kvq, len_ref, hbuf, *rest = refs[N_INPUTS + N_OUTS + 1:]
    kbuf, vbuf, out_ref = outs

    def first(enter):
        return project(seq_block, kv, enter, *inputs, kbuf, vbuf, kvq, len_ref, hbuf, *rest[:N_PROJECT])

    exchange(seq_block, kv, heads, first, kbuf, vbuf, kvq, len_ref, hbuf, wo_hbm, out_ref, *rest[N_PROJECT:])


def exchange(seq_block, kv, heads, first_part, kbuf, vbuf, kvq, len_ref, hbuf, wo_hbm, out_ref,
             score_a, score_b, newest, acc, pbuf, xsend, xrecv, obuf, lhs, wbuf, ysend, yrecv, gbuf,
             sem_w, sem_ps, sem_pr, sem_xs, sem_xr, sem_os, sem_or, sem_ys, sem_yr,
             sem_fs, sem_fr, sem_ss, sem_sr, sem_ds, sem_dr):
    batch, d_model = out_ref.shape
    spi, y = lax.axis_index('sp'), lax.axis_index('tp')
    sp, ny = lax.axis_size('sp'), lax.axis_size('tp')
    nx = sp // 2
    x, c = spi // 2, spi % 2
    base = spi * seq_block
    seq_rows = seq_block * kv
    n_w = kvq.shape[0] // 2
    unit = batch // (sp * SPLITS * 2)
    ur = unit * heads
    rows = batch // nx
    part = rows // (2 * SPLITS)
    half_d = d_model // 2
    cols = half_d // ny
    hc = cols // 2

    def at_x(d):
        return (x + d + nx) % nx

    def at_y(d):
        return (y + d + ny) % ny

    partner = {'tp': y, 'sp': spi + 1 - 2 * c}
    x_dev = {d: {'tp': y, 'sp': at_x(d) * 2 + c} for d in (2, 1, -1)}
    y_dev = {d: {'tp': at_y(d), 'sp': spi} for d in (2, 1, -1)}

    barrier = meet([partner, *x_dev.values(), *y_dev.values()])
    w_copies = []
    for k in range(ROUTES):
        col = pl.multiple_of(c * half_d + at_y(HOPS[k]) * cols, LANES)
        w_copies.append(pltpu.make_async_copy(wo_hbm.at[:, pl.ds(col, cols)], wbuf.at[k], sem_w.at[k]))
    new_arrived, new_tokens = first_part(lambda: pl.semaphore_wait(barrier, 1 + len(x_dev) + len(y_dev)))
    for cp in w_copies:
        cp.start()

    per = BLOCK // LANES
    tile = GROUP * per
    n_tiles = heads // per
    qrows = GROUP * heads
    krows = GROUP * seq_rows
    row_id, col_id = iota((qrows, krows), 0), iota((qrows, krows), 1)
    same = (row_id % tile // per == col_id // seq_rows) & (row_id // (qrows // kv) == col_id % kv)
    col_row = iota((1, krows), 1)
    col_seq = col_row // seq_rows
    col_pos = col_row % seq_rows // kv
    diag = iota((ur, LANES), 0) == iota((ur, LANES), 1)
    fold = LANES ** -0.5 * LOG2E
    halves = [(core, h) for core in range(2) for h in range(2)]
    groups = [(core, h, g) for core, h in halves for g in range(unit // GROUP)]

    def pair(k, n):
        return remote(acc.at[n, k, 1 - c], pbuf.at[n, k], sem_ps.at[n], sem_pr.at[n * ROUTES + k], partner)

    def first(n, k, core, h, g):
        dest = at_x(HOPS[k])
        return (((dest * 2 + core) * SPLITS + n) * 2 + h) * unit + g * GROUP

    def score(n, k, sbuf):
        for at, where in enumerate(groups):
            b0 = first(n, k, *where)
            rows8 = pl.ds(pl.multiple_of(b0 * per, tile), tile)
            q = jnp.concatenate([kvq[core * n_w + j, rows8, :] for core in range(2) for j in range(1, n_w)], axis=0)
            keys = kbuf[pl.ds(pl.multiple_of(b0 * seq_rows, krows), krows), :]
            s = lax.dot_general(q.astype(BF16), keys, (((1,), (1,)), ((), ())), preferred_element_type=F32)
            last = jnp.full((1, krows), len_ref[b0] - base, jnp.int32)
            for i in range(1, GROUP):
                last = jnp.where(col_seq == i, len_ref[b0 + i] - base, last)
            sbuf[at] = jnp.where(same & (col_pos < last), s * fold, NEG_BIG)

    def finish(n, k, sbuf):
        stats = []
        for at, where in enumerate(groups):
            core, h, g = where
            s = sbuf[at]
            m = jnp.maximum(jnp.max(s, axis=1, keepdims=True), FLOOR)
            e = jnp.exp2(s - m)
            stats.append((m, jnp.sum(e, axis=1, keepdims=True)))
            values = vbuf[pl.ds(pl.multiple_of(first(n, k, *where) * seq_rows, krows), krows), :]
            o = jnp.dot(e.astype(BF16), values, preferred_element_type=F32)
            for t in range(n_tiles):
                row = (t * (unit // GROUP) + g) * tile
                acc[n, k, core, h, row:row + tile, :] = o[t * tile:(t + 1) * tile]
        for core, h in halves:
            mine = [stat for where, stat in zip(groups, stats) if where[:2] == (core, h)]
            packed = []
            for which in range(2):
                col = jnp.concatenate([stat[which][t * tile:(t + 1) * tile] for t in range(n_tiles) for stat in mine], axis=0)
                packed.append(jnp.sum(jnp.where(diag, jnp.broadcast_to(col, diag.shape), 0.0), axis=0, keepdims=True))
            packed.append(jnp.zeros((STAT - len(packed), LANES), F32))
            acc[n, k, core, h, ur:ur + STAT, :] = jnp.concatenate(packed, axis=0)
        pair(k, n).start()

    def column(stat):
        return jnp.sum(jnp.where(diag, jnp.broadcast_to(stat, diag.shape), 0.0), axis=1, keepdims=True)

    def merge(refs):
        both = [(r[ur:ur + 1, :], r[ur + 1:ur + 2, :]) for r in refs]
        peak = functools.reduce(jnp.maximum, [m for m, _ in both])
        scale = [jnp.exp2(m - peak) for m, _ in both]
        denom = sum(l * s for (_, l), s in zip(both, scale))
        total = sum(r[:ur, :] * column(s) for r, s in zip(refs, scale))
        return total, peak, denom

    def merge_into(dst, refs):
        total, peak, denom = merge(refs)
        dst[:ur, :] = total
        dst[ur:ur + STAT, :] = jnp.concatenate([peak, denom, jnp.zeros((STAT - 2, LANES), F32)], axis=0)

    def sends(send, recv, ssem, rsem, devs):
        return [[remote(send.at[n, i], recv.at[n, i], ssem.at[n], rsem.at[n * AWAY + i], devs[d])
                 for i, d in enumerate(HOPS[:AWAY])] for n in range(SPLITS)]

    xc = sends(xsend, xrecv, sem_xs, sem_xr, x_dev)
    yc = sends(ysend, yrecv, sem_ys, sem_yr, y_dev)
    oc = [remote(obuf.at[n, c], obuf.at[n, c], sem_os.at[n], sem_or.at[n], partner) for n in range(SPLITS)]

    def both(n, k, h):
        return [acc.at[n, k, c, h], pbuf.at[n, k, h]]

    def x_start(n, k):
        if k == OWN:
            return
        pair(k, n).wait_recv()
        for h in range(2):
            merge_into(xsend.at[n, k, h], both(n, k, h))
        xc[n][k].start()

    def fresh(n):
        two = unit * kv
        parity = iota((two, LANES), 0) % kv
        for h in range(2):
            rows16 = pl.ds(pl.multiple_of((((x * 2 + c) * SPLITS + n) * 2 + h) * two, two), two)
            score_col = []
            for core in range(kv):
                k, v = [jnp.where(parity == core, r, pltpu.roll(r, 1 if core == 0 else two - 1, 0))
                        for r in (kvq[i * n_w, rows16, :].astype(BF16).astype(F32) for i in range(2))]
                for j in range(1, n_w):
                    q = kvq[core * n_w + j, rows16, :].astype(BF16).astype(F32)
                    score_col.append(jnp.sum(q * k, axis=1, keepdims=True) * fold)
                    at = (core * (n_w - 1) + j - 1) * two
                    newest[n, h, at:at + two, :] = v
            col = jnp.broadcast_to(jnp.concatenate(score_col, axis=0), diag.shape)
            peak = jnp.sum(jnp.where(diag, col, 0.0), axis=0, keepdims=True)
            newest[n, h, ur:ur + STAT, :] = jnp.where(iota((STAT, LANES), 0) == 0, jnp.broadcast_to(peak, (STAT, LANES)), 1.0)

    def x_end(n):
        pair(OWN, n).wait_recv()
        for cp in xc[n]:
            cp.wait_recv()
        for h in range(2):
            total, _, denom = merge(both(n, OWN, h) + [newest.at[n, h]] + [xrecv.at[n, i, h] for i in range(AWAY)])
            obuf[n, c, h * ur:(h + 1) * ur, :] = (total / column(denom)).astype(BF16).astype(F32)
        oc[n].start()

    def product(n, k):
        if n == 0:
            w_copies[k].wait()
        return jnp.dot(lhs[n].astype(BF16), wbuf[k], preferred_element_type=F32)

    def y_start(n):
        oc[n].wait_recv()
        for core, h in halves:
            at = core * part + h * unit
            for t in range(n_tiles):
                for i in range(per):
                    head = (t * per + i) * LANES
                    lhs[n, at:at + unit, head:head + LANES] = obuf[
                        n, core, pl.ds(h * ur + t * unit * per + i, unit, stride=per), :]
        for i in range(AWAY):
            prod = product(n, i)
            for h in range(2):
                ysend[n, i, h] = prod[:, h * hc:(h + 1) * hc]
            yc[n][i].start()

    f = x + c * (y - x)
    s = y + c * (x - y)
    def go(copy):
        copy.start()

    def f_dev(d):
        return {'tp': (y + c * d + ny) % ny, 'sp': ((x + (1 - c) * d + nx) % nx) * 2 + c}

    def s_dev(d):
        return {'tp': (y + (1 - c) * d + ny) % ny, 'sp': ((x + c * d + nx) % nx) * 2 + c}

    def block(n, fd, sd):
        return gbuf.at[n, c, (f + fd + nx) % nx, (s + sd + ny) % ny]

    def kind(d, is_half):
        return is_half * 2 + (d > 0)

    def along(ring, n, fd, sd, d, is_half=False):
        ref = block(n, fd, sd)
        if is_half:
            ref = ref.at[0 if d > 0 else 1]
        if ring == 'f':
            i = n * ROUTES + kind(d, is_half)
            return remote(ref, ref, sem_fs.at[n], sem_fr.at[i], f_dev(d))
        i = (n * nx + fd % nx) * ROUTES + kind(d, is_half)
        return remote(ref, ref, sem_ss.at[n], sem_sr.at[i], s_dev(d))

    def over(n, fd, sd):
        i = (n * nx + fd % nx) * ny + sd % ny
        ref = block(n, fd, sd)
        return remote(ref, ref, sem_ds.at[n], sem_dr.at[i], partner)

    def place(n, ci, fi, si, swap):
        xi, yi = fi + swap * (si - fi), si + swap * (fi - si)
        for h in range(2):
            at = pl.ds(pl.multiple_of(ci * half_d + yi * cols + h * hc, LANES), hc)
            for core in range(2):
                first = pl.multiple_of(xi * rows + (core * SPLITS + n) * part, part)
                out_ref[pl.ds(first, part), at] = gbuf[n, ci, fi, si, h, core * part:(core + 1) * part, :].astype(BF16)

    def place_here(n, fd, sd):
        place(n, c, (f + fd + nx) % nx, (s + sd + ny) % ny, c)

    def spread(n, fd):
        for d in (1, -1):
            go(along('s', n, fd, 0, d))
        go(over(n, fd, 0))

    def y_end(n):
        own = product(n, OWN)
        for cp in yc[n]:
            cp.wait_recv()
        for h in range(2):
            total = sum([yrecv[n, i, h] for i in range(AWAY)], own[:, h * hc:(h + 1) * hc])
            at = pl.ds(pl.multiple_of(c * half_d + y * cols + h * hc, LANES), hc)
            kept = jnp.concatenate([hbuf[pl.ds(pl.multiple_of(x * rows + (core * SPLITS + n) * part, part), part), at]
                                    for core in range(2)], axis=0)
            gbuf[n, c, f, s, h] = (kept.astype(F32) + total).astype(BF16).astype(F32)
        for d in (1, -1):
            go(along('f', n, 0, 0, d))
        spread(n, 0)
        place_here(n, 0, 0)

    def pass_on(ring, n, fd, sd, d):
        along(ring, n, fd, sd, d).wait_recv()
        go(along(ring, n, fd, sd, d, True))

    def f_ring(n):
        for d in (1, -1):
            pass_on('f', n, -d, 0, d)
            spread(n, -d)
        for d in (1, -1):
            place_here(n, -d, 0)

    def f_end(n):
        for d in (1, -1):
            along('f', n, 2, 0, d, True).wait_recv()
        spread(n, 2)
        place_here(n, 2, 0)

    def s_ring(n, fd):
        for d in (1, -1):
            pass_on('s', n, fd, -d, d)
            go(over(n, fd, -d))
        for d in (1, -1):
            place_here(n, fd, -d)

    def s_end(n, fd):
        for d in (1, -1):
            along('s', n, fd, 2, d, True).wait_recv()
        go(over(n, fd, 2))
        place_here(n, fd, 2)

    def take(n, fd, sd):
        i = (n * nx + fd % nx) * ny + sd % ny
        fi, si = (s + fd + nx) % nx, (f + sd + ny) % ny
        ref = gbuf.at[n, 1 - c, fi, si]
        remote(ref, ref, sem_ds.at[n], sem_dr.at[i], partner).wait_recv()
        place(n, 1 - c, fi, si, 1 - c)

    def stage(n, i):
        if i == 0:
            f_ring(n)
            s_ring(n, 0)
        elif i == 1:
            f_end(n)
            s_ring(n, -1)
            s_ring(n, 1)
            s_end(n, 0)
        elif i == 2:
            for fd in (0, -1, 1):
                take(n, fd, 0)
            s_ring(n, 2)
            s_end(n, -1)
            s_end(n, 1)
        else:
            for fd, sd in ((2, 0), (0, -1), (0, 1), (0, 2), (-1, -1), (-1, 1), (1, -1), (1, 1)):
                take(n, fd, sd)
            s_end(n, 2)

    scores = (score_a, score_b)
    steps = [(n, k) for n in range(SPLITS) for k in range(ROUTES)]
    score(*steps[0], scores[0])
    for i, step in enumerate(steps):
        if i + 1 < len(steps):
            score(*steps[i + 1], scores[(i + 1) % 2])
        finish(*step, scores[i % 2])
        if i >= LAG:
            x_start(*steps[i - LAG])
    for step in steps[-LAG:]:
        x_start(*step)
    new_arrived()
    for n in range(SPLITS):
        fresh(n)
    new_tokens()
    x_end(0)
    y_start(0)
    x_end(1)
    y_start(1)
    y_end(0)
    y_end(1)
    for i in range(ROUTES):
        for n in range(SPLITS):
            stage(n, i)
    for n in range(SPLITS):
        for fd, sd in ((2, -1), (2, 1), (-1, 2), (1, 2), (2, 2)):
            take(n, fd, sd)
    for n in range(SPLITS):
        done = ((acc.at[n, :, 1 - c], sem_ps), (xsend.at[n], sem_xs), (obuf.at[n, c], sem_os), (ysend.at[n], sem_ys),
                (gbuf.at[n, c, 0, pl.ds(0, AWAY)], sem_fs), (gbuf.at[n, c, pl.ds(0, AWAY)], sem_ss), (gbuf.at[n, c], sem_ds))
        for ref, sem in done:
            remote(ref, ref, sem.at[n], sem_or.at[n], partner).wait_send()


def solution(mesh):
    cache_spec = P('dp', 'sp', 'tp', None)
    sp = mesh.shape['sp']
    tp = mesh.shape['tp']

    def local_step(hidden, lengths, k_cache, v_cache, norm_gain, w_query, w_key, w_value, w_out):
        batch, seq_block, kv, head_dim = k_cache.shape
        d_model = hidden.shape[1]
        width = w_query.shape[1]
        heads = width // head_dim
        n_w = width // (2 * BLOCK) + 1
        flat = batch * seq_block * kv
        hbm = pl.BlockSpec(memory_space=pltpu.HBM)
        vmem = pl.BlockSpec(memory_space=pltpu.VMEM)
        shape = jax.ShapeDtypeStruct
        buf = pltpu.VMEM

        def dma(*shapes):
            return [pltpu.SemaphoreType.DMA(s) if s else pltpu.SemaphoreType.DMA for s in shapes]

        nx = sp // 2
        rows = batch // nx
        cols = d_model // (2 * tp)
        ur = batch // (sp * SPLITS * 2) * heads
        scored = buf((batch // (ROUTES * SPLITS * GROUP), GROUP * heads, GROUP * seq_block * kv), F32)
        travel = buf((SPLITS, AWAY, 2, ur + STAT, head_dim), F32)
        yblock = buf((SPLITS, AWAY, 2, rows // SPLITS, cols // 2), F32)
        n_x, n_f = SPLITS * AWAY, SPLITS * ROUTES
        n_s = n_f * nx
        n_d = SPLITS * nx * tp
        split = (SPLITS,)
        k_new, v_new, out = pl.pallas_call(
            functools.partial(decode_kernel, seq_block, kv, heads),
            out_shape=(buf((flat, head_dim), BF16), buf((flat, head_dim), BF16), buf((batch, d_model), BF16)),
            in_specs=[hbm] * (N_INPUTS + 1),
            out_specs=(vmem, vmem, vmem),
            scratch_shapes=[
                buf((2 * n_w, batch * BLOCK // head_dim, head_dim), F32),
                pltpu.SMEM((batch,), jnp.int32),
                buf((batch, d_model), BF16),
                buf((d_model,), BF16),
                buf((1, d_model), F32),
                buf((batch, d_model), BF16),
                buf((n_w, d_model, BLOCK), BF16),
                *dma((), (), (HID,), (n_w,), (), (), (), (n_w,)),
                scored, scored,
                buf((SPLITS, 2, ur + STAT, head_dim), F32),
                buf((SPLITS, ROUTES, 2, 2, ur + STAT, head_dim), F32),
                buf((SPLITS, ROUTES, 2, ur + STAT, head_dim), F32),
                travel, travel,
                buf((SPLITS, 2, 2 * ur, head_dim), F32),
                buf((SPLITS, rows // SPLITS, width), F32),
                buf((ROUTES, width, cols), BF16),
                yblock, yblock,
                buf((SPLITS, 2, nx, tp, 2, rows // SPLITS, cols // 2), F32),
                *dma((ROUTES,), split, (n_f,), split, (n_x,), split, split, split, (n_x,),
                     split, (n_f,), split, (n_s,), split, (n_d,)),
            ],
            compiler_params=pltpu.CompilerParams(collective_id=0, has_side_effects=True, vmem_limit_bytes=VMEM_MIB * MIB),
            name='decode_step',
        )(lengths, hidden, norm_gain, w_query, w_key, w_value,
          k_cache.reshape(flat, head_dim), v_cache.reshape(flat, head_dim), w_out)
        results = (k_new, v_new, out)
        k_new, v_new, out = pl.pallas_call(
            store_kernel,
            out_shape=tuple(shape(r.shape, r.dtype) for r in results),
            in_specs=[vmem] * N_OUTS,
            out_specs=(hbm,) * N_OUTS,
            scratch_shapes=dma((N_OUTS,)),
            compiler_params=pltpu.CompilerParams(vmem_limit_bytes=MIB),
            name='store',
        )(*results)
        return out, k_new.reshape(k_cache.shape), v_new.reshape(v_cache.shape)

    return jax.shard_map(
        local_step,
        mesh=mesh,
        in_specs=(P('dp', None), P('dp'), cache_spec, cache_spec, P(None), P(None, 'tp'), P(None, 'tp'), P(None, 'tp'), P('tp', None)),
        out_specs=(P('dp', None), cache_spec, cache_spec),
        check_vma=False,
    )
```

```python
import functools
import math

import jax
import jax.numpy as jnp
from jax import lax
from jax.experimental import pallas as pl
from jax.experimental.pallas import tpu as pltpu
from jax.sharding import PartitionSpec as P

EPS = 1e-6
NEG_BIG = -1e30
FLOOR = -0.999e30
LOG2E = math.log2(math.e)
MIB = 1 << 20
VMEM_MIB = 52
F32 = jnp.float32
BF16 = jnp.bfloat16
LANES = 128
SUB = 8
BLOCK = 256
GROUP = 4
SPLITS = 2
PIECES = 16
HID = 4
FAR, RIGHT, LEFT, OWN = range(4)
HOPS = (2, 1, -1, 0)
ONE_HOP_F = ()
ONE_HOP_S = ((1, 2),)
LAG = 3
AWAY = 3
ROUTES = 4
N_INPUTS, N_OUTS, N_PROJECT = 8, 3, 12
STAT = SUB


def remote(src, dst, ssem, rsem, dev):
    return pltpu.make_async_remote_copy(src_ref=src, dst_ref=dst, send_sem=ssem, recv_sem=rsem,
                                        device_id=dev, device_id_type=pl.DeviceIdType.MESH)


def meet(peers):
    barrier = pltpu.get_barrier_semaphore()
    for dev in peers:
        pl.semaphore_signal(barrier, inc=1, device_id=dev, device_id_type=pl.DeviceIdType.MESH)
    return barrier


def iota(shape, dim):
    return lax.broadcasted_iota(jnp.int32, shape, dim)


def project(seq_block, kv, enter, len_hbm, hid_hbm, gain_hbm, wq_hbm, wk_hbm, wv_hbm, kc_hbm, vc_hbm,
            kbuf, vbuf, kvq, len_ref, hbuf, gain_raw, gain_ref, nbuf, wbuf,
            sem_l, sem_g, sem_h, sem_w, sem_k, sem_v, sem_s, sem_r):
    batch, d_model = hid_hbm.shape
    n_w = wbuf.shape[0]
    spi, y = lax.axis_index('sp'), lax.axis_index('tp')
    c = spi % 2
    partner = {'tp': y, 'sp': spi + 1 - 2 * c}
    base = spi * seq_block
    rows_h = batch // HID
    seq_rows = seq_block * kv
    per_piece = batch // PIECES
    crow = per_piece * seq_rows

    hid_copies = [pltpu.make_async_copy(hid_hbm.at[pl.ds(i * rows_h, rows_h)], hbuf.at[pl.ds(i * rows_h, rows_h)], sem_h.at[i])
                  for i in range(HID)]
    len_copy = pltpu.make_async_copy(len_hbm, len_ref, sem_l)
    gain_copy = pltpu.make_async_copy(gain_hbm, gain_raw, sem_g)

    def w_copy(j, src, first):
        return pltpu.make_async_copy(src.at[:, pl.ds(first, BLOCK)], wbuf.at[j], sem_w.at[j])

    def q_copy(j):
        return w_copy(j, wq_hbm, pl.multiple_of(c * (n_w - 1) * BLOCK + (j - 1) * BLOCK, BLOCK))

    def cache_copies(p):
        part = pl.ds(pl.multiple_of(p * crow, crow), crow)
        return [pltpu.make_async_copy(src.at[part], buf.at[part], sem)
                for src, buf, sem in ((kc_hbm, kbuf, sem_k), (vc_hbm, vbuf, sem_v))]

    def trade(j):
        slot = kvq.at[c * n_w + j]
        return remote(slot, slot, sem_s, sem_r.at[j], partner)

    def arrival(j):
        slot = kvq.at[(1 - c) * n_w + j]
        return remote(slot, slot, sem_s, sem_r.at[j], partner)

    for cp in hid_copies + [gain_copy, len_copy]:
        cp.start()
    gain_copy.wait()
    gain_ref[...] = gain_raw[...].astype(F32).reshape(gain_ref.shape)
    hid_copies[0].wait()

    q_copy(1).start()

    def kv_start():
        @pl.when(c == 0)
        def _():
            w_copy(0, wk_hbm, 0).start()

        @pl.when(c == 1)
        def _():
            w_copy(0, wv_hbm, 0).start()

    step = 2 * SUB
    wide = SUB * LANES

    def norm_rows(r, carry):
        row = pl.ds(pl.multiple_of(r * step, step), step)
        cuts = [slice(w, w + wide) for w in range(0, d_model, wide)]
        total = jnp.zeros((step, 1), F32)
        for cut in cuts:
            v = hbuf[row, cut].astype(F32)
            total = total + jnp.sum(v * v, axis=1, keepdims=True)
        inv = lax.rsqrt(total / d_model + EPS)
        for cut in cuts:
            nbuf[row, cut] = (hbuf[row, cut].astype(F32) * inv * gain_ref[:, cut]).astype(BF16)
        return carry

    for i in range(HID):
        if i:
            hid_copies[i].wait()
            if i + 1 < n_w:
                q_copy(i + 1).start()
            else:
                kv_start()
        lax.fori_loop(i * rows_h // step, (i + 1) * rows_h // step, norm_rows, 0, unroll=True)
    enter()

    per_step = PIECES // n_w

    def columns(it, carry):
        j = (it + 1) % n_w
        w_copy(j, wk_hbm, 0).wait()
        for i in range(per_step):
            for cp in cache_copies(it * per_step + i):
                cp.start()

        @pl.when(it > 0)
        def _():
            trade(it).start()

        res = jnp.dot(nbuf[...], wbuf[j], preferred_element_type=F32)
        for i in range(BLOCK // LANES):
            kvq[c * n_w + j, pl.ds(i, batch, stride=BLOCK // LANES), :] = res[:, i * LANES:(i + 1) * LANES]
        return carry

    lax.fori_loop(0, n_w, columns, 0)
    trade(0).start()
    len_copy.wait()
    for src, buf, sem in ((kc_hbm, kbuf, sem_k), (vc_hbm, vbuf, sem_v)):
        pltpu.make_async_copy(src, buf, sem).wait()
    for j in range(1, n_w):
        arrival(j).wait_recv()

    pair_row = iota((step, LANES), 0) % kv
    slot_pos = iota((seq_rows, LANES), 0) // kv

    def update(p, carry):
        for i in range(per_piece):
            b = p * per_piece + i
            here = slot_pos == len_ref[b] - base
            rows = pl.ds(pl.multiple_of(b * seq_rows, step), seq_rows)
            for core, buf in enumerate((kbuf, vbuf)):
                new = kvq[core * n_w, pl.ds(b * kv, 1), :]
                for n in range(1, kv):
                    new = jnp.where(pair_row == n, kvq[core * n_w, pl.ds(b * kv + n, 1), :], new)
                new = jnp.concatenate([new.astype(BF16)] * (seq_rows // step), axis=0)
                buf[rows, :] = jnp.where(here, new, buf[rows, :])
        return carry

    def new_tokens():
        lax.fori_loop(0, PIECES, update, 0)
        sent = kvq.at[pl.ds(c * n_w, n_w)]
        remote(sent, sent, sem_s, sem_r.at[0], partner).wait_send()

    return arrival(0).wait_recv, new_tokens


def store_kernel(*refs):
    copies = [pltpu.make_async_copy(refs[i], refs[N_OUTS + i], refs[-1].at[i]) for i in range(N_OUTS)]
    for cp in copies:
        cp.start()
    for cp in copies:
        cp.wait()


def decode_kernel(seq_block, kv, heads, *refs):
    inputs, wo_hbm, outs = refs[:N_INPUTS], refs[N_INPUTS], refs[N_INPUTS + 1:N_INPUTS + N_OUTS + 1]
    kvq, len_ref, hbuf, *rest = refs[N_INPUTS + N_OUTS + 1:]
    kbuf, vbuf, out_ref = outs

    def first(enter):
        return project(seq_block, kv, enter, *inputs, kbuf, vbuf, kvq, len_ref, hbuf, *rest[:N_PROJECT])

    exchange(seq_block, kv, heads, first, kbuf, vbuf, kvq, len_ref, hbuf, wo_hbm, out_ref, *rest[N_PROJECT:])


def exchange(seq_block, kv, heads, first_part, kbuf, vbuf, kvq, len_ref, hbuf, wo_hbm, out_ref,
             score_a, score_b, newest, acc, pbuf, xsend, xrecv, obuf, lhs, wbuf, ysend, yrecv, gbuf,
             sem_w, sem_ps, sem_pr, sem_xs, sem_xr, sem_os, sem_or, sem_ys, sem_yr,
             sem_fs, sem_fr, sem_ss, sem_sr, sem_ds, sem_dr):
    batch, d_model = out_ref.shape
    spi, y = lax.axis_index('sp'), lax.axis_index('tp')
    sp, ny = lax.axis_size('sp'), lax.axis_size('tp')
    nx = sp // 2
    x, c = spi // 2, spi % 2
    base = spi * seq_block
    seq_rows = seq_block * kv
    n_w = kvq.shape[0] // 2
    unit = batch // (sp * SPLITS * 2)
    ur = unit * heads
    rows = batch // nx
    part = rows // (2 * SPLITS)
    half_d = d_model // 2
    cols = half_d // ny
    hc = cols // 2

    def at_x(d):
        return (x + d + nx) % nx

    def at_y(d):
        return (y + d + ny) % ny

    partner = {'tp': y, 'sp': spi + 1 - 2 * c}
    x_dev = {d: {'tp': y, 'sp': at_x(d) * 2 + c} for d in (2, 1, -1)}
    y_dev = {d: {'tp': at_y(d), 'sp': spi} for d in (2, 1, -1)}

    barrier = meet([partner, *x_dev.values(), *y_dev.values()])
    w_copies = []
    for k in range(ROUTES):
        col = pl.multiple_of(c * half_d + at_y(HOPS[k]) * cols, LANES)
        w_copies.append(pltpu.make_async_copy(wo_hbm.at[:, pl.ds(col, cols)], wbuf.at[k], sem_w.at[k]))
    new_arrived, new_tokens = first_part(lambda: pl.semaphore_wait(barrier, 1 + len(x_dev) + len(y_dev)))
    for cp in w_copies:
        cp.start()

    per = BLOCK // LANES
    tile = GROUP * per
    n_tiles = heads // per
    qrows = GROUP * heads
    krows = GROUP * seq_rows
    row_id, col_id = iota((qrows, krows), 0), iota((qrows, krows), 1)
    same = (row_id % tile // per == col_id // seq_rows) & (row_id // (qrows // kv) == col_id % kv)
    col_row = iota((1, krows), 1)
    col_seq = col_row // seq_rows
    col_pos = col_row % seq_rows // kv
    diag = iota((ur, LANES), 0) == iota((ur, LANES), 1)
    fold = LANES ** -0.5 * LOG2E
    halves = [(core, h) for core in range(2) for h in range(2)]
    groups = [(core, h, g) for core, h in halves for g in range(unit // GROUP)]

    def pair(k, n):
        return remote(acc.at[n, k, 1 - c], pbuf.at[n, k], sem_ps.at[n], sem_pr.at[n * ROUTES + k], partner)

    def first(n, k, core, h, g):
        dest = at_x(HOPS[k])
        return (((dest * 2 + core) * SPLITS + n) * 2 + h) * unit + g * GROUP

    def score(n, k, sbuf):
        for at, where in enumerate(groups):
            b0 = first(n, k, *where)
            rows8 = pl.ds(pl.multiple_of(b0 * per, tile), tile)
            q = jnp.concatenate([kvq[core * n_w + j, rows8, :] for core in range(2) for j in range(1, n_w)], axis=0)
            keys = kbuf[pl.ds(pl.multiple_of(b0 * seq_rows, krows), krows), :]
            s = lax.dot_general(q.astype(BF16), keys, (((1,), (1,)), ((), ())), preferred_element_type=F32)
            last = jnp.full((1, krows), len_ref[b0] - base, jnp.int32)
            for i in range(1, GROUP):
                last = jnp.where(col_seq == i, len_ref[b0 + i] - base, last)
            sbuf[at] = jnp.where(same & (col_pos < last), s * fold, NEG_BIG)

    def finish(n, k, sbuf):
        stats = []
        for at, where in enumerate(groups):
            core, h, g = where
            s = sbuf[at]
            m = jnp.maximum(jnp.max(s, axis=1, keepdims=True), FLOOR)
            e = jnp.exp2(s - m)
            stats.append((m, jnp.sum(e, axis=1, keepdims=True)))
            values = vbuf[pl.ds(pl.multiple_of(first(n, k, *where) * seq_rows, krows), krows), :]
            o = jnp.dot(e.astype(BF16), values, preferred_element_type=F32)
            for t in range(n_tiles):
                row = (t * (unit // GROUP) + g) * tile
                acc[n, k, core, h, row:row + tile, :] = o[t * tile:(t + 1) * tile]
        for core, h in halves:
            mine = [stat for where, stat in zip(groups, stats) if where[:2] == (core, h)]
            packed = []
            for which in range(2):
                col = jnp.concatenate([stat[which][t * tile:(t + 1) * tile] for t in range(n_tiles) for stat in mine], axis=0)
                packed.append(jnp.sum(jnp.where(diag, jnp.broadcast_to(col, diag.shape), 0.0), axis=0, keepdims=True))
            packed.append(jnp.zeros((STAT - len(packed), LANES), F32))
            acc[n, k, core, h, ur:ur + STAT, :] = jnp.concatenate(packed, axis=0)
        pair(k, n).start()

    def column(stat):
        return jnp.sum(jnp.where(diag, jnp.broadcast_to(stat, diag.shape), 0.0), axis=1, keepdims=True)

    def merge(refs):
        both = [(r[ur:ur + 1, :], r[ur + 1:ur + 2, :]) for r in refs]
        peak = functools.reduce(jnp.maximum, [m for m, _ in both])
        scale = [jnp.exp2(m - peak) for m, _ in both]
        denom = sum(l * s for (_, l), s in zip(both, scale))
        total = sum(r[:ur, :] * column(s) for r, s in zip(refs, scale))
        return total, peak, denom

    def merge_into(dst, refs):
        total, peak, denom = merge(refs)
        dst[:ur, :] = total
        dst[ur:ur + STAT, :] = jnp.concatenate([peak, denom, jnp.zeros((STAT - 2, LANES), F32)], axis=0)

    def sends(send, recv, ssem, rsem, devs):
        return [[remote(send.at[n, i], recv.at[n, i], ssem.at[n], rsem.at[n * AWAY + i], devs[d])
                 for i, d in enumerate(HOPS[:AWAY])] for n in range(SPLITS)]

    xc = sends(xsend, xrecv, sem_xs, sem_xr, x_dev)
    yc = sends(ysend, yrecv, sem_ys, sem_yr, y_dev)
    oc = [remote(obuf.at[n, c], obuf.at[n, c], sem_os.at[n], sem_or.at[n], partner) for n in range(SPLITS)]

    def both(n, k, h):
        return [acc.at[n, k, c, h], pbuf.at[n, k, h]]

    def x_start(n, k):
        if k == OWN:
            return
        pair(k, n).wait_recv()
        for h in range(2):
            merge_into(xsend.at[n, k, h], both(n, k, h))
        xc[n][k].start()

    def fresh(n):
        two = unit * kv
        parity = iota((two, LANES), 0) % kv
        for h in range(2):
            rows16 = pl.ds(pl.multiple_of((((x * 2 + c) * SPLITS + n) * 2 + h) * two, two), two)
            score_col = []
            for core in range(kv):
                k, v = [jnp.where(parity == core, r, pltpu.roll(r, 1 if core == 0 else two - 1, 0))
                        for r in (kvq[i * n_w, rows16, :].astype(BF16).astype(F32) for i in range(2))]
                for j in range(1, n_w):
                    q = kvq[core * n_w + j, rows16, :].astype(BF16).astype(F32)
                    score_col.append(jnp.sum(q * k, axis=1, keepdims=True) * fold)
                    at = (core * (n_w - 1) + j - 1) * two
                    newest[n, h, at:at + two, :] = v
            col = jnp.broadcast_to(jnp.concatenate(score_col, axis=0), diag.shape)
            peak = jnp.sum(jnp.where(diag, col, 0.0), axis=0, keepdims=True)
            newest[n, h, ur:ur + STAT, :] = jnp.where(iota((STAT, LANES), 0) == 0, jnp.broadcast_to(peak, (STAT, LANES)), 1.0)

    def x_end(n):
        pair(OWN, n).wait_recv()
        for cp in xc[n]:
            cp.wait_recv()
        for h in range(2):
            total, _, denom = merge(both(n, OWN, h) + [newest.at[n, h]] + [xrecv.at[n, i, h] for i in range(AWAY)])
            obuf[n, c, h * ur:(h + 1) * ur, :] = (total / column(denom)).astype(BF16).astype(F32)
        oc[n].start()

    def product(n, k):
        if n == 0:
            w_copies[k].wait()
        return jnp.dot(lhs[n].astype(BF16), wbuf[k], preferred_element_type=F32)

    def y_start(n):
        oc[n].wait_recv()
        for core, h in halves:
            at = core * part + h * unit
            for t in range(n_tiles):
                for i in range(per):
                    head = (t * per + i) * LANES
                    lhs[n, at:at + unit, head:head + LANES] = obuf[
                        n, core, pl.ds(h * ur + t * unit * per + i, unit, stride=per), :]
        for i in range(AWAY):
            prod = product(n, i)
            for h in range(2):
                ysend[n, i, h] = prod[:, h * hc:(h + 1) * hc]
            yc[n][i].start()

    f = x + c * (y - x)
    s = y + c * (x - y)
    def go(copy):
        copy.start()

    def f_dev(d):
        return {'tp': (y + c * d + ny) % ny, 'sp': ((x + (1 - c) * d + nx) % nx) * 2 + c}

    def s_dev(d):
        return {'tp': (y + (1 - c) * d + ny) % ny, 'sp': ((x + c * d + nx) % nx) * 2 + c}

    def block(n, fd, sd):
        return gbuf.at[n, c, (f + fd + nx) % nx, (s + sd + ny) % ny]

    def kind(d, is_half):
        return 2 if d == 2 else is_half * 2 + (d > 0)

    def along(ring, n, fd, sd, d, is_half=False):
        ref = block(n, fd, sd)
        if is_half:
            ref = ref.at[0 if d > 0 else 1]
        if ring == 'f':
            i = n * ROUTES + kind(d, is_half)
            return remote(ref, ref, sem_fs.at[n], sem_fr.at[i], f_dev(d))
        i = (n * nx + fd % nx) * ROUTES + kind(d, is_half)
        return remote(ref, ref, sem_ss.at[n], sem_sr.at[i], s_dev(d))

    def over(n, fd, sd):
        i = (n * nx + fd % nx) * ny + sd % ny
        ref = block(n, fd, sd)
        return remote(ref, ref, sem_ds.at[n], sem_dr.at[i], partner)

    def place(n, ci, fi, si, swap):
        xi, yi = fi + swap * (si - fi), si + swap * (fi - si)
        for h in range(2):
            at = pl.ds(pl.multiple_of(ci * half_d + yi * cols + h * hc, LANES), hc)
            for core in range(2):
                first = pl.multiple_of(xi * rows + (core * SPLITS + n) * part, part)
                out_ref[pl.ds(first, part), at] = gbuf[n, ci, fi, si, h, core * part:(core + 1) * part, :].astype(BF16)

    def place_here(n, fd, sd):
        place(n, c, (f + fd + nx) % nx, (s + sd + ny) % ny, c)

    def spread(n, fd):
        for d in HOPS[:AWAY] if (n, fd) in ONE_HOP_S else (1, -1):
            go(along('s', n, fd, 0, d))
        go(over(n, fd, 0))

    def y_end(n):
        own = product(n, OWN)
        for cp in yc[n]:
            cp.wait_recv()
        for h in range(2):
            total = sum([yrecv[n, i, h] for i in range(AWAY)], own[:, h * hc:(h + 1) * hc])
            at = pl.ds(pl.multiple_of(c * half_d + y * cols + h * hc, LANES), hc)
            kept = jnp.concatenate([hbuf[pl.ds(pl.multiple_of(x * rows + (core * SPLITS + n) * part, part), part), at]
                                    for core in range(2)], axis=0)
            gbuf[n, c, f, s, h] = (kept.astype(F32) + total).astype(BF16).astype(F32)
        for d in (1, -1, 2) if n in ONE_HOP_F else (1, -1):
            go(along('f', n, 0, 0, d))
        spread(n, 0)
        place_here(n, 0, 0)

    def f_ring(n):
        for d in (1, -1):
            along('f', n, -d, 0, d).wait_recv()
            if n not in ONE_HOP_F:
                go(along('f', n, -d, 0, d, True))
            spread(n, -d)
        for d in (1, -1):
            place_here(n, -d, 0)

    def f_end(n):
        if n in ONE_HOP_F:
            along('f', n, 2, 0, 2).wait_recv()
        else:
            for d in (1, -1):
                along('f', n, 2, 0, d, True).wait_recv()
        spread(n, 2)
        place_here(n, 2, 0)

    def s_ring(n, fd):
        for d in (1, -1):
            along('s', n, fd, -d, d).wait_recv()
            if (n, fd) not in ONE_HOP_S:
                go(along('s', n, fd, -d, d, True))
            go(over(n, fd, -d))
        for d in (1, -1):
            place_here(n, fd, -d)

    def s_end(n, fd):
        if (n, fd) in ONE_HOP_S:
            along('s', n, fd, 2, 2).wait_recv()
        else:
            for d in (1, -1):
                along('s', n, fd, 2, d, True).wait_recv()
        go(over(n, fd, 2))
        place_here(n, fd, 2)

    def take(n, fd, sd):
        i = (n * nx + fd % nx) * ny + sd % ny
        fi, si = (s + fd + nx) % nx, (f + sd + ny) % ny
        ref = gbuf.at[n, 1 - c, fi, si]
        remote(ref, ref, sem_ds.at[n], sem_dr.at[i], partner).wait_recv()
        place(n, 1 - c, fi, si, 1 - c)

    def stage(n, i):
        if i == 0:
            f_ring(n)
            s_ring(n, 0)
        elif i == 1:
            f_end(n)
            s_ring(n, -1)
            s_ring(n, 1)
            s_end(n, 0)
        elif i == 2:
            for fd in (0, -1, 1):
                take(n, fd, 0)
            s_ring(n, 2)
            s_end(n, -1)
            s_end(n, 1)
        else:
            for fd, sd in ((2, 0), (0, -1), (0, 1), (0, 2), (-1, -1), (-1, 1), (1, -1), (1, 1)):
                take(n, fd, sd)
            s_end(n, 2)

    scores = (score_a, score_b)
    steps = [(n, k) for n in range(SPLITS) for k in range(ROUTES)]
    score(*steps[0], scores[0])
    for i, step in enumerate(steps):
        if i + 1 < len(steps):
            score(*steps[i + 1], scores[(i + 1) % 2])
        finish(*step, scores[i % 2])
        if i >= LAG:
            x_start(*steps[i - LAG])
    for step in steps[-LAG:]:
        x_start(*step)
    new_arrived()
    for n in range(SPLITS):
        fresh(n)
    new_tokens()
    x_end(0)
    y_start(0)
    x_end(1)
    y_start(1)
    y_end(0)
    y_end(1)
    for i in range(ROUTES):
        for n in range(SPLITS):
            stage(n, i)
    for n in range(SPLITS):
        for fd, sd in ((2, -1), (2, 1), (-1, 2), (1, 2), (2, 2)):
            take(n, fd, sd)
    for n in range(SPLITS):
        done = ((acc.at[n, :, 1 - c], sem_ps), (xsend.at[n], sem_xs), (obuf.at[n, c], sem_os), (ysend.at[n], sem_ys),
                (gbuf.at[n, c, 0, pl.ds(0, AWAY)], sem_fs), (gbuf.at[n, c, pl.ds(0, AWAY)], sem_ss), (gbuf.at[n, c], sem_ds))
        for ref, sem in done:
            remote(ref, ref, sem.at[n], sem_or.at[n], partner).wait_send()


def solution(mesh):
    cache_spec = P('dp', 'sp', 'tp', None)
    sp = mesh.shape['sp']
    tp = mesh.shape['tp']

    def local_step(hidden, lengths, k_cache, v_cache, norm_gain, w_query, w_key, w_value, w_out):
        batch, seq_block, kv, head_dim = k_cache.shape
        d_model = hidden.shape[1]
        width = w_query.shape[1]
        heads = width // head_dim
        n_w = width // (2 * BLOCK) + 1
        flat = batch * seq_block * kv
        hbm = pl.BlockSpec(memory_space=pltpu.HBM)
        vmem = pl.BlockSpec(memory_space=pltpu.VMEM)
        shape = jax.ShapeDtypeStruct
        buf = pltpu.VMEM

        def dma(*shapes):
            return [pltpu.SemaphoreType.DMA(s) if s else pltpu.SemaphoreType.DMA for s in shapes]

        nx = sp // 2
        rows = batch // nx
        cols = d_model // (2 * tp)
        ur = batch // (sp * SPLITS * 2) * heads
        scored = buf((batch // (ROUTES * SPLITS * GROUP), GROUP * heads, GROUP * seq_block * kv), F32)
        travel = buf((SPLITS, AWAY, 2, ur + STAT, head_dim), F32)
        yblock = buf((SPLITS, AWAY, 2, rows // SPLITS, cols // 2), F32)
        n_x, n_f = SPLITS * AWAY, SPLITS * ROUTES
        n_s = n_f * nx
        n_d = SPLITS * nx * tp
        split = (SPLITS,)
        k_new, v_new, out = pl.pallas_call(
            functools.partial(decode_kernel, seq_block, kv, heads),
            out_shape=(buf((flat, head_dim), BF16), buf((flat, head_dim), BF16), buf((batch, d_model), BF16)),
            in_specs=[hbm] * (N_INPUTS + 1),
            out_specs=(vmem, vmem, vmem),
            scratch_shapes=[
                buf((2 * n_w, batch * BLOCK // head_dim, head_dim), F32),
                pltpu.SMEM((batch,), jnp.int32),
                buf((batch, d_model), BF16),
                buf((d_model,), BF16),
                buf((1, d_model), F32),
                buf((batch, d_model), BF16),
                buf((n_w, d_model, BLOCK), BF16),
                *dma((), (), (HID,), (n_w,), (), (), (), (n_w,)),
                scored, scored,
                buf((SPLITS, 2, ur + STAT, head_dim), F32),
                buf((SPLITS, ROUTES, 2, 2, ur + STAT, head_dim), F32),
                buf((SPLITS, ROUTES, 2, ur + STAT, head_dim), F32),
                travel, travel,
                buf((SPLITS, 2, 2 * ur, head_dim), F32),
                buf((SPLITS, rows // SPLITS, width), F32),
                buf((ROUTES, width, cols), BF16),
                yblock, yblock,
                buf((SPLITS, 2, nx, tp, 2, rows // SPLITS, cols // 2), F32),
                *dma((ROUTES,), split, (n_f,), split, (n_x,), split, split, split, (n_x,),
                     split, (n_f,), split, (n_s,), split, (n_d,)),
            ],
            compiler_params=pltpu.CompilerParams(collective_id=0, has_side_effects=True, vmem_limit_bytes=VMEM_MIB * MIB),
            name='decode_step',
        )(lengths, hidden, norm_gain, w_query, w_key, w_value,
          k_cache.reshape(flat, head_dim), v_cache.reshape(flat, head_dim), w_out)
        results = (k_new, v_new, out)
        k_new, v_new, out = pl.pallas_call(
            store_kernel,
            out_shape=tuple(shape(r.shape, r.dtype) for r in results),
            in_specs=[vmem] * N_OUTS,
            out_specs=(hbm,) * N_OUTS,
            scratch_shapes=dma((N_OUTS,)),
            compiler_params=pltpu.CompilerParams(vmem_limit_bytes=MIB),
            name='store',
        )(*results)
        return out, k_new.reshape(k_cache.shape), v_new.reshape(v_cache.shape)

    return jax.shard_map(
        local_step,
        mesh=mesh,
        in_specs=(P('dp', None), P('dp'), cache_spec, cache_spec, P(None), P(None, 'tp'), P(None, 'tp'), P(None, 'tp'), P('tp', None)),
        out_specs=(P('dp', None), cache_spec, cache_spec),
        check_vma=False,
    )
```

```python
import functools
import math

import jax
import jax.numpy as jnp
from jax import lax
from jax.experimental import pallas as pl
from jax.experimental.pallas import tpu as pltpu
from jax.sharding import PartitionSpec as P

EPS = 1e-6
NEG_BIG = -1e30
FLOOR = -0.999e30
LOG2E = math.log2(math.e)
MIB = 1 << 20
VMEM_MIB = 52
F32 = jnp.float32
BF16 = jnp.bfloat16
LANES = 128
SUB = 8
BLOCK = 256
GROUP = 4
SPLITS = 2
PIECES = 16
HID = 4
OWN = 3
HOPS = (1, 2, -1, 0)
ONE_HOP_F = ()
ONE_HOP_S = ((1, 2),)
LAG = 3
AWAY = 3
ROUTES = 4
N_INPUTS, N_OUTS, N_PROJECT = 8, 3, 12
STAT = SUB


def remote(src, dst, ssem, rsem, dev):
    return pltpu.make_async_remote_copy(src_ref=src, dst_ref=dst, send_sem=ssem, recv_sem=rsem,
                                        device_id=dev, device_id_type=pl.DeviceIdType.MESH)


def meet(peers):
    barrier = pltpu.get_barrier_semaphore()
    for dev in peers:
        pl.semaphore_signal(barrier, inc=1, device_id=dev, device_id_type=pl.DeviceIdType.MESH)
    return barrier


def iota(shape, dim):
    return lax.broadcasted_iota(jnp.int32, shape, dim)


def project(seq_block, kv, enter, len_hbm, hid_hbm, gain_hbm, wq_hbm, wk_hbm, wv_hbm, kc_hbm, vc_hbm,
            kbuf, vbuf, kvq, len_ref, hbuf, gain_raw, gain_ref, nbuf, wbuf,
            sem_l, sem_g, sem_h, sem_w, sem_k, sem_v, sem_s, sem_r):
    batch, d_model = hid_hbm.shape
    n_w = wbuf.shape[0]
    spi, y = lax.axis_index('sp'), lax.axis_index('tp')
    c = spi % 2
    partner = {'tp': y, 'sp': spi + 1 - 2 * c}
    base = spi * seq_block
    rows_h = batch // HID
    seq_rows = seq_block * kv
    per_piece = batch // PIECES
    crow = per_piece * seq_rows

    hid_copies = [pltpu.make_async_copy(hid_hbm.at[pl.ds(i * rows_h, rows_h)], hbuf.at[pl.ds(i * rows_h, rows_h)], sem_h.at[i])
                  for i in range(HID)]
    len_copy = pltpu.make_async_copy(len_hbm, len_ref, sem_l)
    gain_copy = pltpu.make_async_copy(gain_hbm, gain_raw, sem_g)

    def w_copy(j, src, first):
        return pltpu.make_async_copy(src.at[:, pl.ds(first, BLOCK)], wbuf.at[j], sem_w.at[j])

    def q_copy(j):
        return w_copy(j, wq_hbm, pl.multiple_of(c * (n_w - 1) * BLOCK + (j - 1) * BLOCK, BLOCK))

    def cache_copies(p):
        part = pl.ds(pl.multiple_of(p * crow, crow), crow)
        return [pltpu.make_async_copy(src.at[part], buf.at[part], sem)
                for src, buf, sem in ((kc_hbm, kbuf, sem_k), (vc_hbm, vbuf, sem_v))]

    def trade(j):
        slot = kvq.at[c * n_w + j]
        return remote(slot, slot, sem_s, sem_r.at[j], partner)

    def arrival(j):
        slot = kvq.at[(1 - c) * n_w + j]
        return remote(slot, slot, sem_s, sem_r.at[j], partner)

    for cp in hid_copies + [gain_copy, len_copy]:
        cp.start()
    gain_copy.wait()
    gain_ref[...] = gain_raw[...].astype(F32).reshape(gain_ref.shape)
    hid_copies[0].wait()

    q_copy(1).start()

    def kv_start():
        @pl.when(c == 0)
        def _():
            w_copy(0, wk_hbm, 0).start()

        @pl.when(c == 1)
        def _():
            w_copy(0, wv_hbm, 0).start()

    step = 2 * SUB
    wide = SUB * LANES

    def norm_rows(r, carry):
        row = pl.ds(pl.multiple_of(r * step, step), step)
        cuts = [slice(w, w + wide) for w in range(0, d_model, wide)]
        total = jnp.zeros((step, 1), F32)
        for cut in cuts:
            v = hbuf[row, cut].astype(F32)
            total = total + jnp.sum(v * v, axis=1, keepdims=True)
        inv = lax.rsqrt(total / d_model + EPS)
        for cut in cuts:
            nbuf[row, cut] = (hbuf[row, cut].astype(F32) * inv * gain_ref[:, cut]).astype(BF16)
        return carry

    for i in range(HID):
        if i:
            hid_copies[i].wait()
            if i + 1 < n_w:
                q_copy(i + 1).start()
            else:
                kv_start()
        lax.fori_loop(i * rows_h // step, (i + 1) * rows_h // step, norm_rows, 0, unroll=True)
    enter()

    per_step = PIECES // n_w

    def columns(it, carry):
        j = (it + 1) % n_w
        w_copy(j, wk_hbm, 0).wait()
        for i in range(per_step):
            for cp in cache_copies(it * per_step + i):
                cp.start()

        @pl.when(it > 0)
        def _():
            trade(it).start()

        res = jnp.dot(nbuf[...], wbuf[j], preferred_element_type=F32)
        for i in range(BLOCK // LANES):
            kvq[c * n_w + j, pl.ds(i, batch, stride=BLOCK // LANES), :] = res[:, i * LANES:(i + 1) * LANES]
        return carry

    lax.fori_loop(0, n_w, columns, 0)
    trade(0).start()
    len_copy.wait()
    for src, buf, sem in ((kc_hbm, kbuf, sem_k), (vc_hbm, vbuf, sem_v)):
        pltpu.make_async_copy(src, buf, sem).wait()
    for j in range(1, n_w):
        arrival(j).wait_recv()

    pair_row = iota((step, LANES), 0) % kv
    slot_pos = iota((seq_rows, LANES), 0) // kv

    def update(p, carry):
        for i in range(per_piece):
            b = p * per_piece + i
            here = slot_pos == len_ref[b] - base
            rows = pl.ds(pl.multiple_of(b * seq_rows, step), seq_rows)
            for core, buf in enumerate((kbuf, vbuf)):
                new = kvq[core * n_w, pl.ds(b * kv, 1), :]
                for n in range(1, kv):
                    new = jnp.where(pair_row == n, kvq[core * n_w, pl.ds(b * kv + n, 1), :], new)
                new = jnp.concatenate([new.astype(BF16)] * (seq_rows // step), axis=0)
                buf[rows, :] = jnp.where(here, new, buf[rows, :])
        return carry

    def new_tokens():
        lax.fori_loop(0, PIECES, update, 0)
        sent = kvq.at[pl.ds(c * n_w, n_w)]
        remote(sent, sent, sem_s, sem_r.at[0], partner).wait_send()

    return arrival(0).wait_recv, new_tokens


def store_kernel(*refs):
    copies = [pltpu.make_async_copy(refs[i], refs[N_OUTS + i], refs[-1].at[i]) for i in range(N_OUTS)]
    for cp in copies:
        cp.start()
    for cp in copies:
        cp.wait()


def decode_kernel(seq_block, kv, heads, *refs):
    inputs, wo_hbm, outs = refs[:N_INPUTS], refs[N_INPUTS], refs[N_INPUTS + 1:N_INPUTS + N_OUTS + 1]
    kvq, len_ref, hbuf, *rest = refs[N_INPUTS + N_OUTS + 1:]
    kbuf, vbuf, out_ref = outs

    def first(enter):
        return project(seq_block, kv, enter, *inputs, kbuf, vbuf, kvq, len_ref, hbuf, *rest[:N_PROJECT])

    exchange(seq_block, kv, heads, first, kbuf, vbuf, kvq, len_ref, hbuf, wo_hbm, out_ref, *rest[N_PROJECT:])


def exchange(seq_block, kv, heads, first_part, kbuf, vbuf, kvq, len_ref, hbuf, wo_hbm, out_ref,
             score_a, score_b, newest, acc, pbuf, xsend, xrecv, obuf, lhs, wbuf, ysend, yrecv, gbuf,
             sem_w, sem_ps, sem_pr, sem_xs, sem_xr, sem_os, sem_or, sem_ys, sem_yr,
             sem_fs, sem_fr, sem_ss, sem_sr, sem_ds, sem_dr):
    batch, d_model = out_ref.shape
    spi, y = lax.axis_index('sp'), lax.axis_index('tp')
    sp, ny = lax.axis_size('sp'), lax.axis_size('tp')
    nx = sp // 2
    x, c = spi // 2, spi % 2
    base = spi * seq_block
    seq_rows = seq_block * kv
    n_w = kvq.shape[0] // 2
    unit = batch // (sp * SPLITS * 2)
    ur = unit * heads
    rows = batch // nx
    part = rows // (2 * SPLITS)
    half_d = d_model // 2
    cols = half_d // ny
    hc = cols // 2

    def at_x(d):
        return (x + d + nx) % nx

    def at_y(d):
        return (y + d + ny) % ny

    partner = {'tp': y, 'sp': spi + 1 - 2 * c}
    x_dev = {d: {'tp': y, 'sp': at_x(d) * 2 + c} for d in (2, 1, -1)}
    y_dev = {d: {'tp': at_y(d), 'sp': spi} for d in (2, 1, -1)}

    barrier = meet([partner, *x_dev.values(), *y_dev.values()])
    w_copies = []
    for k in range(ROUTES):
        col = pl.multiple_of(c * half_d + at_y(HOPS[k]) * cols, LANES)
        w_copies.append(pltpu.make_async_copy(wo_hbm.at[:, pl.ds(col, cols)], wbuf.at[k], sem_w.at[k]))
    new_arrived, new_tokens = first_part(lambda: pl.semaphore_wait(barrier, 1 + len(x_dev) + len(y_dev)))
    for cp in w_copies:
        cp.start()

    per = BLOCK // LANES
    tile = GROUP * per
    n_tiles = heads // per
    qrows = GROUP * heads
    krows = GROUP * seq_rows
    row_id, col_id = iota((qrows, krows), 0), iota((qrows, krows), 1)
    same = (row_id % tile // per == col_id // seq_rows) & (row_id // (qrows // kv) == col_id % kv)
    col_row = iota((1, krows), 1)
    col_seq = col_row // seq_rows
    col_pos = col_row % seq_rows // kv
    diag = iota((ur, LANES), 0) == iota((ur, LANES), 1)
    fold = LANES ** -0.5 * LOG2E
    halves = [(core, h) for core in range(2) for h in range(2)]
    groups = [(core, h, g) for core, h in halves for g in range(unit // GROUP)]

    def pair(k, n):
        return remote(acc.at[n, k, 1 - c], pbuf.at[n, k], sem_ps.at[n], sem_pr.at[n * ROUTES + k], partner)

    def first(n, k, core, h, g):
        dest = at_x(HOPS[k])
        return (((dest * 2 + core) * SPLITS + n) * 2 + h) * unit + g * GROUP

    def score(n, k, sbuf):
        for at, where in enumerate(groups):
            b0 = first(n, k, *where)
            rows8 = pl.ds(pl.multiple_of(b0 * per, tile), tile)
            q = jnp.concatenate([kvq[core * n_w + j, rows8, :] for core in range(2) for j in range(1, n_w)], axis=0)
            keys = kbuf[pl.ds(pl.multiple_of(b0 * seq_rows, krows), krows), :]
            s = lax.dot_general(q.astype(BF16), keys, (((1,), (1,)), ((), ())), preferred_element_type=F32)
            last = jnp.full((1, krows), len_ref[b0] - base, jnp.int32)
            for i in range(1, GROUP):
                last = jnp.where(col_seq == i, len_ref[b0 + i] - base, last)
            sbuf[at] = jnp.where(same & (col_pos < last), s * fold, NEG_BIG)

    def finish(n, k, sbuf):
        stats = []
        for at, where in enumerate(groups):
            core, h, g = where
            s = sbuf[at]
            m = jnp.maximum(jnp.max(s, axis=1, keepdims=True), FLOOR)
            e = jnp.exp2(s - m)
            stats.append((m, jnp.sum(e, axis=1, keepdims=True)))
            values = vbuf[pl.ds(pl.multiple_of(first(n, k, *where) * seq_rows, krows), krows), :]
            o = jnp.dot(e.astype(BF16), values, preferred_element_type=F32)
            for t in range(n_tiles):
                row = (t * (unit // GROUP) + g) * tile
                acc[n, k, core, h, row:row + tile, :] = o[t * tile:(t + 1) * tile]
        for core, h in halves:
            mine = [stat for where, stat in zip(groups, stats) if where[:2] == (core, h)]
            packed = []
            for which in range(2):
                col = jnp.concatenate([stat[which][t * tile:(t + 1) * tile] for t in range(n_tiles) for stat in mine], axis=0)
                packed.append(jnp.sum(jnp.where(diag, jnp.broadcast_to(col, diag.shape), 0.0), axis=0, keepdims=True))
            packed.append(jnp.zeros((STAT - len(packed), LANES), F32))
            acc[n, k, core, h, ur:ur + STAT, :] = jnp.concatenate(packed, axis=0)
        pair(k, n).start()

    def column(stat):
        return jnp.sum(jnp.where(diag, jnp.broadcast_to(stat, diag.shape), 0.0), axis=1, keepdims=True)

    def merge(refs):
        both = [(r[ur:ur + 1, :], r[ur + 1:ur + 2, :]) for r in refs]
        peak = functools.reduce(jnp.maximum, [m for m, _ in both])
        scale = [jnp.exp2(m - peak) for m, _ in both]
        denom = sum(l * s for (_, l), s in zip(both, scale))
        total = sum(r[:ur, :] * column(s) for r, s in zip(refs, scale))
        return total, peak, denom

    def merge_into(dst, refs):
        total, peak, denom = merge(refs)
        dst[:ur, :] = total
        dst[ur:ur + STAT, :] = jnp.concatenate([peak, denom, jnp.zeros((STAT - 2, LANES), F32)], axis=0)

    def sends(send, recv, ssem, rsem, devs):
        return [[remote(send.at[n, i], recv.at[n, i], ssem.at[n], rsem.at[n * AWAY + i], devs[d])
                 for i, d in enumerate(HOPS[:AWAY])] for n in range(SPLITS)]

    xc = sends(xsend, xrecv, sem_xs, sem_xr, x_dev)
    yc = sends(ysend, yrecv, sem_ys, sem_yr, y_dev)
    oc = [remote(obuf.at[n, c], obuf.at[n, c], sem_os.at[n], sem_or.at[n], partner) for n in range(SPLITS)]

    def both(n, k, h):
        return [acc.at[n, k, c, h], pbuf.at[n, k, h]]

    def x_start(n, k):
        if k == OWN:
            return
        pair(k, n).wait_recv()
        for h in range(2):
            merge_into(xsend.at[n, k, h], both(n, k, h))
        xc[n][k].start()

    def fresh(n):
        two = unit * kv
        parity = iota((two, LANES), 0) % kv
        for h in range(2):
            rows16 = pl.ds(pl.multiple_of((((x * 2 + c) * SPLITS + n) * 2 + h) * two, two), two)
            score_col = []
            for core in range(kv):
                k, v = [jnp.where(parity == core, r, pltpu.roll(r, 1 if core == 0 else two - 1, 0))
                        for r in (kvq[i * n_w, rows16, :].astype(BF16).astype(F32) for i in range(2))]
                for j in range(1, n_w):
                    q = kvq[core * n_w + j, rows16, :].astype(BF16).astype(F32)
                    score_col.append(jnp.sum(q * k, axis=1, keepdims=True) * fold)
                    at = (core * (n_w - 1) + j - 1) * two
                    newest[n, h, at:at + two, :] = v
            col = jnp.broadcast_to(jnp.concatenate(score_col, axis=0), diag.shape)
            peak = jnp.sum(jnp.where(diag, col, 0.0), axis=0, keepdims=True)
            newest[n, h, ur:ur + STAT, :] = jnp.where(iota((STAT, LANES), 0) == 0, jnp.broadcast_to(peak, (STAT, LANES)), 1.0)

    def x_end(n):
        pair(OWN, n).wait_recv()
        for cp in xc[n]:
            cp.wait_recv()
        for h in range(2):
            total, _, denom = merge(both(n, OWN, h) + [newest.at[n, h]] + [xrecv.at[n, i, h] for i in range(AWAY)])
            obuf[n, c, h * ur:(h + 1) * ur, :] = (total / column(denom)).astype(BF16).astype(F32)
        oc[n].start()

    def product(n, k):
        if n == 0:
            w_copies[k].wait()
        return jnp.dot(lhs[n].astype(BF16), wbuf[k], preferred_element_type=F32)

    def y_start(n):
        oc[n].wait_recv()
        for core, h in halves:
            at = core * part + h * unit
            for t in range(n_tiles):
                for i in range(per):
                    head = (t * per + i) * LANES
                    lhs[n, at:at + unit, head:head + LANES] = obuf[
                        n, core, pl.ds(h * ur + t * unit * per + i, unit, stride=per), :]
        for i in range(AWAY):
            prod = product(n, i)
            for h in range(2):
                ysend[n, i, h] = prod[:, h * hc:(h + 1) * hc]
            yc[n][i].start()

    f = x + c * (y - x)
    s = y + c * (x - y)
    def go(copy):
        copy.start()

    def f_dev(d):
        return {'tp': (y + c * d + ny) % ny, 'sp': ((x + (1 - c) * d + nx) % nx) * 2 + c}

    def s_dev(d):
        return {'tp': (y + (1 - c) * d + ny) % ny, 'sp': ((x + c * d + nx) % nx) * 2 + c}

    def block(n, fd, sd):
        return gbuf.at[n, c, (f + fd + nx) % nx, (s + sd + ny) % ny]

    def kind(d, is_half):
        return 2 if d == 2 else is_half * 2 + (d > 0)

    def along(ring, n, fd, sd, d, is_half=False):
        ref = block(n, fd, sd)
        if is_half:
            ref = ref.at[0 if d > 0 else 1]
        if ring == 'f':
            i = n * ROUTES + kind(d, is_half)
            return remote(ref, ref, sem_fs.at[n], sem_fr.at[i], f_dev(d))
        i = (n * nx + fd % nx) * ROUTES + kind(d, is_half)
        return remote(ref, ref, sem_ss.at[n], sem_sr.at[i], s_dev(d))

    def over(n, fd, sd):
        i = (n * nx + fd % nx) * ny + sd % ny
        ref = block(n, fd, sd)
        return remote(ref, ref, sem_ds.at[n], sem_dr.at[i], partner)

    def place(n, ci, fi, si, swap):
        xi, yi = fi + swap * (si - fi), si + swap * (fi - si)
        for h in range(2):
            at = pl.ds(pl.multiple_of(ci * half_d + yi * cols + h * hc, LANES), hc)
            for core in range(2):
                first = pl.multiple_of(xi * rows + (core * SPLITS + n) * part, part)
                out_ref[pl.ds(first, part), at] = gbuf[n, ci, fi, si, h, core * part:(core + 1) * part, :].astype(BF16)

    def place_here(n, fd, sd):
        place(n, c, (f + fd + nx) % nx, (s + sd + ny) % ny, c)

    def spread(n, fd):
        for d in HOPS[:AWAY] if (n, fd) in ONE_HOP_S else (1, -1):
            go(along('s', n, fd, 0, d))
        go(over(n, fd, 0))

    def y_end(n):
        own = product(n, OWN)
        for cp in yc[n]:
            cp.wait_recv()
        for h in range(2):
            total = sum([yrecv[n, i, h] for i in range(AWAY)], own[:, h * hc:(h + 1) * hc])
            at = pl.ds(pl.multiple_of(c * half_d + y * cols + h * hc, LANES), hc)
            kept = jnp.concatenate([hbuf[pl.ds(pl.multiple_of(x * rows + (core * SPLITS + n) * part, part), part), at]
                                    for core in range(2)], axis=0)
            gbuf[n, c, f, s, h] = (kept.astype(F32) + total).astype(BF16).astype(F32)
        for d in (1, -1, 2) if n in ONE_HOP_F else (1, -1):
            go(along('f', n, 0, 0, d))
        spread(n, 0)
        place_here(n, 0, 0)

    def f_ring(n):
        for d in (1, -1):
            along('f', n, -d, 0, d).wait_recv()
            if n not in ONE_HOP_F:
                go(along('f', n, -d, 0, d, True))
            spread(n, -d)
        for d in (1, -1):
            place_here(n, -d, 0)

    def f_end(n):
        if n in ONE_HOP_F:
            along('f', n, 2, 0, 2).wait_recv()
        else:
            for d in (1, -1):
                along('f', n, 2, 0, d, True).wait_recv()
        spread(n, 2)
        place_here(n, 2, 0)

    def s_ring(n, fd):
        for d in (1, -1):
            along('s', n, fd, -d, d).wait_recv()
            if (n, fd) not in ONE_HOP_S:
                go(along('s', n, fd, -d, d, True))
            go(over(n, fd, -d))
        for d in (1, -1):
            place_here(n, fd, -d)

    def s_end(n, fd):
        if (n, fd) in ONE_HOP_S:
            along('s', n, fd, 2, 2).wait_recv()
        else:
            for d in (1, -1):
                along('s', n, fd, 2, d, True).wait_recv()
        go(over(n, fd, 2))
        place_here(n, fd, 2)

    def take(n, fd, sd):
        i = (n * nx + fd % nx) * ny + sd % ny
        fi, si = (s + fd + nx) % nx, (f + sd + ny) % ny
        ref = gbuf.at[n, 1 - c, fi, si]
        remote(ref, ref, sem_ds.at[n], sem_dr.at[i], partner).wait_recv()
        place(n, 1 - c, fi, si, 1 - c)

    def stage(n, i):
        if i == 0:
            f_ring(n)
            s_ring(n, 0)
        elif i == 1:
            f_end(n)
            s_ring(n, -1)
            s_ring(n, 1)
            s_end(n, 0)
        elif i == 2:
            for fd in (0, -1, 1):
                take(n, fd, 0)
            s_ring(n, 2)
            s_end(n, -1)
            s_end(n, 1)
        else:
            for fd, sd in ((2, 0), (0, -1), (0, 1), (0, 2), (-1, -1), (-1, 1), (1, -1), (1, 1)):
                take(n, fd, sd)
            s_end(n, 2)

    scores = (score_a, score_b)
    steps = [(n, k) for n in range(SPLITS) for k in range(ROUTES)]
    score(*steps[0], scores[0])
    for i, step in enumerate(steps):
        if i + 1 < len(steps):
            score(*steps[i + 1], scores[(i + 1) % 2])
        finish(*step, scores[i % 2])
        if i >= LAG:
            x_start(*steps[i - LAG])
    for step in steps[-LAG:]:
        x_start(*step)
    new_arrived()
    for n in range(SPLITS):
        fresh(n)
    new_tokens()
    x_end(0)
    y_start(0)
    x_end(1)
    y_start(1)
    y_end(0)
    y_end(1)
    for i in range(ROUTES):
        for n in range(SPLITS):
            stage(n, i)
    for n in range(SPLITS):
        for fd, sd in ((2, -1), (2, 1), (-1, 2), (1, 2), (2, 2)):
            take(n, fd, sd)
    for n in range(SPLITS):
        done = ((acc.at[n, :, 1 - c], sem_ps), (xsend.at[n], sem_xs), (obuf.at[n, c], sem_os), (ysend.at[n], sem_ys),
                (gbuf.at[n, c, 0, pl.ds(0, AWAY)], sem_fs), (gbuf.at[n, c, pl.ds(0, AWAY)], sem_ss), (gbuf.at[n, c], sem_ds))
        for ref, sem in done:
            remote(ref, ref, sem.at[n], sem_or.at[n], partner).wait_send()


def solution(mesh):
    cache_spec = P('dp', 'sp', 'tp', None)
    sp = mesh.shape['sp']
    tp = mesh.shape['tp']

    def local_step(hidden, lengths, k_cache, v_cache, norm_gain, w_query, w_key, w_value, w_out):
        batch, seq_block, kv, head_dim = k_cache.shape
        d_model = hidden.shape[1]
        width = w_query.shape[1]
        heads = width // head_dim
        n_w = width // (2 * BLOCK) + 1
        flat = batch * seq_block * kv
        hbm = pl.BlockSpec(memory_space=pltpu.HBM)
        vmem = pl.BlockSpec(memory_space=pltpu.VMEM)
        shape = jax.ShapeDtypeStruct
        buf = pltpu.VMEM

        def dma(*shapes):
            return [pltpu.SemaphoreType.DMA(s) if s else pltpu.SemaphoreType.DMA for s in shapes]

        nx = sp // 2
        rows = batch // nx
        cols = d_model // (2 * tp)
        ur = batch // (sp * SPLITS * 2) * heads
        scored = buf((batch // (ROUTES * SPLITS * GROUP), GROUP * heads, GROUP * seq_block * kv), F32)
        travel = buf((SPLITS, AWAY, 2, ur + STAT, head_dim), F32)
        yblock = buf((SPLITS, AWAY, 2, rows // SPLITS, cols // 2), F32)
        n_x, n_f = SPLITS * AWAY, SPLITS * ROUTES
        n_s = n_f * nx
        n_d = SPLITS * nx * tp
        split = (SPLITS,)
        k_new, v_new, out = pl.pallas_call(
            functools.partial(decode_kernel, seq_block, kv, heads),
            out_shape=(buf((flat, head_dim), BF16), buf((flat, head_dim), BF16), buf((batch, d_model), BF16)),
            in_specs=[hbm] * (N_INPUTS + 1),
            out_specs=(vmem, vmem, vmem),
            scratch_shapes=[
                buf((2 * n_w, batch * BLOCK // head_dim, head_dim), F32),
                pltpu.SMEM((batch,), jnp.int32),
                buf((batch, d_model), BF16),
                buf((d_model,), BF16),
                buf((1, d_model), F32),
                buf((batch, d_model), BF16),
                buf((n_w, d_model, BLOCK), BF16),
                *dma((), (), (HID,), (n_w,), (), (), (), (n_w,)),
                scored, scored,
                buf((SPLITS, 2, ur + STAT, head_dim), F32),
                buf((SPLITS, ROUTES, 2, 2, ur + STAT, head_dim), F32),
                buf((SPLITS, ROUTES, 2, ur + STAT, head_dim), F32),
                travel, travel,
                buf((SPLITS, 2, 2 * ur, head_dim), F32),
                buf((SPLITS, rows // SPLITS, width), F32),
                buf((ROUTES, width, cols), BF16),
                yblock, yblock,
                buf((SPLITS, 2, nx, tp, 2, rows // SPLITS, cols // 2), F32),
                *dma((ROUTES,), split, (n_f,), split, (n_x,), split, split, split, (n_x,),
                     split, (n_f,), split, (n_s,), split, (n_d,)),
            ],
            compiler_params=pltpu.CompilerParams(collective_id=0, has_side_effects=True, vmem_limit_bytes=VMEM_MIB * MIB),
            name='decode_step',
        )(lengths, hidden, norm_gain, w_query, w_key, w_value,
          k_cache.reshape(flat, head_dim), v_cache.reshape(flat, head_dim), w_out)
        results = (k_new, v_new, out)
        k_new, v_new, out = pl.pallas_call(
            store_kernel,
            out_shape=tuple(shape(r.shape, r.dtype) for r in results),
            in_specs=[vmem] * N_OUTS,
            out_specs=(hbm,) * N_OUTS,
            scratch_shapes=dma((N_OUTS,)),
            compiler_params=pltpu.CompilerParams(vmem_limit_bytes=MIB),
            name='store',
        )(*results)
        return out, k_new.reshape(k_cache.shape), v_new.reshape(v_cache.shape)

    return jax.shard_map(
        local_step,
        mesh=mesh,
        in_specs=(P('dp', None), P('dp'), cache_spec, cache_spec, P(None), P(None, 'tp'), P(None, 'tp'), P(None, 'tp'), P('tp', None)),
        out_specs=(P('dp', None), cache_spec, cache_spec),
        check_vma=False,
    )
```

```python
import functools
import math

import jax
import jax.numpy as jnp
from jax import lax
from jax.experimental import pallas as pl
from jax.experimental.pallas import tpu as pltpu
from jax.sharding import PartitionSpec as P

EPS = 1e-6
NEG_BIG = -1e30
FLOOR = -0.999e30
LOG2E = math.log2(math.e)
MIB = 1 << 20
VMEM_MIB = 52
F32 = jnp.float32
BF16 = jnp.bfloat16
LANES = 128
SUB = 8
BLOCK = 256
GROUP = 4
SPLITS = 2
PIECES = 16
HID = 4
OWN = 3
HOPS = (1, 2, -1, 0)
ONE_HOP_F = ()
ONE_HOP_S = ((1, 2),)
LAG = 3
AWAY = 3
ROUTES = 4
N_INPUTS, N_OUTS, N_PROJECT = 8, 3, 12
STAT = SUB


def remote(src, dst, ssem, rsem, dev):
    return pltpu.make_async_remote_copy(src_ref=src, dst_ref=dst, send_sem=ssem, recv_sem=rsem,
                                        device_id=dev, device_id_type=pl.DeviceIdType.MESH)


def meet(peers):
    barrier = pltpu.get_barrier_semaphore()
    for dev in peers:
        pl.semaphore_signal(barrier, inc=1, device_id=dev, device_id_type=pl.DeviceIdType.MESH)
    return barrier


def iota(shape, dim):
    return lax.broadcasted_iota(jnp.int32, shape, dim)


def project(seq_block, kv, enter, len_hbm, hid_hbm, gain_hbm, wq_hbm, wk_hbm, wv_hbm, kc_hbm, vc_hbm,
            kbuf, vbuf, kvq, len_ref, hbuf, gain_raw, gain_ref, nbuf, wbuf,
            sem_l, sem_g, sem_h, sem_w, sem_k, sem_v, sem_s, sem_r):
    batch, d_model = hid_hbm.shape
    n_w = wbuf.shape[0]
    spi, y = lax.axis_index('sp'), lax.axis_index('tp')
    c = spi % 2
    partner = {'tp': y, 'sp': spi + 1 - 2 * c}
    base = spi * seq_block
    rows_h = batch // HID
    seq_rows = seq_block * kv
    per_piece = batch // PIECES
    crow = per_piece * seq_rows

    hid_copies = [pltpu.make_async_copy(hid_hbm.at[pl.ds(i * rows_h, rows_h)], hbuf.at[pl.ds(i * rows_h, rows_h)], sem_h.at[i])
                  for i in range(HID)]
    len_copy = pltpu.make_async_copy(len_hbm, len_ref, sem_l)
    gain_copy = pltpu.make_async_copy(gain_hbm, gain_raw, sem_g)

    def w_copy(j, src, first):
        return pltpu.make_async_copy(src.at[:, pl.ds(first, BLOCK)], wbuf.at[j], sem_w.at[j])

    def q_copy(j):
        return w_copy(j, wq_hbm, pl.multiple_of(c * (n_w - 1) * BLOCK + (j - 1) * BLOCK, BLOCK))

    def cache_copies(p):
        part = pl.ds(pl.multiple_of(p * crow, crow), crow)
        return [pltpu.make_async_copy(src.at[part], buf.at[part], sem)
                for src, buf, sem in ((kc_hbm, kbuf, sem_k), (vc_hbm, vbuf, sem_v))]

    def trade(j):
        slot = kvq.at[c * n_w + j]
        return remote(slot, slot, sem_s, sem_r.at[j], partner)

    def arrival(j):
        slot = kvq.at[(1 - c) * n_w + j]
        return remote(slot, slot, sem_s, sem_r.at[j], partner)

    for cp in hid_copies + [gain_copy, len_copy]:
        cp.start()
    gain_copy.wait()
    gain_ref[...] = gain_raw[...].astype(F32).reshape(gain_ref.shape)
    hid_copies[0].wait()

    q_copy(1).start()

    def kv_start():
        @pl.when(c == 0)
        def _():
            w_copy(0, wk_hbm, 0).start()

        @pl.when(c == 1)
        def _():
            w_copy(0, wv_hbm, 0).start()

    step = 2 * SUB
    wide = SUB * LANES

    def norm_rows(r, carry):
        row = pl.ds(pl.multiple_of(r * step, step), step)
        cuts = [slice(w, w + wide) for w in range(0, d_model, wide)]
        total = jnp.zeros((step, 1), F32)
        for cut in cuts:
            v = hbuf[row, cut].astype(F32)
            total = total + jnp.sum(v * v, axis=1, keepdims=True)
        inv = lax.rsqrt(total / d_model + EPS)
        for cut in cuts:
            nbuf[row, cut] = (hbuf[row, cut].astype(F32) * inv * gain_ref[:, cut]).astype(BF16)
        return carry

    for i in range(HID):
        if i:
            hid_copies[i].wait()
            if i + 1 < n_w:
                q_copy(i + 1).start()
            else:
                kv_start()
        lax.fori_loop(i * rows_h // step, (i + 1) * rows_h // step, norm_rows, 0, unroll=True)
    enter()

    per_step = PIECES // n_w

    def columns(it, carry):
        j = (it + 1) % n_w
        w_copy(j, wk_hbm, 0).wait()
        @pl.when(it < 2)
        def _():
            for i in range(2 * per_step):
                for cp in cache_copies(it * 2 * per_step + i):
                    cp.start()

        @pl.when(it > 0)
        def _():
            trade(it).start()

        res = jnp.dot(nbuf[...], wbuf[j], preferred_element_type=F32)
        for i in range(BLOCK // LANES):
            kvq[c * n_w + j, pl.ds(i, batch, stride=BLOCK // LANES), :] = res[:, i * LANES:(i + 1) * LANES]
        return carry

    lax.fori_loop(0, n_w, columns, 0)
    trade(0).start()
    len_copy.wait()
    for src, buf, sem in ((kc_hbm, kbuf, sem_k), (vc_hbm, vbuf, sem_v)):
        pltpu.make_async_copy(src, buf, sem).wait()
    for j in range(1, n_w):
        arrival(j).wait_recv()

    pair_row = iota((step, LANES), 0) % kv
    slot_pos = iota((seq_rows, LANES), 0) // kv

    def update(p, carry):
        for i in range(per_piece):
            b = p * per_piece + i
            here = slot_pos == len_ref[b] - base
            rows = pl.ds(pl.multiple_of(b * seq_rows, step), seq_rows)
            for core, buf in enumerate((kbuf, vbuf)):
                new = kvq[core * n_w, pl.ds(b * kv, 1), :]
                for n in range(1, kv):
                    new = jnp.where(pair_row == n, kvq[core * n_w, pl.ds(b * kv + n, 1), :], new)
                new = jnp.concatenate([new.astype(BF16)] * (seq_rows // step), axis=0)
                buf[rows, :] = jnp.where(here, new, buf[rows, :])
        return carry

    def new_tokens():
        lax.fori_loop(0, PIECES, update, 0)
        sent = kvq.at[pl.ds(c * n_w, n_w)]
        remote(sent, sent, sem_s, sem_r.at[0], partner).wait_send()

    return arrival(0).wait_recv, new_tokens


def store_kernel(*refs):
    copies = [pltpu.make_async_copy(refs[i], refs[N_OUTS + i], refs[-1].at[i]) for i in range(N_OUTS)]
    for cp in copies:
        cp.start()
    for cp in copies:
        cp.wait()


def decode_kernel(seq_block, kv, heads, *refs):
    inputs, wo_hbm, outs = refs[:N_INPUTS], refs[N_INPUTS], refs[N_INPUTS + 1:N_INPUTS + N_OUTS + 1]
    kvq, len_ref, hbuf, *rest = refs[N_INPUTS + N_OUTS + 1:]
    kbuf, vbuf, out_ref = outs

    def first(enter):
        return project(seq_block, kv, enter, *inputs, kbuf, vbuf, kvq, len_ref, hbuf, *rest[:N_PROJECT])

    exchange(seq_block, kv, heads, first, kbuf, vbuf, kvq, len_ref, hbuf, wo_hbm, out_ref, *rest[N_PROJECT:])


def exchange(seq_block, kv, heads, first_part, kbuf, vbuf, kvq, len_ref, hbuf, wo_hbm, out_ref,
             score_a, score_b, newest, acc, pbuf, xsend, xrecv, obuf, lhs, wbuf, ysend, yrecv, gbuf,
             sem_w, sem_ps, sem_pr, sem_xs, sem_xr, sem_os, sem_or, sem_ys, sem_yr,
             sem_fs, sem_fr, sem_ss, sem_sr, sem_ds, sem_dr):
    batch, d_model = out_ref.shape
    spi, y = lax.axis_index('sp'), lax.axis_index('tp')
    sp, ny = lax.axis_size('sp'), lax.axis_size('tp')
    nx = sp // 2
    x, c = spi // 2, spi % 2
    base = spi * seq_block
    seq_rows = seq_block * kv
    n_w = kvq.shape[0] // 2
    unit = batch // (sp * SPLITS * 2)
    ur = unit * heads
    rows = batch // nx
    part = rows // (2 * SPLITS)
    half_d = d_model // 2
    cols = half_d // ny
    hc = cols // 2

    def at_x(d):
        return (x + d + nx) % nx

    def at_y(d):
        return (y + d + ny) % ny

    partner = {'tp': y, 'sp': spi + 1 - 2 * c}
    x_dev = {d: {'tp': y, 'sp': at_x(d) * 2 + c} for d in (2, 1, -1)}
    y_dev = {d: {'tp': at_y(d), 'sp': spi} for d in (2, 1, -1)}

    barrier = meet([partner, *x_dev.values(), *y_dev.values()])
    w_copies = []
    for k in range(ROUTES):
        col = pl.multiple_of(c * half_d + at_y(HOPS[k]) * cols, LANES)
        w_copies.append(pltpu.make_async_copy(wo_hbm.at[:, pl.ds(col, cols)], wbuf.at[k], sem_w.at[k]))
    new_arrived, new_tokens = first_part(lambda: pl.semaphore_wait(barrier, 1 + len(x_dev) + len(y_dev)))
    for cp in w_copies:
        cp.start()

    per = BLOCK // LANES
    tile = GROUP * per
    n_tiles = heads // per
    qrows = GROUP * heads
    krows = GROUP * seq_rows
    row_id, col_id = iota((qrows, krows), 0), iota((qrows, krows), 1)
    same = (row_id % tile // per == col_id // seq_rows) & (row_id // (qrows // kv) == col_id % kv)
    col_row = iota((1, krows), 1)
    col_seq = col_row // seq_rows
    col_pos = col_row % seq_rows // kv
    diag = iota((ur, LANES), 0) == iota((ur, LANES), 1)
    fold = LANES ** -0.5 * LOG2E
    halves = [(core, h) for core in range(2) for h in range(2)]
    groups = [(core, h, g) for core, h in halves for g in range(unit // GROUP)]

    def pair(k, n):
        return remote(acc.at[n, k, 1 - c], pbuf.at[n, k], sem_ps.at[n], sem_pr.at[n * ROUTES + k], partner)

    def first(n, k, core, h, g):
        dest = at_x(HOPS[k])
        return (((dest * 2 + core) * SPLITS + n) * 2 + h) * unit + g * GROUP

    def score(n, k, sbuf):
        for at, where in enumerate(groups):
            b0 = first(n, k, *where)
            rows8 = pl.ds(pl.multiple_of(b0 * per, tile), tile)
            q = jnp.concatenate([kvq[core * n_w + j, rows8, :] for core in range(2) for j in range(1, n_w)], axis=0)
            keys = kbuf[pl.ds(pl.multiple_of(b0 * seq_rows, krows), krows), :]
            s = lax.dot_general(q.astype(BF16), keys, (((1,), (1,)), ((), ())), preferred_element_type=F32)
            last = jnp.full((1, krows), len_ref[b0] - base, jnp.int32)
            for i in range(1, GROUP):
                last = jnp.where(col_seq == i, len_ref[b0 + i] - base, last)
            sbuf[at] = jnp.where(same & (col_pos < last), s * fold, NEG_BIG)

    def finish(n, k, sbuf):
        stats = []
        for at, where in enumerate(groups):
            core, h, g = where
            s = sbuf[at]
            m = jnp.maximum(jnp.max(s, axis=1, keepdims=True), FLOOR)
            e = jnp.exp2(s - m)
            stats.append((m, jnp.sum(e, axis=1, keepdims=True)))
            values = vbuf[pl.ds(pl.multiple_of(first(n, k, *where) * seq_rows, krows), krows), :]
            o = jnp.dot(e.astype(BF16), values, preferred_element_type=F32)
            for t in range(n_tiles):
                row = (t * (unit // GROUP) + g) * tile
                acc[n, k, core, h, row:row + tile, :] = o[t * tile:(t + 1) * tile]
        for core, h in halves:
            mine = [stat for where, stat in zip(groups, stats) if where[:2] == (core, h)]
            packed = []
            for which in range(2):
                col = jnp.concatenate([stat[which][t * tile:(t + 1) * tile] for t in range(n_tiles) for stat in mine], axis=0)
                packed.append(jnp.sum(jnp.where(diag, jnp.broadcast_to(col, diag.shape), 0.0), axis=0, keepdims=True))
            packed.append(jnp.zeros((STAT - len(packed), LANES), F32))
            acc[n, k, core, h, ur:ur + STAT, :] = jnp.concatenate(packed, axis=0)
        pair(k, n).start()

    def column(stat):
        return jnp.sum(jnp.where(diag, jnp.broadcast_to(stat, diag.shape), 0.0), axis=1, keepdims=True)

    def merge(refs):
        both = [(r[ur:ur + 1, :], r[ur + 1:ur + 2, :]) for r in refs]
        peak = functools.reduce(jnp.maximum, [m for m, _ in both])
        scale = [jnp.exp2(m - peak) for m, _ in both]
        denom = sum(l * s for (_, l), s in zip(both, scale))
        total = sum(r[:ur, :] * column(s) for r, s in zip(refs, scale))
        return total, peak, denom

    def merge_into(dst, refs):
        total, peak, denom = merge(refs)
        dst[:ur, :] = total
        dst[ur:ur + STAT, :] = jnp.concatenate([peak, denom, jnp.zeros((STAT - 2, LANES), F32)], axis=0)

    def sends(send, recv, ssem, rsem, devs):
        return [[remote(send.at[n, i], recv.at[n, i], ssem.at[n], rsem.at[n * AWAY + i], devs[d])
                 for i, d in enumerate(HOPS[:AWAY])] for n in range(SPLITS)]

    xc = sends(xsend, xrecv, sem_xs, sem_xr, x_dev)
    yc = sends(ysend, yrecv, sem_ys, sem_yr, y_dev)
    oc = [remote(obuf.at[n, c], obuf.at[n, c], sem_os.at[n], sem_or.at[n], partner) for n in range(SPLITS)]

    def both(n, k, h):
        return [acc.at[n, k, c, h], pbuf.at[n, k, h]]

    def x_start(n, k):
        if k == OWN:
            return
        pair(k, n).wait_recv()
        for h in range(2):
            merge_into(xsend.at[n, k, h], both(n, k, h))
        xc[n][k].start()

    def fresh(n):
        two = unit * kv
        parity = iota((two, LANES), 0) % kv
        for h in range(2):
            rows16 = pl.ds(pl.multiple_of((((x * 2 + c) * SPLITS + n) * 2 + h) * two, two), two)
            score_col = []
            for core in range(kv):
                k, v = [jnp.where(parity == core, r, pltpu.roll(r, 1 if core == 0 else two - 1, 0))
                        for r in (kvq[i * n_w, rows16, :].astype(BF16).astype(F32) for i in range(2))]
                for j in range(1, n_w):
                    q = kvq[core * n_w + j, rows16, :].astype(BF16).astype(F32)
                    score_col.append(jnp.sum(q * k, axis=1, keepdims=True) * fold)
                    at = (core * (n_w - 1) + j - 1) * two
                    newest[n, h, at:at + two, :] = v
            col = jnp.broadcast_to(jnp.concatenate(score_col, axis=0), diag.shape)
            peak = jnp.sum(jnp.where(diag, col, 0.0), axis=0, keepdims=True)
            newest[n, h, ur:ur + STAT, :] = jnp.where(iota((STAT, LANES), 0) == 0, jnp.broadcast_to(peak, (STAT, LANES)), 1.0)

    def x_end(n):
        pair(OWN, n).wait_recv()
        for cp in xc[n]:
            cp.wait_recv()
        for h in range(2):
            total, _, denom = merge(both(n, OWN, h) + [newest.at[n, h]] + [xrecv.at[n, i, h] for i in range(AWAY)])
            obuf[n, c, h * ur:(h + 1) * ur, :] = (total / column(denom)).astype(BF16).astype(F32)
        oc[n].start()

    def product(n, k):
        if n == 0:
            w_copies[k].wait()
        return jnp.dot(lhs[n].astype(BF16), wbuf[k], preferred_element_type=F32)

    def y_start(n):
        oc[n].wait_recv()
        for core, h in halves:
            at = core * part + h * unit
            for t in range(n_tiles):
                for i in range(per):
                    head = (t * per + i) * LANES
                    lhs[n, at:at + unit, head:head + LANES] = obuf[
                        n, core, pl.ds(h * ur + t * unit * per + i, unit, stride=per), :]
        for i in range(AWAY):
            prod = product(n, i)
            for h in range(2):
                ysend[n, i, h] = prod[:, h * hc:(h + 1) * hc]
            yc[n][i].start()

    f = x + c * (y - x)
    s = y + c * (x - y)
    def go(copy):
        copy.start()

    def f_dev(d):
        return {'tp': (y + c * d + ny) % ny, 'sp': ((x + (1 - c) * d + nx) % nx) * 2 + c}

    def s_dev(d):
        return {'tp': (y + (1 - c) * d + ny) % ny, 'sp': ((x + c * d + nx) % nx) * 2 + c}

    def block(n, fd, sd):
        return gbuf.at[n, c, (f + fd + nx) % nx, (s + sd + ny) % ny]

    def kind(d, is_half):
        return 2 if d == 2 else is_half * 2 + (d > 0)

    def along(ring, n, fd, sd, d, is_half=False):
        ref = block(n, fd, sd)
        if is_half:
            ref = ref.at[0 if d > 0 else 1]
        if ring == 'f':
            i = n * ROUTES + kind(d, is_half)
            return remote(ref, ref, sem_fs.at[n], sem_fr.at[i], f_dev(d))
        i = (n * nx + fd % nx) * ROUTES + kind(d, is_half)
        return remote(ref, ref, sem_ss.at[n], sem_sr.at[i], s_dev(d))

    def over(n, fd, sd):
        i = (n * nx + fd % nx) * ny + sd % ny
        ref = block(n, fd, sd)
        return remote(ref, ref, sem_ds.at[n], sem_dr.at[i], partner)

    def place(n, ci, fi, si, swap):
        xi, yi = fi + swap * (si - fi), si + swap * (fi - si)
        for h in range(2):
            at = pl.ds(pl.multiple_of(ci * half_d + yi * cols + h * hc, LANES), hc)
            for core in range(2):
                first = pl.multiple_of(xi * rows + (core * SPLITS + n) * part, part)
                out_ref[pl.ds(first, part), at] = gbuf[n, ci, fi, si, h, core * part:(core + 1) * part, :].astype(BF16)

    def place_here(n, fd, sd):
        place(n, c, (f + fd + nx) % nx, (s + sd + ny) % ny, c)

    def spread(n, fd):
        for d in HOPS[:AWAY] if (n, fd) in ONE_HOP_S else (1, -1):
            go(along('s', n, fd, 0, d))
        go(over(n, fd, 0))

    def y_end(n):
        own = product(n, OWN)
        for cp in yc[n]:
            cp.wait_recv()
        for h in range(2):
            total = sum([yrecv[n, i, h] for i in range(AWAY)], own[:, h * hc:(h + 1) * hc])
            at = pl.ds(pl.multiple_of(c * half_d + y * cols + h * hc, LANES), hc)
            kept = jnp.concatenate([hbuf[pl.ds(pl.multiple_of(x * rows + (core * SPLITS + n) * part, part), part), at]
                                    for core in range(2)], axis=0)
            gbuf[n, c, f, s, h] = (kept.astype(F32) + total).astype(BF16).astype(F32)
        for d in (1, -1, 2) if n in ONE_HOP_F else (1, -1):
            go(along('f', n, 0, 0, d))
        spread(n, 0)
        place_here(n, 0, 0)

    def f_ring(n):
        for d in (1, -1):
            along('f', n, -d, 0, d).wait_recv()
            if n not in ONE_HOP_F:
                go(along('f', n, -d, 0, d, True))
            spread(n, -d)
        for d in (1, -1):
            place_here(n, -d, 0)

    def f_end(n):
        if n in ONE_HOP_F:
            along('f', n, 2, 0, 2).wait_recv()
        else:
            for d in (1, -1):
                along('f', n, 2, 0, d, True).wait_recv()
        spread(n, 2)
        place_here(n, 2, 0)

    def s_ring(n, fd):
        for d in (1, -1):
            along('s', n, fd, -d, d).wait_recv()
            if (n, fd) not in ONE_HOP_S:
                go(along('s', n, fd, -d, d, True))
            go(over(n, fd, -d))
        for d in (1, -1):
            place_here(n, fd, -d)

    def s_end(n, fd):
        if (n, fd) in ONE_HOP_S:
            along('s', n, fd, 2, 2).wait_recv()
        else:
            for d in (1, -1):
                along('s', n, fd, 2, d, True).wait_recv()
        go(over(n, fd, 2))
        place_here(n, fd, 2)

    def take(n, fd, sd):
        i = (n * nx + fd % nx) * ny + sd % ny
        fi, si = (s + fd + nx) % nx, (f + sd + ny) % ny
        ref = gbuf.at[n, 1 - c, fi, si]
        remote(ref, ref, sem_ds.at[n], sem_dr.at[i], partner).wait_recv()
        place(n, 1 - c, fi, si, 1 - c)

    def stage(n, i):
        if i == 0:
            f_ring(n)
            s_ring(n, 0)
        elif i == 1:
            f_end(n)
            s_ring(n, -1)
            s_ring(n, 1)
            s_end(n, 0)
        elif i == 2:
            for fd in (0, -1, 1):
                take(n, fd, 0)
            s_ring(n, 2)
            s_end(n, -1)
            s_end(n, 1)
        else:
            for fd, sd in ((2, 0), (0, -1), (0, 1), (0, 2), (-1, -1), (-1, 1), (1, -1), (1, 1)):
                take(n, fd, sd)
            s_end(n, 2)

    scores = (score_a, score_b)
    steps = [(n, k) for n in range(SPLITS) for k in range(ROUTES)]
    score(*steps[0], scores[0])
    for i, step in enumerate(steps):
        if i + 1 < len(steps):
            score(*steps[i + 1], scores[(i + 1) % 2])
        finish(*step, scores[i % 2])
        if i >= LAG:
            x_start(*steps[i - LAG])
    for step in steps[-LAG:]:
        x_start(*step)
    new_arrived()
    for n in range(SPLITS):
        fresh(n)
    new_tokens()
    x_end(0)
    y_start(0)
    x_end(1)
    y_start(1)
    y_end(0)
    y_end(1)
    for i in range(ROUTES):
        for n in range(SPLITS):
            stage(n, i)
    for n in range(SPLITS):
        for fd, sd in ((2, -1), (2, 1), (-1, 2), (1, 2), (2, 2)):
            take(n, fd, sd)
    for n in range(SPLITS):
        done = ((acc.at[n, :, 1 - c], sem_ps), (xsend.at[n], sem_xs), (obuf.at[n, c], sem_os), (ysend.at[n], sem_ys),
                (gbuf.at[n, c, 0, pl.ds(0, AWAY)], sem_fs), (gbuf.at[n, c, pl.ds(0, AWAY)], sem_ss), (gbuf.at[n, c], sem_ds))
        for ref, sem in done:
            remote(ref, ref, sem.at[n], sem_or.at[n], partner).wait_send()


def solution(mesh):
    cache_spec = P('dp', 'sp', 'tp', None)
    sp = mesh.shape['sp']
    tp = mesh.shape['tp']

    def local_step(hidden, lengths, k_cache, v_cache, norm_gain, w_query, w_key, w_value, w_out):
        batch, seq_block, kv, head_dim = k_cache.shape
        d_model = hidden.shape[1]
        width = w_query.shape[1]
        heads = width // head_dim
        n_w = width // (2 * BLOCK) + 1
        flat = batch * seq_block * kv
        hbm = pl.BlockSpec(memory_space=pltpu.HBM)
        vmem = pl.BlockSpec(memory_space=pltpu.VMEM)
        shape = jax.ShapeDtypeStruct
        buf = pltpu.VMEM

        def dma(*shapes):
            return [pltpu.SemaphoreType.DMA(s) if s else pltpu.SemaphoreType.DMA for s in shapes]

        nx = sp // 2
        rows = batch // nx
        cols = d_model // (2 * tp)
        ur = batch // (sp * SPLITS * 2) * heads
        scored = buf((batch // (ROUTES * SPLITS * GROUP), GROUP * heads, GROUP * seq_block * kv), F32)
        travel = buf((SPLITS, AWAY, 2, ur + STAT, head_dim), F32)
        yblock = buf((SPLITS, AWAY, 2, rows // SPLITS, cols // 2), F32)
        n_x, n_f = SPLITS * AWAY, SPLITS * ROUTES
        n_s = n_f * nx
        n_d = SPLITS * nx * tp
        split = (SPLITS,)
        k_new, v_new, out = pl.pallas_call(
            functools.partial(decode_kernel, seq_block, kv, heads),
            out_shape=(buf((flat, head_dim), BF16), buf((flat, head_dim), BF16), buf((batch, d_model), BF16)),
            in_specs=[hbm] * (N_INPUTS + 1),
            out_specs=(vmem, vmem, vmem),
            scratch_shapes=[
                buf((2 * n_w, batch * BLOCK // head_dim, head_dim), F32),
                pltpu.SMEM((batch,), jnp.int32),
                buf((batch, d_model), BF16),
                buf((d_model,), BF16),
                buf((1, d_model), F32),
                buf((batch, d_model), BF16),
                buf((n_w, d_model, BLOCK), BF16),
                *dma((), (), (HID,), (n_w,), (), (), (), (n_w,)),
                scored, scored,
                buf((SPLITS, 2, ur + STAT, head_dim), F32),
                buf((SPLITS, ROUTES, 2, 2, ur + STAT, head_dim), F32),
                buf((SPLITS, ROUTES, 2, ur + STAT, head_dim), F32),
                travel, travel,
                buf((SPLITS, 2, 2 * ur, head_dim), F32),
                buf((SPLITS, rows // SPLITS, width), F32),
                buf((ROUTES, width, cols), BF16),
                yblock, yblock,
                buf((SPLITS, 2, nx, tp, 2, rows // SPLITS, cols // 2), F32),
                *dma((ROUTES,), split, (n_f,), split, (n_x,), split, split, split, (n_x,),
                     split, (n_f,), split, (n_s,), split, (n_d,)),
            ],
            compiler_params=pltpu.CompilerParams(collective_id=0, has_side_effects=True, vmem_limit_bytes=VMEM_MIB * MIB),
            name='decode_step',
        )(lengths, hidden, norm_gain, w_query, w_key, w_value,
          k_cache.reshape(flat, head_dim), v_cache.reshape(flat, head_dim), w_out)
        results = (k_new, v_new, out)
        k_new, v_new, out = pl.pallas_call(
            store_kernel,
            out_shape=tuple(shape(r.shape, r.dtype) for r in results),
            in_specs=[vmem] * N_OUTS,
            out_specs=(hbm,) * N_OUTS,
            scratch_shapes=dma((N_OUTS,)),
            compiler_params=pltpu.CompilerParams(vmem_limit_bytes=MIB),
            name='store',
        )(*results)
        return out, k_new.reshape(k_cache.shape), v_new.reshape(v_cache.shape)

    return jax.shard_map(
        local_step,
        mesh=mesh,
        in_specs=(P('dp', None), P('dp'), cache_spec, cache_spec, P(None), P(None, 'tp'), P(None, 'tp'), P(None, 'tp'), P('tp', None)),
        out_specs=(P('dp', None), cache_spec, cache_spec),
        check_vma=False,
    )
```
